768 devices in a mesh: gx: 4 (over y_lo, core), gy: 16 (over x, y_hi), gz: 12 (over z).
Axes of the slice: x: 4, y: 8 (y_hi: 4, y_lo: 2; y = y_hi * 2 + y_lo), z: 12, core: 2. Of those that a mesh axis runs over, the one named last changes fastest.
Arguments:
- velocity: float32 [3, 32, 256, 1536], P(None, 'gx', 'gy', 'gz'), may hold values from -6 to 6
- diffusion: float32 [3], replicated, may hold values from 0.5 to 4
Outputs:
- viscous_velocity: float32 [3, 32, 256, 1536], P(None, 'gx', 'gy', 'gz')
- residual: float32 [3, 32, 256, 1536], P(None, 'gx', 'gy', 'gz')
The draws below stay inside these ranges and needn't reach their ends.
All inputs are finite; a program needn't handle non-finite values.
Results may differ from the reference program's by a relative error of at most 0.0003.
Values sent between devices are 32-bit elements; how exact they have to be, the bound alone decides.
No kernel may reach another device: no remote copies, remote signals or barrier semaphores. Data moves between devices by JAX's collectives and lax.ppermute only.
A program may use at most 32 MiB of HBM per device.

```python
import math
import jax
import jax.numpy as jnp

ITERS = 3
NX = 32
NY = 256
NZ = 1536


def level_of(stream_key, shape, cuts, least, top_value):
    def one(axis_at, parts):
        draws = jax.random.uniform(jax.random.fold_in(jax.random.fold_in(stream_key, 6), axis_at), (parts,), jnp.float32, least / len(cuts), top_value / len(cuts))
        return jnp.repeat(jnp.exp(draws), shape[axis_at] // parts).reshape((-1,) + (1,) * (len(shape) - axis_at - 1))

    loudness = one(*cuts[0])
    for cut in cuts[1:]:
        loudness = loudness * one(*cut)
    return loudness


def bell_draw(own_key, extent, width, limit, pieces=(), kind=jnp.bfloat16):
    result = width * jax.random.normal(own_key, extent, jnp.float32)
    if pieces:
        result = result * level_of(own_key, extent, pieces, -0.22, 0.18)
    return jnp.clip(result, -limit, limit).astype(kind)


def setup_inputs(seed: int = 0) -> dict:
    key_list = jax.random.split(jax.random.key(seed), 3)
    return {
        "velocity": bell_draw(key_list[0], (3, NX, NY, NZ), 1.0, 6.0, ((1, 4), (2, 16), (3, 12)), jnp.float32),
        "diffusion": jnp.clip(jnp.exp(jax.random.uniform(key_list[1], (3,), jnp.float32, math.log(0.5), math.log(4.0))), 0.5, 4.0),
    }


time_step = 0.25


def trimmed(array, axis, offset):
    index = [slice(None)] + [slice(1, -1)] * 3
    index[axis + 1] = slice(1 + offset, array.shape[axis + 1] - 1 + offset)
    return array[tuple(index)]


def advection(padded):
    total = None
    for axis in range(3):
        flux = padded[axis:axis + 1] * padded
        term = (trimmed(flux, axis, 1) - trimmed(flux, axis, -1)) * 0.5
        total = term if total is None else total + term
    return total


def operate(field, coefficient):
    padded = jnp.pad(field, ((0, 0), (1, 1), (1, 1), (1, 1)))
    beside = padded[:, 2:, 1:-1, 1:-1] + padded[:, :-2, 1:-1, 1:-1]
    beside = beside + padded[:, 1:-1, 2:, 1:-1] + padded[:, 1:-1, :-2, 1:-1]
    beside = beside + padded[:, 1:-1, 1:-1, 2:] + padded[:, 1:-1, 1:-1, :-2]
    return (1.0 + 6.0 * coefficient) * field - coefficient * beside


def inner(first, second):
    return jnp.sum(first * second, axis=(1, 2, 3))[:, None, None, None]


def reference(velocity, diffusion):
    coefficient = diffusion[:, None, None, None]
    padded = jnp.pad(velocity, ((0, 0), (1, 1), (1, 1), (1, 1)))
    section = velocity - time_step * advection(padded)
    solution = jnp.zeros_like(section)
    residual = section
    direction = section
    norm_now = inner(residual, residual)
    for iteration in range(ITERS):
        image = operate(direction, coefficient)
        step_size = norm_now / inner(direction, image)
        solution = solution + step_size * direction
        residual = residual - step_size * image
        norm_next = inner(residual, residual)
        direction = residual + (norm_next / norm_now) * direction
        norm_now = norm_next
    return solution, residual
```

```python
import jax
import jax.numpy as jnp
from jax import lax
from jax.sharding import Mesh
from jax.sharding import PartitionSpec as P

ITERS = 3
GX_GY_GZ = ("gx_0", "gx_1", "gy_0", "gy_1", "gz")
GX = ("gx_0", "gx_1")
GY = ("gy_0", "gy_1")


time_step = 0.25


def extended(value, sides, width):
    edges = {}
    for axis, dim in sides:
        size, length = (lax.axis_size(axis), value.shape[dim])
        up = [(i, (i + 1) % size) for i in range(size - 1)]
        last = lax.slice_in_dim(value, length - width, length, axis=dim)
        first = lax.slice_in_dim(value, 0, width, axis=dim)
        edges[dim] = (
            lax.ppermute(last, axis, up),
            lax.ppermute(first, axis, [(b, a) for a, b in up]),
        )
    done = []
    for _, dim in sides:
        low, high = edges[dim]
        around = [(width, width) if d in done else (0, 0) for d in range(value.ndim)]
        value = jnp.concatenate([jnp.pad(low, around), value, jnp.pad(high, around)], axis=dim)
        done.append(dim)
    return value


def over_axes(value, axes):
    for axis in axes:
        value = lax.psum(value, axis)
    return value


def with_halo(value, sides, width):
    for axis, dim in sides:
        size, length = (lax.axis_size(axis), value.shape[dim])
        up = [(i, (i + 1) % size) for i in range(size - 1)]
        down = [(j, i) for i, j in up]
        last = lax.slice_in_dim(value, length - width, length, axis=dim)
        first = lax.slice_in_dim(value, 0, width, axis=dim)
        before = lax.ppermute(last, axis, up)
        after = lax.ppermute(first, axis, down)
        value = jnp.concatenate([before, value, after], axis=dim)
    return value


def trimmed(array, axis, offset):
    index = [slice(None)] + [slice(1, -1)] * 3
    index[axis + 1] = slice(1 + offset, array.shape[axis + 1] - 1 + offset)
    return array[tuple(index)]


def advection(padded):
    total = None
    for axis in range(3):
        flux = padded[axis : axis + 1] * padded
        term = (trimmed(flux, axis, 1) - trimmed(flux, axis, -1)) * 0.5
        total = term if total is None else total + term
    return total


def apply_padded(padded, field, coefficient):
    beside = padded[:, 2:, 1:-1, 1:-1] + padded[:, :-2, 1:-1, 1:-1]
    beside = beside + padded[:, 1:-1, 2:, 1:-1] + padded[:, 1:-1, :-2, 1:-1]
    beside = beside + padded[:, 1:-1, 1:-1, 2:] + padded[:, 1:-1, 1:-1, :-2]
    return (1.0 + 6.0 * coefficient) * field - coefficient * beside


def operate(field, coefficient):
    padded = extended(field, ((GX, 1), (GY, 2), ("gz", 3)), 1)
    return apply_padded(padded, field, coefficient)


def products(residual, image):
    sums = (
        over_axes(jnp.sum(residual * residual, axis=(1, 2, 3)), GX_GY_GZ),
        over_axes(jnp.sum(residual * image, axis=(1, 2, 3)), GX_GY_GZ),
    )
    return (sums[0][:, None, None, None], sums[1][:, None, None, None])


def valid_cells(block_index, block_total, count, margin):
    position = block_index * count - margin + jnp.arange(count + 2 * margin)
    return ((position >= 0) & (position < count * block_total)).astype(jnp.float32)


def inside_mask(velocity, margin):
    mask_x = valid_cells(lax.axis_index(GX), lax.axis_size(GX), velocity.shape[1], margin)
    mask_y = valid_cells(lax.axis_index(GY), lax.axis_size(GY), velocity.shape[2], margin)
    mask_z = valid_cells(lax.axis_index("gz"), lax.axis_size("gz"), velocity.shape[3], margin)
    return (mask_x[:, None, None] * mask_y[None, :, None] * mask_z[None, None, :])[None]


def identity_cut(field):
    return field


def gathered_sum(value, axes):
    count = lax.axis_size(axes)
    spread = jnp.broadcast_to(value[None], (count,) + value.shape)
    return jnp.sum(lax.all_to_all(spread, axes, 0, 0, tiled=True), axis=0)


def weights_of(moments, coefficient):
    scale = 6.0 * coefficient

    def inner(first, second):
        return sum(f * s * moments[i + j] for i, f in enumerate(first) for j, s in enumerate(second))

    def plus(first, factor, second):
        size = max(len(first), len(second))
        padded = [list(v) + [0.0] * (size - len(v)) for v in (first, second)]
        return [f + factor * s for f, s in zip(*padded)]

    one = jnp.ones_like(coefficient)
    total, residual, direction = [], [one], [one]
    now = moments[0]
    for iteration in range(ITERS):
        image = plus(direction, scale, [0.0] + direction)
        step = now / inner(direction, image)
        total = plus(total, step, direction)
        residual = plus(residual, -step, image)
        if iteration + 1 < ITERS:
            new = inner(residual, residual)
            direction = plus(residual, new / now, direction)
            now = new
    return total, residual


def laplace(field):
    padded = jnp.pad(field, ((0, 0), (1, 1), (1, 1), (1, 1)))
    beside = padded[:, 2:, 1:-1, 1:-1] + padded[:, :-2, 1:-1, 1:-1]
    beside = beside + padded[:, 1:-1, 2:, 1:-1] + padded[:, 1:-1, :-2, 1:-1]
    beside = beside + padded[:, 1:-1, 1:-1, 2:] + padded[:, 1:-1, 1:-1, :-2]
    return field - beside * (1.0 / 6.0)


def body(velocity, diffusion):
    margin = ITERS
    deep = with_halo(velocity, ((GX, 1), (GY, 2), ("gz", 3)), margin + 1)
    inside = inside_mask(velocity, margin)
    section = (deep[:, 1:-1, 1:-1, 1:-1] - time_step * advection(deep)) * inside

    def cut(field):
        return field[:, margin:-margin, margin:-margin, margin:-margin]

    powers = [section]
    for _ in range(ITERS):
        powers.append(laplace(powers[-1]) * inside)
    powers = [cut(p) for p in powers]
    local = [jnp.sum(powers[k // 2] * powers[(k + 1) // 2], axis=(1, 2, 3)) for k in range(2 * ITERS)]
    moments = gathered_sum(gathered_sum(jnp.concatenate(local), GX + GY), ("gz",))
    moments = [moments[3 * k : 3 * k + 3] for k in range(2 * ITERS)]
    total, rest = weights_of(moments, diffusion)
    total, rest = ([w[:, None, None, None] for w in v] for v in (total, rest))
    return (
        sum(w * p for w, p in zip(total, powers)),
        sum(w * p for w, p in zip(rest, powers)),
    )


def solution(mesh):
    finer = Mesh(
        mesh.devices.reshape(2, 2, 4, 4, mesh.shape["gz"]), ("gx_0", "gx_1", "gy_0", "gy_1", "gz")
    )
    return jax.shard_map(
        body,
        mesh=finer,
        in_specs=(P(None, GX, GY, "gz"), P()),
        out_specs=(P(None, GX, GY, "gz"), P(None, GX, GY, "gz")),
        check_vma=False,
    )
```

```python
import functools

import jax
import jax.numpy as jnp
from jax import lax
from jax.experimental import pallas as pl
from jax.experimental.pallas import tpu as pltpu
from jax.sharding import Mesh
from jax.sharding import PartitionSpec as P

ITERS = 3
GX = ("gx_0", "gx_1")
GY = ("gy_0", "gy_1")
GZ = ("gz",)
HALO = ITERS + 1

time_step = 0.25

NX, NY, NZ = 8, 16, 128
EX, EY = NX + 2 * HALO, NY + 2 * HALO
GROUPS = 4
STEP = NZ // GROUPS
MOMENTS = 2 * ITERS


def lanes(shape):
    return lax.broadcasted_iota(jnp.int32, shape, len(shape) - 1)


def rows(shape):
    return lax.broadcasted_iota(jnp.int32, shape, len(shape) - 2)


def back(value, axis):
    return pltpu.roll(value, value.shape[axis] - 1, axis)


def ahead(value, axis):
    return pltpu.roll(value, 1, axis)


def turned(value, shift):
    shift = shift % value.shape[-1]
    return pltpu.roll(value, shift, value.ndim - 1) if shift else value


def pack_y(own, below, above, up, down):
    def plane(c, i, part):
        if i < NX:
            return own[c, i, part, :]
        return above[c, i - NX, part, :] if i < NX + HALO else below[c, i - NX - HALO, part, :]

    for c in range(3):
        for p in range(8):
            up[c, p, 4:8, :] = plane(c, p, slice(NY - HALO, NY))
            up[c, p, 0:4, :] = plane(c, p + 8, slice(NY - HALO, NY))
            down[c, p, 0:4, :] = plane(c, p, slice(0, HALO))
            down[c, p, 4:8, :] = plane(c, p + 8, slice(0, HALO))


def pack_z(own, below, above, low, high, whole, up, down):
    sub = rows((8, NZ))
    lane = lanes((8, NZ))
    for c in range(3):
        for t in range(3):
            ups = jnp.zeros((8, NZ), jnp.float32)
            downs = jnp.zeros((8, NZ), jnp.float32)
            for i in range(EX):
                if t < 2:
                    part = slice(8 * t, 8 * t + 8)
                    if i < NX:
                        tile = own[c, i, part, :]
                    elif i < NX + HALO:
                        tile = above[c, i - NX, part, :]
                    else:
                        tile = below[c, i - NX - HALO, part, :]
                elif i < 8:
                    tile = jnp.where(sub < 4, high[c, i], low[c, i])
                else:
                    tile = pltpu.roll(jnp.where(sub < 4, low[c, i - 8], high[c, i - 8]), 4, 0)
                whole[c, i, 8 * t : 8 * t + 8, :] = tile
                place = STEP * (i // 4) + 4 * (i % 4)
                here = (lane >= place) & (lane < place + 4)
                ups = jnp.where(here, turned(tile, place - (NZ - HALO)), ups)
                downs = jnp.where(here, turned(tile, place), downs)
            up[c, 8 * t : 8 * t + 8, :] = ups
            down[c, 8 * t : 8 * t + 8, :] = downs


def section_of(at, here, before, after):
    result = []
    for c in range(3):
        slope = after[c] - before[c]
        flux = at[1] * at[c]
        slope = slope + (back(flux, 0) - ahead(flux, 0))
        flux = at[2] * at[c]
        slope = slope + (back(flux, 1) - ahead(flux, 1))
        result.append((at[c] - (0.5 * time_step) * slope) * here)
    return result


def laplace_of(at, before, after):
    beside = (before + after) + (back(at, 0) + ahead(at, 0))
    beside = beside + (back(at, 1) + ahead(at, 1))
    return at - beside * (1.0 / 6.0)


def pairs():
    return [(k // 2, (k + 1) // 2) for k in range(MOMENTS)]


def inner_lanes(place, whole, powers, sums, edge, *work):
    at_x, last_x, at_y, last_y = (place[k] for k in range(4))
    row = rows((EY, NZ))
    keep = jnp.float32(1.0)
    below_y = jnp.where(at_y == 0, 0.0, keep)
    above_y = jnp.where(at_y == last_y, 0.0, keep)
    in_y = jnp.where(row < NY, 1.0, jnp.where(row < NY + HALO, above_y, below_y))
    below_x = in_y * jnp.where(at_x == 0, 0.0, keep)
    above_x = in_y * jnp.where(at_x == last_x, 0.0, keep)

    def inside(x):
        return below_x if x < 0 else (above_x if x >= NX else in_y)

    def plane(x):
        return [whole[c, x % EX] for c in range(3)]

    def products(value):
        return [value[0] * value[c] for c in range(3)]

    lane = lanes((8, NZ))
    for c in range(3):
        for p in range(GROUPS):
            for t in range(3):
                part = slice(8 * t, 8 * t + 8)
                tile = jnp.zeros((8, NZ), jnp.float32)
                for g in range(GROUPS):
                    source = whole[c, GROUPS * g + p, part, :]
                    first = STEP * g + 4
                    tile = jnp.where((lane >= first) & (lane < first + 8), turned(source, first), tile)
                    first = STEP * g + 16
                    tile = jnp.where((lane >= first) & (lane < first + 8), turned(source, first - 120), tile)
                edge[c, p, part, :] = tile

    for x in range(-ITERS, NX + ITERS):
        new = section_of(plane(x), inside(x), products(plane(x - 1)), products(plane(x + 1)))
        for c in range(3):
            work[0][c, x % EX] = new[c]
            if 0 <= x < NX:
                powers[0, c, x] = new[c][:NY]
    for k in range(1, ITERS + 1):
        reach = ITERS - k
        for x in range(-reach, NX + reach):
            for c in range(3):
                source = work[k - 1]
                new = laplace_of(source[c, x % EX], source[c, (x - 1) % EX], source[c, (x + 1) % EX])
                if k < ITERS:
                    new = new * inside(x)
                    work[k][c, x % EX] = new
                if 0 <= x < NX:
                    powers[k, c, x] = new[:NY]
    valid = (lane >= HALO) & (lane < NZ - HALO)
    for c in range(3):
        total = [jnp.zeros((8, NZ), jnp.float32) for _ in range(MOMENTS)]
        for x in range(NX):
            for t in range(2):
                v = [powers[k, c, x, 8 * t : 8 * t + 8, :] for k in range(ITERS + 1)]
                total = [s + v[a] * v[b] for s, (a, b) in zip(total, pairs())]
        for k in range(MOMENTS):
            sums[c, k] = jnp.where(valid, total[k], 0.0)


def edge_lanes(place, edge, low, high, sums, powers, moments, whole, *work):
    at_x, last_x, at_y, last_y, at_z, last_z = (place[k] for k in range(6))
    row = rows((EY, NZ))
    lane = lanes((EY, NZ))
    group, offset = lane // STEP, lane % STEP
    outside = (row >= NY + HALO) & (at_y == 0)
    outside |= (row >= NY) & (row < NY + HALO) & (at_y == last_y)
    outside |= (group == 3) & (at_x == 0)
    outside |= (group == 2) & (at_x == last_x)
    outside |= (offset < 4) & (at_z == 0)
    outside |= (offset >= 24) & (at_z == last_z)
    inside = jnp.where(outside, 0.0, 1.0)
    for c in range(3):
        for p in range(GROUPS):
            value = jnp.where(offset < 4, turned(low[c], -4 * p), edge[c, p])
            whole[c, p] = jnp.where((offset >= 24) & (offset < 28), turned(high[c], 24 - 4 * p), value)

    def beyond(read, p):
        return turned(read(0), -STEP) if p == GROUPS - 1 else read(p + 1)

    def behind(read, p):
        return turned(read(GROUPS - 1), STEP) if p == 0 else read(p - 1)

    for p in range(GROUPS):
        at = [whole[c, p] for c in range(3)]
        before, after = (
            [side(lambda q, c=c: whole[0, q] * whole[c, q], p) for c in range(3)] for side in (behind, beyond)
        )
        new = section_of(at, inside, before, after)
        for c in range(3):
            work[0][c, p] = new[c]
            powers[0, c, p] = new[c][:NY]
    for k in range(1, ITERS + 1):
        for p in range(GROUPS):
            for c in range(3):
                read = functools.partial(lambda c, q: work[k - 1][c, q], c)
                new = laplace_of(read(p), behind(read, p), beyond(read, p))
                if k < ITERS:
                    new = new * inside
                    work[k][c, p] = new
                powers[k, c, p] = new[:NY]
    lane = lanes((8, NZ))
    group, offset = lane // STEP, lane % STEP
    valid = (group < 2) & (((offset >= 4) & (offset < 8)) | ((offset >= 20) & (offset < 24)))
    for c in range(3):
        total = [jnp.zeros((8, NZ), jnp.float32) for _ in range(MOMENTS)]
        for p in range(GROUPS):
            for t in range(2):
                v = [powers[k, c, p, 8 * t : 8 * t + 8, :] for k in range(ITERS + 1)]
                total = [s + v[a] * v[b] for s, (a, b) in zip(total, pairs())]
        for k in range(MOMENTS):
            value = jnp.where(valid, total[k], 0.0) + sums[c, k]
            value = jnp.sum(jnp.sum(value, axis=0, keepdims=True), axis=1, keepdims=True)
            moments[3 * k + c : 3 * k + c + 1, :] = jnp.broadcast_to(value, (1, NZ))


def combine(weights, powers, edges, total, rest):
    lane = lanes((8, NZ))

    def mix(out, first, count, c, read):
        value = weights[first + c : first + c + 1, :] * read(0)
        for k in range(1, count):
            value = value + weights[first + 3 * k + c : first + 3 * k + c + 1, :] * read(k)
        return value

    for out, first, count in ((total, 0, ITERS), (rest, 3 * ITERS, ITERS + 1)):
        for c in range(3):
            for p in range(GROUPS):
                for t in range(2):
                    part = slice(8 * t, 8 * t + 8)
                    side = mix(out, first, count, c, lambda k: edges[k, c, p, part, :])
                    for g in range(2):
                        x = GROUPS * g + p
                        value = mix(out, first, count, c, lambda k: powers[k, c, x, part, :])
                        value = jnp.where(lane < HALO, turned(side, -(STEP * g + 4)), value)
                        value = jnp.where(lane >= NZ - HALO, turned(side, 104 - STEP * g), value)
                        out[c, x, part, :] = value


def kernel(body, outs, scratch=(), scalars=0):
    vmem = pl.BlockSpec(memory_space=pltpu.VMEM)
    smem = pl.BlockSpec(memory_space=pltpu.SMEM)

    def call(*args):
        return pl.pallas_call(
            body,
            in_specs=[smem] * scalars + [vmem] * (len(args) - scalars),
            out_specs=[vmem] * len(outs),
            out_shape=[jax.ShapeDtypeStruct(s, jnp.float32) for s in outs],
            scratch_shapes=[pltpu.VMEM(s, jnp.float32) for s in scratch],
            name=body.__name__,
        )(*args)

    return call


def exchanged(up, down, axis):
    size = lax.axis_size(axis)
    steps = [(i, i + 1) for i in range(size - 1)]
    return lax.ppermute(up, axis, steps), lax.ppermute(down, axis, [(b, a) for a, b in steps])


def gathered_sum(value, axes):
    count = lax.axis_size(axes)
    spread = jnp.broadcast_to(value[None], (count,) + value.shape)
    return jnp.sum(lax.all_to_all(spread, axes, 0, 0, tiled=True), axis=0)


def weights_of(moments, coefficient):
    scale = 6.0 * coefficient

    def inner(first, second):
        return sum(f * s * moments[i + j] for i, f in enumerate(first) for j, s in enumerate(second))

    def plus(first, factor, second):
        size = max(len(first), len(second))
        padded = [list(v) + [0.0] * (size - len(v)) for v in (first, second)]
        return [f + factor * s for f, s in zip(*padded)]

    one = jnp.ones_like(coefficient)
    total, residual, direction = [], [one], [one]
    now = moments[0]
    for iteration in range(ITERS):
        image = plus(direction, scale, [0.0] + direction)
        step = now / inner(direction, image)
        total = plus(total, step, direction)
        residual = plus(residual, -step, image)
        if iteration + 1 < ITERS:
            new = inner(residual, residual)
            direction = plus(residual, new / now, direction)
            now = new
    return total, residual


def body(velocity, diffusion):
    place = jnp.stack([f(a) - k for a in (GX, GY, GZ) for f, k in ((lax.axis_index, 0), (lax.axis_size, 1))])
    block = (3, NX, NY, NZ)
    below, above = exchanged(velocity[:, NX - HALO :], velocity[:, :HALO], GX)
    up, down = kernel(pack_y, [(3, 8, 8, NZ)] * 2)(velocity, below, above)
    low, high = exchanged(up, down, GY)
    wide = (3, EX, EY, NZ)
    tiles = (3, GROUPS, EY, NZ)
    whole, up, down = kernel(pack_z, [wide, (3, EY, NZ), (3, EY, NZ)])(velocity, below, above, low, high)
    low, high = exchanged(up, down, GZ)
    powers, sums, edge = kernel(
        inner_lanes, [(ITERS + 1,) + block, (3, MOMENTS, 8, NZ), tiles], [wide] * ITERS, 1
    )(place, whole)
    edges, moments = kernel(
        edge_lanes, [(ITERS + 1, 3, GROUPS, NY, NZ), (3 * MOMENTS, NZ)], [tiles] * (ITERS + 1), 1
    )(place, edge, low, high, sums)
    moments = gathered_sum(gathered_sum(moments[:, 0], GX + GY), GZ)
    moments = [moments[3 * k : 3 * k + 3] for k in range(MOMENTS)]
    total, rest = weights_of(moments, diffusion)
    weights = jnp.broadcast_to(jnp.concatenate(total + rest)[:, None], (3 * (2 * ITERS + 1), NZ))
    total, rest = kernel(combine, [block] * 2)(weights, powers, edges)
    return total, rest


def solution(mesh):
    finer = Mesh(
        mesh.devices.reshape(2, 2, 4, 4, mesh.shape["gz"]), ("gx_0", "gx_1", "gy_0", "gy_1", "gz")
    )
    return jax.shard_map(
        body,
        mesh=finer,
        in_specs=(P(None, GX, GY, "gz"), P()),
        out_specs=(P(None, GX, GY, "gz"), P(None, GX, GY, "gz")),
        check_vma=False,
    )
```

```python
import functools

import jax
import jax.numpy as jnp
from jax import lax
from jax.experimental import pallas as pl
from jax.experimental.pallas import tpu as pltpu
from jax.sharding import Mesh
from jax.sharding import PartitionSpec as P

ITERS = 3
GX = ("gx_0", "gx_1")
GY = ("gy_0", "gy_1")
GZ = ("gz",)
HALO = ITERS + 1

time_step = 0.25

NX, NY, NZ = 8, 16, 128
EX, EY = NX + 2 * HALO, NY + 2 * HALO
GROUPS = 4
STEP = NZ // GROUPS
MOMENTS = 2 * ITERS


def lanes(shape):
    return lax.broadcasted_iota(jnp.int32, shape, len(shape) - 1)


def rows(shape):
    return lax.broadcasted_iota(jnp.int32, shape, len(shape) - 2)


def back(value, axis):
    return pltpu.roll(value, value.shape[axis] - 1, axis)


def ahead(value, axis):
    return pltpu.roll(value, 1, axis)


def turned(value, shift):
    shift = shift % value.shape[-1]
    return pltpu.roll(value, shift, value.ndim - 1) if shift else value


def pack_y(block, own, up, down):
    own[...] = block[...]
    for c in range(3):
        for q in range(4):
            up[c, q, 4:8, :] = block[c, q, NY - HALO : NY, :]
            up[c, q, 0:4, :] = block[c, q + 4, NY - HALO : NY, :]
            down[c, q, 0:4, :] = block[c, q, 0:HALO, :]
            down[c, q, 4:8, :] = block[c, q + 4, 0:HALO, :]


def beside_y(low, high, c, x):
    sub = rows((8, NZ))
    if x < 4:
        return jnp.where(sub < 4, high[c, x], low[c, x])
    return pltpu.roll(jnp.where(sub < 4, low[c, x - 4], high[c, x - 4]), 4, 0)


def pack_x(own, low, high, up, down):
    for c in range(3):
        for n in range(HALO):
            for t in range(2):
                up[c, 2 * n + t] = own[c, NX - HALO + n, 8 * t : 8 * t + 8, :]
                down[c, 2 * n + t] = own[c, n, 8 * t : 8 * t + 8, :]
        for n in range(HALO - 1):
            up[c, 8 + n] = beside_y(low, high, c, NX - HALO + 1 + n)
            down[c, 8 + n] = beside_y(low, high, c, n)


def pack_z(own, low, high, below, above, whole, up, down):
    lane = lanes((8, NZ))
    zero = jnp.zeros((8, NZ), jnp.float32)

    def tile_of(c, i, t):
        if i < NX:
            return own[c, i, 8 * t : 8 * t + 8, :] if t < 2 else beside_y(low, high, c, i)
        n = i - NX
        if n < HALO:
            return above[c, 2 * n + t] if t < 2 else (above[c, 8 + n] if n < HALO - 1 else zero)
        n -= HALO
        return below[c, 2 * n + t] if t < 2 else (below[c, 7 + n] if n > 0 else zero)

    for c in range(3):
        for t in range(3):
            ups, downs = zero, zero
            for i in range(EX):
                tile = tile_of(c, i, t)
                whole[c, i, 8 * t : 8 * t + 8, :] = tile
                place = STEP * (i // 4) + 4 * (i % 4)
                here = (lane >= place) & (lane < place + 4)
                ups = jnp.where(here, turned(tile, place - (NZ - HALO)), ups)
                downs = jnp.where(here, turned(tile, place), downs)
            up[c, 8 * t : 8 * t + 8, :] = ups
            down[c, 8 * t : 8 * t + 8, :] = downs


def two_sum(a, b):
    total = a + b
    part = total - a
    return total, (a - (total - part)) + (b - part)


def split(a):
    large = a * 4097.0
    high = large - (large - a)
    return high, a - high


def two_product(a, b):
    total = a * b
    (ah, al), (bh, bl) = split(a), split(b)
    return total, ((ah * bh - total) + ah * bl + al * bh) + al * bl


def added(first, second):
    total, rest = two_sum(first[0], second[0])
    return total, (first[1] + second[1]) + rest


def rolled(value, shift, axis):
    return tuple(pltpu.roll(v, shift, axis) for v in value)


def chosen(where, first, second):
    return tuple(jnp.where(where, f, s) for f, s in zip(first, second))


def lane_totals(values):
    row, lane = rows((8, NZ)), lanes((8, NZ))
    reverse = (row % 2) * 4 + (row // 2 % 2) * 2 + row // 4
    zero = jnp.zeros((8, NZ), jnp.float32)
    found = zero
    for g in range(0, len(values), 8):
        group = values[g : g + 8]
        group = group + [(zero, zero)] * (8 - len(group))
        for half in (4, 2, 1):
            early = row % (2 * half) < half
            group = [
                added(
                    chosen(early, first, rolled(second, half, 0)),
                    chosen(early, rolled(first, 8 - half, 0), second),
                )
                for first, second in zip(group[::2], group[1::2])
            ]
        total = group[0]
        for half in (64, 32, 16, 8, 4, 2, 1):
            total = added(total, rolled(total, half, 1))
        total = two_sum(*total)
        found = jnp.where(lane == g + reverse, total[0], found)
        found = jnp.where(lane == 64 + g + reverse, total[1], found)
    return jnp.sum(found, axis=0, keepdims=True)


def folded(read, count):
    tiles = []
    for first in range(0, count, 8):
        size = min(8, count - first)
        tile = read(first, size)
        if size < 8:
            tile = jnp.concatenate([tile, jnp.zeros((8 - size, NZ), jnp.float32)], axis=0)
        tiles.append((tile, turned(tile, 64)))
    while len(tiles) > 1:
        tiles = [added(f, s) for f, s in zip(tiles[::2], tiles[1::2])] + tiles[len(tiles) // 2 * 2 :]
    total = tiles[0]
    for half in (4, 2, 1):
        total = added(total, rolled(total, half, 0))
    return two_sum(*total)


def fold(parts, out):
    high, rest = folded(lambda first, size: parts[first : first + size, :], parts.shape[0])
    row = jnp.where(lanes((8, NZ)) < 64, high, turned(rest, 64))[0:1]
    out[...] = jnp.broadcast_to(row, out.shape)


def section_of(at, here, before, after):
    result = []
    for c in range(3):
        slope = after[c] - before[c]
        flux = at[1] * at[c]
        slope = slope + (back(flux, 0) - ahead(flux, 0))
        flux = at[2] * at[c]
        slope = slope + (back(flux, 1) - ahead(flux, 1))
        result.append((at[c] - (0.5 * time_step) * slope) * here)
    return result


def laplace_of(at, before, after):
    beside = (before + after) + (back(at, 0) + ahead(at, 0))
    beside = beside + (back(at, 1) + ahead(at, 1))
    return at - beside * (1.0 / 6.0)


def pairs():
    return [(k // 2, (k + 1) // 2) for k in range(MOMENTS)]


def inner_lanes(flags, whole, powers, sums, edge, *work):
    row = rows((EY, NZ))
    in_y = jnp.where(row < NY, 1.0, jnp.where(row < NY + HALO, flags[3:4, :], flags[2:3, :]))
    below_x, above_x = in_y * flags[0:1, :], in_y * flags[1:2, :]

    def inside(x):
        return below_x if x < 0 else (above_x if x >= NX else in_y)

    def plane(x):
        return [whole[c, x % EX] for c in range(3)]

    def products(value):
        return [value[0] * value[c] for c in range(3)]

    lane = lanes((8, NZ))
    for c in range(3):
        for p in range(GROUPS):
            for t in range(3):
                part = slice(8 * t, 8 * t + 8)
                tile = jnp.zeros((8, NZ), jnp.float32)
                for g in range(GROUPS):
                    source = whole[c, GROUPS * g + p, part, :]
                    first = STEP * g + 4
                    tile = jnp.where((lane >= first) & (lane < first + 8), turned(source, first), tile)
                    first = STEP * g + 16
                    tile = jnp.where((lane >= first) & (lane < first + 8), turned(source, first - 120), tile)
                edge[c, p, part, :] = tile

    for x in range(-ITERS, NX + ITERS):
        new = section_of(plane(x), inside(x), products(plane(x - 1)), products(plane(x + 1)))
        for c in range(3):
            work[0][c, x % EX] = new[c]
            if 0 <= x < NX:
                powers[0, c, x] = new[c][:NY]
    for k in range(1, ITERS + 1):
        reach = ITERS - k
        for x in range(-reach, NX + reach):
            for c in range(3):
                source = work[k - 1]
                new = laplace_of(source[c, x % EX], source[c, (x - 1) % EX], source[c, (x + 1) % EX])
                if k < ITERS:
                    new = new * inside(x)
                    work[k][c, x % EX] = new
                if 0 <= x < NX:
                    powers[k, c, x] = new[:NY]
    valid = (lane >= HALO) & (lane < NZ - HALO)
    zero = jnp.zeros((8, NZ), jnp.float32)
    for c in range(3):
        total = [(zero, zero)] * MOMENTS
        for x in range(NX):
            for t in range(2):
                v = [powers[k, c, x, 8 * t : 8 * t + 8, :] for k in range(ITERS + 1)]
                total = [added(s, (v[a] * v[b], zero)) for s, (a, b) in zip(total, pairs())]
        for k in range(MOMENTS):
            for part in range(2):
                sums[c, k, part] = jnp.where(valid, total[k][part], 0.0)


def edge_lanes(flags, edge, low, high, sums, powers, moments, whole, *work):
    row = rows((EY, NZ))
    lane = lanes((EY, NZ))
    group, offset = lane // STEP, lane % STEP
    inside = jnp.where(row >= NY + HALO, flags[2:3, :], jnp.where(row >= NY, flags[3:4, :], 1.0))
    inside *= jnp.where(group == 3, flags[0:1, :], jnp.where(group == 2, flags[1:2, :], 1.0))
    inside *= jnp.where(offset < 4, flags[4:5, :], jnp.where(offset >= 24, flags[5:6, :], 1.0))
    for c in range(3):
        for p in range(GROUPS):
            value = jnp.where(offset < 4, turned(low[c], -4 * p), edge[c, p])
            whole[c, p] = jnp.where((offset >= 24) & (offset < 28), turned(high[c], 24 - 4 * p), value)

    def beyond(read, p):
        return turned(read(0), -STEP) if p == GROUPS - 1 else read(p + 1)

    def behind(read, p):
        return turned(read(GROUPS - 1), STEP) if p == 0 else read(p - 1)

    for p in range(GROUPS):
        at = [whole[c, p] for c in range(3)]
        before, after = (
            [side(lambda q, c=c: whole[0, q] * whole[c, q], p) for c in range(3)] for side in (behind, beyond)
        )
        new = section_of(at, inside, before, after)
        for c in range(3):
            work[0][c, p] = new[c]
            powers[0, c, p] = new[c][:NY]
    for k in range(1, ITERS + 1):
        for p in range(GROUPS):
            for c in range(3):
                read = functools.partial(lambda c, q: work[k - 1][c, q], c)
                new = laplace_of(read(p), behind(read, p), beyond(read, p))
                if k < ITERS:
                    new = new * inside
                    work[k][c, p] = new
                powers[k, c, p] = new[:NY]
    lane = lanes((8, NZ))
    group, offset = lane // STEP, lane % STEP
    valid = (group < 2) & (((offset >= 4) & (offset < 8)) | ((offset >= 20) & (offset < 24)))
    zero = jnp.zeros((8, NZ), jnp.float32)
    totals = []
    for k in range(MOMENTS):
        a, b = pairs()[k]
        for c in range(3):
            total = (sums[c, k, 0], sums[c, k, 1])
            for p in range(GROUPS):
                for t in range(2):
                    part = slice(8 * t, 8 * t + 8)
                    value = powers[a, c, p, part, :] * powers[b, c, p, part, :]
                    total = added(total, (jnp.where(valid, value, 0.0), zero))
            totals.append(total)
    moments[...] = jnp.broadcast_to(lane_totals(totals), moments.shape)


def weights_of(moments, scale):
    middle = moments[1][0] / moments[0][0]
    moments = list(moments)
    for r in range(1, MOMENTS):
        for k in range(MOMENTS - 1, r - 1, -1):
            total, rest = two_product(middle, moments[k - 1][0])
            rest = rest + middle * moments[k - 1][1]
            moments[k] = two_sum(*added(moments[k], (-total, -rest)))
    moments = [m[0] for m in moments]
    diagonal = 1.0 + scale * middle

    def inner(first, second):
        return sum(f * s * moments[i + j] for i, f in enumerate(first) for j, s in enumerate(second))

    def plus(first, factor, second):
        size = max(len(first), len(second))
        padded = [list(v) + [0.0] * (size - len(v)) for v in (first, second)]
        return [f + factor * s for f, s in zip(*padded)]

    def in_powers_of_l(weights):
        weights = list(weights)
        for r in range(len(weights) - 1):
            for k in range(len(weights) - 2, r - 1, -1):
                weights[k] = weights[k] - middle * weights[k + 1]
        return weights

    one = jnp.ones_like(scale)
    total, residual, direction = [], [one], [one]
    now = moments[0]
    for iteration in range(ITERS):
        image = plus([diagonal * d for d in direction], scale, [0.0] + direction)
        step = now / inner(direction, image)
        total = plus(total, step, direction)
        residual = plus(residual, -step, image)
        if iteration + 1 < ITERS:
            new = inner(residual, residual)
            direction = plus(residual, new / now, direction)
            now = new
    return in_powers_of_l(total), in_powers_of_l(residual)


def combine(parts, scale, powers, edges, total, rest):
    lane = lanes((8, NZ))
    high, low = folded(lambda first, size: parts[first : first + size, :], parts.shape[0])
    moments = [(turned(high, -3 * k), turned(low, -3 * k)) for k in range(MOMENTS)]

    def spread(value, c):
        return jnp.broadcast_to(jnp.sum(jnp.where(lane == c, value, 0.0), axis=1, keepdims=True), (8, NZ))

    for out, weights in zip((total, rest), weights_of(moments, jnp.broadcast_to(scale[0:1, :], (8, NZ)))):
        for c in range(3):
            factors = [spread(w, c) for w in weights]

            def mix(read):
                return sum(f * read(k) for k, f in enumerate(factors))

            for p in range(GROUPS):
                for t in range(2):
                    part = slice(8 * t, 8 * t + 8)
                    side = mix(lambda k: edges[k, c, p, part, :])
                    for g in range(2):
                        x = GROUPS * g + p
                        value = mix(lambda k: powers[k, c, x, part, :])
                        value = jnp.where(lane < HALO, turned(side, -(STEP * g + 4)), value)
                        value = jnp.where(lane >= NZ - HALO, turned(side, 104 - STEP * g), value)
                        out[c, x, part, :] = value


def kernel(body, outs, scratch=(), whole_array=False):
    vmem = pl.BlockSpec(memory_space=pltpu.VMEM)
    shape = jax.ShapeDtypeStruct if whole_array else pltpu.VMEM

    def call(*args):
        return pl.pallas_call(
            body,
            in_specs=[vmem] * len(args),
            out_specs=[vmem] * len(outs),
            out_shape=[shape(s, jnp.float32) for s in outs],
            scratch_shapes=[pltpu.VMEM(s, jnp.float32) for s in scratch],
            name=body.__name__,
        )(*args)

    return call


def held(value):
    return pltpu.with_memory_space_constraint(value, pltpu.VMEM)


def exchanged(up, down, axis):
    size = lax.axis_size(axis)
    steps = [(i, i + 1) for i in range(size - 1)]
    return lax.ppermute(up, axis, steps), lax.ppermute(down, axis, [(b, a) for a, b in steps])


def gathered(row, axes):
    return lax.all_to_all(row, axes, 0, 0, tiled=True)


def body(velocity, diffusion):
    ends = [f for a in (GX, GY, GZ) for f in (lax.axis_index(a) > 0, lax.axis_index(a) + 1 < lax.axis_size(a))]
    flags = jnp.broadcast_to(jnp.stack(ends + ends[:2]).astype(jnp.float32)[:, None], (8, NZ))
    scale = jnp.broadcast_to(jnp.pad(6.0 * diffusion, (0, NZ - 3))[None], (8, NZ))
    block, wide, tiles = (3, NX, NY, NZ), (3, EX, EY, NZ), (3, GROUPS, EY, NZ)
    flags, scale = held(flags), held(scale)
    own, up, down = kernel(pack_y, [block] + [(3, 4, 8, NZ)] * 2)(velocity)
    low, high = map(held, exchanged(up, down, GY))
    up, down = kernel(pack_x, [(3, 11, 8, NZ)] * 2)(own, low, high)
    below, above = map(held, exchanged(up, down, GX))
    whole, up, down = kernel(pack_z, [wide, (3, EY, NZ), (3, EY, NZ)])(own, low, high, below, above)
    low, high = map(held, exchanged(up, down, GZ))
    powers, sums, edge = kernel(
        inner_lanes, [(ITERS + 1,) + block, (3, MOMENTS, 2, 8, NZ), tiles], [wide] * ITERS
    )(flags, whole)
    planes, stack = lax.axis_size(GX + GY), lax.axis_size(GZ)
    edges, row = kernel(
        edge_lanes, [(ITERS + 1, 3, GROUPS, NY, NZ), (planes, NZ)], [tiles] * (ITERS + 1)
    )(flags, edge, low, high, sums)
    (row,) = kernel(fold, [(stack, NZ)])(held(gathered(row, GX + GY)))
    return kernel(combine, [block] * 2, whole_array=True)(held(gathered(row, GZ)), scale, powers, edges)


def solution(mesh):
    finer = Mesh(
        mesh.devices.reshape(2, 2, 4, 4, mesh.shape["gz"]), ("gx_0", "gx_1", "gy_0", "gy_1", "gz")
    )
    return jax.shard_map(
        body,
        mesh=finer,
        in_specs=(P(None, GX, GY, "gz"), P()),
        out_specs=(P(None, GX, GY, "gz"), P(None, GX, GY, "gz")),
        check_vma=False,
    )
```

```python
import functools

import jax
import jax.numpy as jnp
from jax import lax
from jax.experimental import pallas as pl
from jax.experimental.pallas import tpu as pltpu
from jax.sharding import Mesh
from jax.sharding import PartitionSpec as P

ITERS = 3
GX = ("gx_0", "gx_1")
GY = ("gy_0", "gy_1")
GZ = ("gz",)
HALO = ITERS + 1

time_step = 0.25

NX, NY, NZ = 8, 16, 128
EX, EY = NX + 2 * HALO, NY + 2 * HALO
GROUPS = 4
STEP = NZ // GROUPS
MOMENTS = 2 * ITERS


def lanes(shape):
    return lax.broadcasted_iota(jnp.int32, shape, len(shape) - 1)


def rows(shape):
    return lax.broadcasted_iota(jnp.int32, shape, len(shape) - 2)


def back(value, axis):
    return pltpu.roll(value, value.shape[axis] - 1, axis)


def ahead(value, axis):
    return pltpu.roll(value, 1, axis)


def turned(value, shift):
    shift = shift % value.shape[-1]
    return pltpu.roll(value, shift, value.ndim - 1) if shift else value


def pack_y(block, own, up, down):
    own[...] = block[...]
    for c in range(3):
        for q in range(4):
            up[c, q, 4:8, :] = block[c, q, NY - HALO : NY, :]
            up[c, q, 0:4, :] = block[c, q + 4, NY - HALO : NY, :]
            down[c, q, 0:4, :] = block[c, q, 0:HALO, :]
            down[c, q, 4:8, :] = block[c, q + 4, 0:HALO, :]


def beside_y(low, high, c, x):
    sub = rows((8, NZ))
    if x < 4:
        return jnp.where(sub < 4, high[c, x], low[c, x])
    return pltpu.roll(jnp.where(sub < 4, low[c, x - 4], high[c, x - 4]), 4, 0)


def pack_x(own, low, high, up, down):
    for c in range(3):
        for n in range(HALO):
            for t in range(2):
                up[c, 2 * n + t] = own[c, NX - HALO + n, 8 * t : 8 * t + 8, :]
                down[c, 2 * n + t] = own[c, n, 8 * t : 8 * t + 8, :]
        for n in range(HALO - 1):
            up[c, 8 + n] = beside_y(low, high, c, NX - HALO + 1 + n)
            down[c, 8 + n] = beside_y(low, high, c, n)


def pack_z(own, low, high, below, above, whole, up, down):
    lane = lanes((8, NZ))
    zero = jnp.zeros((8, NZ), jnp.float32)

    def tile_of(c, i, t):
        if i < NX:
            return own[c, i, 8 * t : 8 * t + 8, :] if t < 2 else beside_y(low, high, c, i)
        n = i - NX
        if n < HALO:
            return above[c, 2 * n + t] if t < 2 else (above[c, 8 + n] if n < HALO - 1 else zero)
        n -= HALO
        return below[c, 2 * n + t] if t < 2 else (below[c, 7 + n] if n > 0 else zero)

    for c in range(3):
        for t in range(3):
            ups, downs = zero, zero
            for i in range(EX):
                tile = tile_of(c, i, t)
                whole[c, i, 8 * t : 8 * t + 8, :] = tile
                place = STEP * (i // 4) + 4 * (i % 4)
                here = (lane >= place) & (lane < place + 4)
                ups = jnp.where(here, turned(tile, place - (NZ - HALO)), ups)
                downs = jnp.where(here, turned(tile, place), downs)
            up[c, 8 * t : 8 * t + 8, :] = ups
            down[c, 8 * t : 8 * t + 8, :] = downs


def two_sum(a, b):
    total = a + b
    part = total - a
    return total, (a - (total - part)) + (b - part)


def split(a):
    large = a * 4097.0
    high = large - (large - a)
    return high, a - high


def two_product(a, b):
    total = a * b
    (ah, al), (bh, bl) = split(a), split(b)
    return total, ((ah * bh - total) + ah * bl + al * bh) + al * bl


def added(first, second):
    total, rest = two_sum(first[0], second[0])
    return total, (first[1] + second[1]) + rest


def rolled(value, shift, axis):
    return tuple(pltpu.roll(v, shift, axis) for v in value)


def chosen(where, first, second):
    return tuple(jnp.where(where, f, s) for f, s in zip(first, second))


def lane_totals(values):
    row, lane = rows((8, NZ)), lanes((8, NZ))
    reverse = (row % 2) * 4 + (row // 2 % 2) * 2 + row // 4
    zero = jnp.zeros((8, NZ), jnp.float32)
    found = zero
    for g in range(0, len(values), 8):
        group = values[g : g + 8]
        group = group + [(zero, zero)] * (8 - len(group))
        for half in (4, 2, 1):
            early = row % (2 * half) < half
            group = [
                added(
                    chosen(early, first, rolled(second, half, 0)),
                    chosen(early, rolled(first, 8 - half, 0), second),
                )
                for first, second in zip(group[::2], group[1::2])
            ]
        total = group[0]
        for half in (64, 32, 16, 8, 4, 2, 1):
            total = added(total, rolled(total, half, 1))
        total = two_sum(*total)
        found = jnp.where(lane == g + reverse, total[0], found)
        found = jnp.where(lane == 64 + g + reverse, total[1], found)
    return jnp.sum(found, axis=0, keepdims=True)


def folded(read, count):
    tiles = []
    for first in range(0, count, 8):
        size = min(8, count - first)
        tile = read(first, size)
        if size < 8:
            tile = jnp.concatenate([tile, jnp.zeros((8 - size, NZ), jnp.float32)], axis=0)
        tiles.append((tile, turned(tile, 64)))
    while len(tiles) > 1:
        tiles = [added(f, s) for f, s in zip(tiles[::2], tiles[1::2])] + tiles[len(tiles) // 2 * 2 :]
    total = tiles[0]
    for half in (4, 2, 1):
        total = added(total, rolled(total, half, 0))
    return two_sum(*total)


def fold(parts, out):
    high, rest = folded(lambda first, size: parts[first : first + size, :], parts.shape[0])
    row = jnp.where(lanes((8, NZ)) < 64, high, turned(rest, 64))[0:1]
    out[...] = jnp.broadcast_to(row, out.shape)


def section_of(at, here, before, after):
    result = []
    for c in range(3):
        slope = after[c] - before[c]
        flux = at[1] * at[c]
        slope = slope + (back(flux, 0) - ahead(flux, 0))
        flux = at[2] * at[c]
        slope = slope + (back(flux, 1) - ahead(flux, 1))
        result.append((at[c] - (0.5 * time_step) * slope) * here)
    return result


def laplace_of(at, before, after):
    beside = (before + after) + (back(at, 0) + ahead(at, 0))
    beside = beside + (back(at, 1) + ahead(at, 1))
    return at - beside * (1.0 / 6.0)


def pairs():
    return [(k // 2, (k + 1) // 2) for k in range(MOMENTS)]


def inner_lanes(flags, whole, powers, sums, edge, *work):
    row = rows((EY, NZ))
    in_y = jnp.where(row < NY, 1.0, jnp.where(row < NY + HALO, flags[3:4, :], flags[2:3, :]))
    below_x, above_x = in_y * flags[0:1, :], in_y * flags[1:2, :]

    def inside(x):
        return below_x if x < 0 else (above_x if x >= NX else in_y)

    def plane(x):
        return [whole[c, x % EX] for c in range(3)]

    def products(value):
        return [value[0] * value[c] for c in range(3)]

    lane = lanes((8, NZ))
    for c in range(3):
        for p in range(GROUPS):
            for t in range(3):
                part = slice(8 * t, 8 * t + 8)
                tile = jnp.zeros((8, NZ), jnp.float32)
                for g in range(GROUPS):
                    source = whole[c, GROUPS * g + p, part, :]
                    first = STEP * g + 4
                    tile = jnp.where((lane >= first) & (lane < first + 8), turned(source, first), tile)
                    first = STEP * g + 16
                    tile = jnp.where((lane >= first) & (lane < first + 8), turned(source, first - 120), tile)
                edge[c, p, part, :] = tile

    for x in range(-ITERS, NX + ITERS):
        new = section_of(plane(x), inside(x), products(plane(x - 1)), products(plane(x + 1)))
        for c in range(3):
            work[0][c, x % EX] = new[c]
            if 0 <= x < NX:
                powers[0, c, x] = new[c][:NY]
    for k in range(1, ITERS + 1):
        reach = ITERS - k
        for x in range(-reach, NX + reach):
            for c in range(3):
                source = work[k - 1]
                new = laplace_of(source[c, x % EX], source[c, (x - 1) % EX], source[c, (x + 1) % EX])
                if k < ITERS:
                    new = new * inside(x)
                    work[k][c, x % EX] = new
                if 0 <= x < NX:
                    powers[k, c, x] = new[:NY]
    valid = (lane >= HALO) & (lane < NZ - HALO)
    zero = jnp.zeros((8, NZ), jnp.float32)
    for c in range(3):
        total = [(zero, zero)] * MOMENTS
        for x in range(NX):
            for t in range(2):
                v = [powers[k, c, x, 8 * t : 8 * t + 8, :] for k in range(ITERS + 1)]
                total = [added(s, (v[a] * v[b], zero)) for s, (a, b) in zip(total, pairs())]
        for k in range(MOMENTS):
            for part in range(2):
                sums[c, k, part] = jnp.where(valid, total[k][part], 0.0)


def edge_lanes(flags, edge, low, high, sums, powers, moments, whole, *work):
    row = rows((EY, NZ))
    lane = lanes((EY, NZ))
    group, offset = lane // STEP, lane % STEP
    inside = jnp.where(row >= NY + HALO, flags[2:3, :], jnp.where(row >= NY, flags[3:4, :], 1.0))
    inside *= jnp.where(group == 3, flags[0:1, :], jnp.where(group == 2, flags[1:2, :], 1.0))
    inside *= jnp.where(offset < 4, flags[4:5, :], jnp.where(offset >= 24, flags[5:6, :], 1.0))
    for c in range(3):
        for p in range(GROUPS):
            value = jnp.where(offset < 4, turned(low[c], -4 * p), edge[c, p])
            whole[c, p] = jnp.where((offset >= 24) & (offset < 28), turned(high[c], 24 - 4 * p), value)

    def beyond(read, p):
        return turned(read(0), -STEP) if p == GROUPS - 1 else read(p + 1)

    def behind(read, p):
        return turned(read(GROUPS - 1), STEP) if p == 0 else read(p - 1)

    for p in range(GROUPS):
        at = [whole[c, p] for c in range(3)]
        before, after = (
            [side(lambda q, c=c: whole[0, q] * whole[c, q], p) for c in range(3)] for side in (behind, beyond)
        )
        new = section_of(at, inside, before, after)
        for c in range(3):
            work[0][c, p] = new[c]
            powers[0, c, p] = new[c][:NY]
    for k in range(1, ITERS + 1):
        for p in range(GROUPS):
            for c in range(3):
                read = functools.partial(lambda c, q: work[k - 1][c, q], c)
                new = laplace_of(read(p), behind(read, p), beyond(read, p))
                if k < ITERS:
                    new = new * inside
                    work[k][c, p] = new
                powers[k, c, p] = new[:NY]
    lane = lanes((8, NZ))
    group, offset = lane // STEP, lane % STEP
    valid = (group < 2) & (((offset >= 4) & (offset < 8)) | ((offset >= 20) & (offset < 24)))
    zero = jnp.zeros((8, NZ), jnp.float32)
    totals = []
    for k in range(MOMENTS):
        a, b = pairs()[k]
        for c in range(3):
            total = (sums[c, k, 0], sums[c, k, 1])
            for p in range(GROUPS):
                for t in range(2):
                    part = slice(8 * t, 8 * t + 8)
                    value = powers[a, c, p, part, :] * powers[b, c, p, part, :]
                    total = added(total, (jnp.where(valid, value, 0.0), zero))
            totals.append(total)
    moments[...] = jnp.broadcast_to(lane_totals(totals), moments.shape)


def weights_of(moments, scale):
    middle = moments[1][0] / moments[0][0]
    moments = list(moments)
    for r in range(1, MOMENTS):
        for k in range(MOMENTS - 1, r - 1, -1):
            total, rest = two_product(middle, moments[k - 1][0])
            rest = rest + middle * moments[k - 1][1]
            moments[k] = two_sum(*added(moments[k], (-total, -rest)))
    moments = [m[0] for m in moments]
    diagonal = 1.0 + scale * middle

    def inner(first, second):
        return sum(f * s * moments[i + j] for i, f in enumerate(first) for j, s in enumerate(second))

    def plus(first, factor, second):
        size = max(len(first), len(second))
        padded = [list(v) + [0.0] * (size - len(v)) for v in (first, second)]
        return [f + factor * s for f, s in zip(*padded)]

    def in_powers_of_l(weights):
        weights = list(weights)
        for r in range(len(weights) - 1):
            for k in range(len(weights) - 2, r - 1, -1):
                weights[k] = weights[k] - middle * weights[k + 1]
        return weights

    one = jnp.ones_like(scale)
    total, residual, direction = [], [one], [one]
    now = moments[0]
    for iteration in range(ITERS):
        image = plus([diagonal * d for d in direction], scale, [0.0] + direction)
        step = now / inner(direction, image)
        total = plus(total, step, direction)
        residual = plus(residual, -step, image)
        if iteration + 1 < ITERS:
            new = inner(residual, residual)
            direction = plus(residual, new / now, direction)
            now = new
    return in_powers_of_l(total), in_powers_of_l(residual)


def combine(parts, scale, powers, edges, total, rest):
    lane = lanes((8, NZ))
    high, low = folded(lambda first, size: parts[first : first + size, :], parts.shape[0])
    moments = [(turned(high, -3 * k), turned(low, -3 * k)) for k in range(MOMENTS)]

    def spread(value, c):
        return jnp.broadcast_to(jnp.sum(jnp.where(lane == c, value, 0.0), axis=1, keepdims=True), (8, NZ))

    for out, weights in zip((total, rest), weights_of(moments, jnp.broadcast_to(scale[0:1, :], (8, NZ)))):
        for c in range(3):
            factors = [spread(w, c) for w in weights]

            def mix(read):
                return sum(f * read(k) for k, f in enumerate(factors))

            for p in range(GROUPS):
                for t in range(2):
                    part = slice(8 * t, 8 * t + 8)
                    side = mix(lambda k: edges[k, c, p, part, :])
                    for g in range(2):
                        x = GROUPS * g + p
                        value = mix(lambda k: powers[k, c, x, part, :])
                        value = jnp.where(lane < HALO, turned(side, -(STEP * g + 4)), value)
                        value = jnp.where(lane >= NZ - HALO, turned(side, 104 - STEP * g), value)
                        out[c, x, part, :] = value


def kernel(body, outs, scratch=(), first=False, last=False):
    vmem = pl.BlockSpec(memory_space=pltpu.VMEM)
    shape = jax.ShapeDtypeStruct if last else pltpu.VMEM

    def call(*args):
        if not first:
            args = [pltpu.with_memory_space_constraint(a, pltpu.VMEM) for a in args]
        return pl.pallas_call(
            body,
            in_specs=[vmem] * len(args),
            out_specs=[vmem] * len(outs),
            out_shape=[shape(s, jnp.float32) for s in outs],
            scratch_shapes=[pltpu.VMEM(s, jnp.float32) for s in scratch],
            name=body.__name__,
        )(*args)

    return call


def exchanged(up, down, axis):
    size = lax.axis_size(axis)
    steps = [(i, i + 1) for i in range(size - 1)]
    return lax.ppermute(up, axis, steps), lax.ppermute(down, axis, [(b, a) for a, b in steps])


def gathered(row, axes):
    return lax.all_to_all(row, axes, 0, 0, tiled=True)


def body(velocity, diffusion):
    ends = [f for a in (GX, GY, GZ) for f in (lax.axis_index(a) > 0, lax.axis_index(a) + 1 < lax.axis_size(a))]
    flags = jnp.broadcast_to(jnp.stack(ends + ends[:2]).astype(jnp.float32)[:, None], (8, NZ))
    scale = jnp.broadcast_to(jnp.pad(6.0 * diffusion, (0, NZ - 3))[None], (8, NZ))
    block, wide, tiles = (3, NX, NY, NZ), (3, EX, EY, NZ), (3, GROUPS, EY, NZ)
    own, up, down = kernel(pack_y, [block] + [(3, 4, 8, NZ)] * 2, first=True)(velocity)
    low, high = exchanged(up, down, GY)
    up, down = kernel(pack_x, [(3, 11, 8, NZ)] * 2)(own, low, high)
    below, above = exchanged(up, down, GX)
    whole, up, down = kernel(pack_z, [wide, (3, EY, NZ), (3, EY, NZ)])(own, low, high, below, above)
    low, high = exchanged(up, down, GZ)
    powers, sums, edge = kernel(
        inner_lanes, [(ITERS + 1,) + block, (3, MOMENTS, 2, 8, NZ), tiles], [wide] * ITERS
    )(flags, whole)
    planes, stack = lax.axis_size(GX + GY), lax.axis_size(GZ)
    edges, row = kernel(
        edge_lanes, [(ITERS + 1, 3, GROUPS, NY, NZ), (planes, NZ)], [tiles] * (ITERS + 1)
    )(flags, edge, low, high, sums)
    (row,) = kernel(fold, [(stack, NZ)])(gathered(row, GX + GY))
    return kernel(combine, [block] * 2, last=True)(gathered(row, GZ), scale, powers, edges)


def solution(mesh):
    finer = Mesh(
        mesh.devices.reshape(2, 2, 4, 4, mesh.shape["gz"]), ("gx_0", "gx_1", "gy_0", "gy_1", "gz")
    )
    return jax.shard_map(
        body,
        mesh=finer,
        in_specs=(P(None, GX, GY, "gz"), P()),
        out_specs=(P(None, GX, GY, "gz"), P(None, GX, GY, "gz")),
        check_vma=False,
    )
```

```python
import functools

import jax
import jax.numpy as jnp
from jax import lax
from jax.experimental import pallas as pl
from jax.experimental.pallas import tpu as pltpu
from jax.sharding import Mesh
from jax.sharding import PartitionSpec as P

ITERS = 3
GX = ("gx_0", "gx_1")
GY = ("gy_0", "gy_1")
GZ = ("gz",)
HALO = ITERS + 1

time_step = 0.25

NX, NY, NZ = 8, 16, 128
EX, EY = NX + 2 * HALO, NY + 2 * HALO
GROUPS = 4
STEP = NZ // GROUPS
MOMENTS = 2 * ITERS


def lanes(shape):
    return lax.broadcasted_iota(jnp.int32, shape, len(shape) - 1)


def rows(shape):
    return lax.broadcasted_iota(jnp.int32, shape, len(shape) - 2)


def back(value, axis):
    return pltpu.roll(value, value.shape[axis] - 1, axis)


def ahead(value, axis):
    return pltpu.roll(value, 1, axis)


def turned(value, shift):
    shift = shift % value.shape[-1]
    return pltpu.roll(value, shift, value.ndim - 1) if shift else value


def is_odd(axes):
    return lax.axis_index(axes) % 2 == 1


def pack_y(block, own, first, second):
    odd = is_odd(GY)
    sub = rows((8, NZ))
    own[...] = block[...]
    for c in range(3):
        for q in range(4):
            up = jnp.where(sub >= 4, block[c, q, 8:16, :], pltpu.roll(block[c, q + 4, 8:16, :], 4, 0))
            down = jnp.where(sub < 4, block[c, q, 0:8, :], pltpu.roll(block[c, q + 4, 0:8, :], 4, 0))
            first[c, q] = jnp.where(odd, up, down)
            second[c, q] = jnp.where(odd, down, up)


def beside_y(odd, first, second, c, x):
    low = jnp.where(odd, second[c, x % 4], first[c, x % 4])
    high = jnp.where(odd, first[c, x % 4], second[c, x % 4])
    sub = rows((8, NZ))
    if x < 4:
        return jnp.where(sub < 4, high, low)
    return pltpu.roll(jnp.where(sub < 4, low, high), 4, 0)


def pack_x(own, low, high, first, second):
    odd_y, odd = is_odd(GY), is_odd(GX)

    def put(c, n, up, down):
        first[c, n] = jnp.where(odd, up, down)
        second[c, n] = jnp.where(odd, down, up)

    for c in range(3):
        for n in range(HALO):
            for t in range(2):
                part = slice(8 * t, 8 * t + 8)
                put(c, 2 * n + t, own[c, NX - HALO + n, part, :], own[c, n, part, :])
        for n in range(HALO - 1):
            put(
                c,
                8 + n,
                beside_y(odd_y, low, high, c, NX - HALO + 1 + n),
                beside_y(odd_y, low, high, c, n),
            )


def pack_z(own, first_y, second_y, first_x, second_x, whole, up, down):
    odd_y, odd = is_odd(GY), is_odd(GX)
    lane = lanes((8, NZ))
    zero = jnp.zeros((8, NZ), jnp.float32)

    def tile_of(c, i, t):
        if i < NX:
            return own[c, i, 8 * t : 8 * t + 8, :] if t < 2 else beside_y(odd_y, first_y, second_y, c, i)
        n = i - NX
        if n < HALO:
            if t == 2 and n == HALO - 1:
                return zero
            k = 2 * n + t if t < 2 else 8 + n
            return jnp.where(odd, first_x[c, k], second_x[c, k])
        n -= HALO
        if t == 2 and n == 0:
            return zero
        k = 2 * n + t if t < 2 else 7 + n
        return jnp.where(odd, second_x[c, k], first_x[c, k])

    for c in range(3):
        for t in range(3):
            ups, downs = zero, zero
            for i in range(EX):
                tile = tile_of(c, i, t)
                whole[c, i, 8 * t : 8 * t + 8, :] = tile
                place = STEP * (i // 4) + 4 * (i % 4)
                here = (lane >= place) & (lane < place + 4)
                ups = jnp.where(here, turned(tile, place - (NZ - HALO)), ups)
                downs = jnp.where(here, turned(tile, place), downs)
            up[c, 8 * t : 8 * t + 8, :] = ups
            down[c, 8 * t : 8 * t + 8, :] = downs


def two_sum(a, b):
    total = a + b
    part = total - a
    return total, (a - (total - part)) + (b - part)


def split(a):
    large = a * 4097.0
    high = large - (large - a)
    return high, a - high


def two_product(a, b):
    total = a * b
    (ah, al), (bh, bl) = split(a), split(b)
    return total, ((ah * bh - total) + ah * bl + al * bh) + al * bl


def added(first, second):
    total, rest = two_sum(first[0], second[0])
    return total, (first[1] + second[1]) + rest


def rolled(value, shift, axis):
    return tuple(pltpu.roll(v, shift, axis) for v in value)


def chosen(where, first, second):
    return tuple(jnp.where(where, f, s) for f, s in zip(first, second))


def lane_totals(values):
    row, lane = rows((8, NZ)), lanes((8, NZ))
    reverse = (row % 2) * 4 + (row // 2 % 2) * 2 + row // 4
    zero = jnp.zeros((8, NZ), jnp.float32)
    found = zero
    for g in range(0, len(values), 8):
        group = values[g : g + 8]
        group = group + [(zero, zero)] * (8 - len(group))
        for half in (4, 2, 1):
            early = row % (2 * half) < half
            group = [
                added(
                    chosen(early, first, rolled(second, half, 0)),
                    chosen(early, rolled(first, 8 - half, 0), second),
                )
                for first, second in zip(group[::2], group[1::2])
            ]
        total = group[0]
        for half in (64, 32, 16, 8, 4, 2, 1):
            total = added(total, rolled(total, half, 1))
        total = two_sum(*total)
        found = jnp.where(lane == g + reverse, total[0], found)
        found = jnp.where(lane == 64 + g + reverse, total[1], found)
    return jnp.sum(found, axis=0, keepdims=True)


def folded(read, count):
    tiles = []
    for first in range(0, count, 8):
        size = min(8, count - first)
        tile = read(first, size)
        if size < 8:
            tile = jnp.concatenate([tile, jnp.zeros((8 - size, NZ), jnp.float32)], axis=0)
        tiles.append((tile, turned(tile, 64)))
    while len(tiles) > 1:
        tiles = [added(f, s) for f, s in zip(tiles[::2], tiles[1::2])] + tiles[len(tiles) // 2 * 2 :]
    total = tiles[0]
    for half in (4, 2, 1):
        total = added(total, rolled(total, half, 0))
    return two_sum(*total)


def fold(parts, out):
    high, rest = folded(lambda first, size: parts[first : first + size, :], parts.shape[0])
    row = jnp.where(lanes((8, NZ)) < 64, high, turned(rest, 64))[0:1]
    out[...] = jnp.broadcast_to(row, out.shape)


def section_of(at, here, before, after):
    result = []
    for c in range(3):
        slope = after[c] - before[c]
        flux = at[1] * at[c]
        slope = slope + (back(flux, 0) - ahead(flux, 0))
        flux = at[2] * at[c]
        slope = slope + (back(flux, 1) - ahead(flux, 1))
        result.append((at[c] - (0.5 * time_step) * slope) * here)
    return result


def laplace_of(at, before, after):
    beside = (before + after) + (back(at, 0) + ahead(at, 0))
    beside = beside + (back(at, 1) + ahead(at, 1))
    return at - beside * (1.0 / 6.0)


def pairs():
    return [(k // 2, (k + 1) // 2) for k in range(MOMENTS)]


def inner_lanes(flags, whole, powers, sums, edge, *work):
    row = rows((EY, NZ))
    in_y = jnp.where(row < NY, 1.0, jnp.where(row < NY + HALO, flags[3:4, :], flags[2:3, :]))
    below_x, above_x = in_y * flags[0:1, :], in_y * flags[1:2, :]

    def inside(x):
        return below_x if x < 0 else (above_x if x >= NX else in_y)

    def plane(x):
        return [whole[c, x % EX] for c in range(3)]

    def products(value):
        return [value[0] * value[c] for c in range(3)]

    lane = lanes((8, NZ))
    for c in range(3):
        for p in range(GROUPS):
            for t in range(3):
                part = slice(8 * t, 8 * t + 8)
                tile = jnp.zeros((8, NZ), jnp.float32)
                for g in range(GROUPS):
                    source = whole[c, GROUPS * g + p, part, :]
                    first = STEP * g + 4
                    tile = jnp.where((lane >= first) & (lane < first + 8), turned(source, first), tile)
                    first = STEP * g + 16
                    tile = jnp.where((lane >= first) & (lane < first + 8), turned(source, first - 120), tile)
                edge[c, p, part, :] = tile

    for x in range(-ITERS, NX + ITERS):
        new = section_of(plane(x), inside(x), products(plane(x - 1)), products(plane(x + 1)))
        for c in range(3):
            work[0][c, x % EX] = new[c]
            if 0 <= x < NX:
                powers[0, c, x] = new[c][:NY]
    for k in range(1, ITERS + 1):
        reach = ITERS - k
        for x in range(-reach, NX + reach):
            for c in range(3):
                source = work[k - 1]
                new = laplace_of(source[c, x % EX], source[c, (x - 1) % EX], source[c, (x + 1) % EX])
                if k < ITERS:
                    new = new * inside(x)
                    work[k][c, x % EX] = new
                if 0 <= x < NX:
                    powers[k, c, x] = new[:NY]
    valid = (lane >= HALO) & (lane < NZ - HALO)
    zero = jnp.zeros((8, NZ), jnp.float32)
    for c in range(3):
        total = [(zero, zero)] * MOMENTS
        for x in range(NX):
            for t in range(2):
                v = [powers[k, c, x, 8 * t : 8 * t + 8, :] for k in range(ITERS + 1)]
                total = [added(s, (v[a] * v[b], zero)) for s, (a, b) in zip(total, pairs())]
        for k in range(MOMENTS):
            for part in range(2):
                sums[c, k, part] = jnp.where(valid, total[k][part], 0.0)


def edge_lanes(flags, edge, low, high, sums, powers, moments, whole, *work):
    row = rows((EY, NZ))
    lane = lanes((EY, NZ))
    group, offset = lane // STEP, lane % STEP
    inside = jnp.where(row >= NY + HALO, flags[2:3, :], jnp.where(row >= NY, flags[3:4, :], 1.0))
    inside *= jnp.where(group == 3, flags[0:1, :], jnp.where(group == 2, flags[1:2, :], 1.0))
    inside *= jnp.where(offset < 4, flags[4:5, :], jnp.where(offset >= 24, flags[5:6, :], 1.0))
    for c in range(3):
        for p in range(GROUPS):
            value = jnp.where(offset < 4, turned(low[c], -4 * p), edge[c, p])
            whole[c, p] = jnp.where((offset >= 24) & (offset < 28), turned(high[c], 24 - 4 * p), value)

    def beyond(read, p):
        return turned(read(0), -STEP) if p == GROUPS - 1 else read(p + 1)

    def behind(read, p):
        return turned(read(GROUPS - 1), STEP) if p == 0 else read(p - 1)

    for p in range(GROUPS):
        at = [whole[c, p] for c in range(3)]
        before, after = (
            [side(lambda q, c=c: whole[0, q] * whole[c, q], p) for c in range(3)] for side in (behind, beyond)
        )
        new = section_of(at, inside, before, after)
        for c in range(3):
            work[0][c, p] = new[c]
            powers[0, c, p] = new[c][:NY]
    for k in range(1, ITERS + 1):
        for p in range(GROUPS):
            for c in range(3):
                read = functools.partial(lambda c, q: work[k - 1][c, q], c)
                new = laplace_of(read(p), behind(read, p), beyond(read, p))
                if k < ITERS:
                    new = new * inside
                    work[k][c, p] = new
                powers[k, c, p] = new[:NY]
    lane = lanes((8, NZ))
    group, offset = lane // STEP, lane % STEP
    valid = (group < 2) & (((offset >= 4) & (offset < 8)) | ((offset >= 20) & (offset < 24)))
    zero = jnp.zeros((8, NZ), jnp.float32)
    totals = []
    for k in range(MOMENTS):
        a, b = pairs()[k]
        for c in range(3):
            total = (sums[c, k, 0], sums[c, k, 1])
            for p in range(GROUPS):
                for t in range(2):
                    part = slice(8 * t, 8 * t + 8)
                    value = powers[a, c, p, part, :] * powers[b, c, p, part, :]
                    total = added(total, (jnp.where(valid, value, 0.0), zero))
            totals.append(total)
    moments[...] = jnp.broadcast_to(lane_totals(totals), moments.shape)


def weights_of(moments, scale):
    middle = moments[1][0] / moments[0][0]
    moments = list(moments)
    for r in range(1, MOMENTS):
        for k in range(MOMENTS - 1, r - 1, -1):
            total, rest = two_product(middle, moments[k - 1][0])
            rest = rest + middle * moments[k - 1][1]
            moments[k] = two_sum(*added(moments[k], (-total, -rest)))
    moments = [m[0] for m in moments]
    diagonal = 1.0 + scale * middle

    def inner(first, second):
        return sum(f * s * moments[i + j] for i, f in enumerate(first) for j, s in enumerate(second))

    def plus(first, factor, second):
        size = max(len(first), len(second))
        padded = [list(v) + [0.0] * (size - len(v)) for v in (first, second)]
        return [f + factor * s for f, s in zip(*padded)]

    def in_powers_of_l(weights):
        weights = list(weights)
        for r in range(len(weights) - 1):
            for k in range(len(weights) - 2, r - 1, -1):
                weights[k] = weights[k] - middle * weights[k + 1]
        return weights

    one = jnp.ones_like(scale)
    total, residual, direction = [], [one], [one]
    now = moments[0]
    for iteration in range(ITERS):
        image = plus([diagonal * d for d in direction], scale, [0.0] + direction)
        step = now / inner(direction, image)
        total = plus(total, step, direction)
        residual = plus(residual, -step, image)
        if iteration + 1 < ITERS:
            new = inner(residual, residual)
            direction = plus(residual, new / now, direction)
            now = new
    return in_powers_of_l(total), in_powers_of_l(residual)


def combine(parts, flags, powers, edges, total, rest):
    lane = lanes((8, NZ))
    high, low = folded(lambda first, size: parts[first : first + size, :], parts.shape[0])
    moments = [(turned(high, -3 * k), turned(low, -3 * k)) for k in range(MOMENTS)]

    def spread(value, c):
        return jnp.broadcast_to(jnp.sum(jnp.where(lane == c, value, 0.0), axis=1, keepdims=True), (8, NZ))

    for out, weights in zip((total, rest), weights_of(moments, jnp.broadcast_to(flags[6:7, :], (8, NZ)))):
        for c in range(3):
            factors = [spread(w, c) for w in weights]

            def mix(read):
                return sum(f * read(k) for k, f in enumerate(factors))

            for p in range(GROUPS):
                for t in range(2):
                    part = slice(8 * t, 8 * t + 8)
                    side = mix(lambda k: edges[k, c, p, part, :])
                    for g in range(2):
                        x = GROUPS * g + p
                        value = mix(lambda k: powers[k, c, x, part, :])
                        value = jnp.where(lane < HALO, turned(side, -(STEP * g + 4)), value)
                        value = jnp.where(lane >= NZ - HALO, turned(side, 104 - STEP * g), value)
                        out[c, x, part, :] = value


def kernel(body, outs, scratch=(), first=False, last=False):
    vmem = pl.BlockSpec(memory_space=pltpu.VMEM)
    shape = jax.ShapeDtypeStruct if last else pltpu.VMEM

    def call(*args):
        if not first:
            args = [pltpu.with_memory_space_constraint(a, pltpu.VMEM) for a in args]
        return pl.pallas_call(
            body,
            in_specs=[vmem] * len(args),
            out_specs=[vmem] * len(outs),
            out_shape=[shape(s, jnp.float32) for s in outs],
            scratch_shapes=[pltpu.VMEM(s, jnp.float32) for s in scratch],
            name=body.__name__,
        )(*args)

    return call


def exchanged(up, down, axis):
    size = lax.axis_size(axis)
    steps = [(i, i + 1) for i in range(size - 1)]
    return lax.ppermute(up, axis, steps), lax.ppermute(down, axis, [(b, a) for a, b in steps])


def swapped(first, second, axis):
    size = lax.axis_size(axis)

    def pairs_from(start):
        up = [(i, i + 1) for i in range(start, size - 1, 2)]
        return up + [(b, a) for a, b in up]

    return lax.ppermute(first, axis, pairs_from(1)), lax.ppermute(second, axis, pairs_from(0))


def gathered(row, axes):
    return lax.all_to_all(row, axes, 0, 0, tiled=True)


def body(velocity, diffusion):
    ends = [f for a in (GX, GY, GZ) for f in (lax.axis_index(a) > 0, lax.axis_index(a) + 1 < lax.axis_size(a))]
    flags = jnp.broadcast_to(jnp.stack(ends).astype(jnp.float32)[:, None], (6, NZ))
    flags = jnp.concatenate([flags, jnp.broadcast_to(jnp.pad(6.0 * diffusion, (0, NZ - 3))[None], (2, NZ))])
    block, wide, tiles = (3, NX, NY, NZ), (3, EX, EY, NZ), (3, GROUPS, EY, NZ)
    own, up, down = kernel(pack_y, [block] + [(3, 4, 8, NZ)] * 2, first=True)(velocity)
    low, high = swapped(up, down, GY)
    up, down = kernel(pack_x, [(3, 11, 8, NZ)] * 2)(own, low, high)
    below, above = swapped(up, down, GX)
    whole, up, down = kernel(pack_z, [wide, (3, EY, NZ), (3, EY, NZ)])(own, low, high, below, above)
    low, high = exchanged(up, down, GZ)
    powers, sums, edge = kernel(
        inner_lanes, [(ITERS + 1,) + block, (3, MOMENTS, 2, 8, NZ), tiles], [wide] * ITERS
    )(flags, whole)
    planes, stack = lax.axis_size(GX + GY), lax.axis_size(GZ)
    edges, row = kernel(
        edge_lanes, [(ITERS + 1, 3, GROUPS, NY, NZ), (planes, NZ)], [tiles] * (ITERS + 1)
    )(flags, edge, low, high, sums)
    (row,) = kernel(fold, [(stack, NZ)])(gathered(row, GX + GY))
    return kernel(combine, [block] * 2, last=True)(gathered(row, GZ), flags, powers, edges)


def solution(mesh):
    finer = Mesh(
        mesh.devices.reshape(2, 2, 4, 4, mesh.shape["gz"]), ("gx_0", "gx_1", "gy_0", "gy_1", "gz")
    )
    return jax.shard_map(
        body,
        mesh=finer,
        in_specs=(P(None, GX, GY, "gz"), P()),
        out_specs=(P(None, GX, GY, "gz"), P(None, GX, GY, "gz")),
        check_vma=False,
    )
```

```python
import functools

import jax
import jax.numpy as jnp
from jax import lax
from jax.experimental import pallas as pl
from jax.experimental.pallas import tpu as pltpu
from jax.sharding import Mesh
from jax.sharding import PartitionSpec as P

ITERS = 3
GX = ("gx_0", "gx_1")
GY = ("gy_0", "gy_1")
GZ = ("gz",)
HALO = ITERS + 1

time_step = 0.25

NX, NY, NZ = 8, 16, 128
EX, EY = NX + 2 * HALO, NY + 2 * HALO
GROUPS = 4
STEP = NZ // GROUPS
MOMENTS = 2 * ITERS


def lanes(shape):
    return lax.broadcasted_iota(jnp.int32, shape, len(shape) - 1)


def rows(shape):
    return lax.broadcasted_iota(jnp.int32, shape, len(shape) - 2)


def back(value, axis):
    return pltpu.roll(value, value.shape[axis] - 1, axis)


def ahead(value, axis):
    return pltpu.roll(value, 1, axis)


def turned(value, shift):
    shift = shift % value.shape[-1]
    return pltpu.roll(value, shift, value.ndim - 1) if shift else value


def is_odd(axes):
    return lax.axis_index(axes) % 2 == 1


def pack_y(block, own, first, second):
    odd = is_odd(GY)
    sub = rows((8, NZ))
    own[...] = block[...]
    for c in range(3):
        for q in range(4):
            up = jnp.where(sub >= 4, block[c, q, 8:16, :], pltpu.roll(block[c, q + 4, 8:16, :], 4, 0))
            down = jnp.where(sub < 4, block[c, q, 0:8, :], pltpu.roll(block[c, q + 4, 0:8, :], 4, 0))
            first[c, q] = jnp.where(odd, up, down)
            second[c, q] = jnp.where(odd, down, up)


def beside_y(odd, first, second, c, x):
    low = jnp.where(odd, second[c, x % 4], first[c, x % 4])
    high = jnp.where(odd, first[c, x % 4], second[c, x % 4])
    sub = rows((8, NZ))
    if x < 4:
        return jnp.where(sub < 4, high, low)
    return pltpu.roll(jnp.where(sub < 4, low, high), 4, 0)


def pack_x(own, low, high, first, second):
    odd_y, odd = is_odd(GY), is_odd(GX)

    def put(c, n, up, down):
        first[c, n] = jnp.where(odd, up, down)
        second[c, n] = jnp.where(odd, down, up)

    for c in range(3):
        for n in range(HALO):
            for t in range(2):
                part = slice(8 * t, 8 * t + 8)
                put(c, 2 * n + t, own[c, NX - HALO + n, part, :], own[c, n, part, :])
        for n in range(HALO - 1):
            put(
                c,
                8 + n,
                beside_y(odd_y, low, high, c, NX - HALO + 1 + n),
                beside_y(odd_y, low, high, c, n),
            )


def pack_z(own, first_y, second_y, first_x, second_x, whole, up, down):
    odd_y, odd = is_odd(GY), is_odd(GX)
    lane = lanes((8, NZ))
    zero = jnp.zeros((8, NZ), jnp.float32)

    def tile_of(c, i, t):
        if i < NX:
            return own[c, i, 8 * t : 8 * t + 8, :] if t < 2 else beside_y(odd_y, first_y, second_y, c, i)
        n = i - NX
        if n < HALO:
            if t == 2 and n == HALO - 1:
                return zero
            k = 2 * n + t if t < 2 else 8 + n
            return jnp.where(odd, first_x[c, k], second_x[c, k])
        n -= HALO
        if t == 2 and n == 0:
            return zero
        k = 2 * n + t if t < 2 else 7 + n
        return jnp.where(odd, second_x[c, k], first_x[c, k])

    for c in range(3):
        for t in range(3):
            ups, downs = zero, zero
            for i in range(EX):
                tile = tile_of(c, i, t)
                whole[c, i, 8 * t : 8 * t + 8, :] = tile
                place = STEP * (i // 4) + 4 * (i % 4)
                here = (lane >= place) & (lane < place + 4)
                ups = jnp.where(here, turned(tile, place - (NZ - HALO)), ups)
                downs = jnp.where(here, turned(tile, place), downs)
            up[c, 8 * t : 8 * t + 8, :] = ups
            down[c, 8 * t : 8 * t + 8, :] = downs


def two_sum(a, b):
    total = a + b
    part = total - a
    return total, (a - (total - part)) + (b - part)


def split(a):
    large = a * 4097.0
    high = large - (large - a)
    return high, a - high


def two_product(a, b):
    total = a * b
    (ah, al), (bh, bl) = split(a), split(b)
    return total, ((ah * bh - total) + ah * bl + al * bh) + al * bl


def added(first, second):
    total, rest = two_sum(first[0], second[0])
    return total, (first[1] + second[1]) + rest


def rolled(value, shift, axis):
    return tuple(pltpu.roll(v, shift, axis) for v in value)


def chosen(where, first, second):
    return tuple(jnp.where(where, f, s) for f, s in zip(first, second))


def lane_totals(values):
    row, lane = rows((8, NZ)), lanes((8, NZ))
    reverse = (row % 2) * 4 + (row // 2 % 2) * 2 + row // 4
    zero = jnp.zeros((8, NZ), jnp.float32)
    found = zero
    for g in range(0, len(values), 8):
        group = values[g : g + 8]
        group = group + [(zero, zero)] * (8 - len(group))
        for half in (4, 2, 1):
            early = row % (2 * half) < half
            group = [
                added(
                    chosen(early, first, rolled(second, half, 0)),
                    chosen(early, rolled(first, 8 - half, 0), second),
                )
                for first, second in zip(group[::2], group[1::2])
            ]
        total = group[0]
        for half in (64, 32, 16, 8, 4, 2, 1):
            total = added(total, rolled(total, half, 1))
        total = two_sum(*total)
        found = jnp.where(lane == g + reverse, total[0], found)
        found = jnp.where(lane == 64 + g + reverse, total[1], found)
    return jnp.sum(found, axis=0, keepdims=True)


def folded(read, count):
    tiles = []
    for first in range(0, count, 8):
        size = min(8, count - first)
        tile = read(first, size)
        if size < 8:
            tile = jnp.concatenate([tile, jnp.zeros((8 - size, NZ), jnp.float32)], axis=0)
        tiles.append((tile, turned(tile, 64)))
    while len(tiles) > 1:
        tiles = [added(f, s) for f, s in zip(tiles[::2], tiles[1::2])] + tiles[len(tiles) // 2 * 2 :]
    total = tiles[0]
    for half in (4, 2, 1):
        total = added(total, rolled(total, half, 0))
    return two_sum(*total)


def fold(parts, out):
    high, rest = folded(lambda first, size: parts[first : first + size, :], parts.shape[0])
    row = jnp.where(lanes((8, NZ)) < 64, high, turned(rest, 64))[0:1]
    out[...] = jnp.broadcast_to(row, out.shape)


def section_of(at, here, before, after):
    result = []
    for c in range(3):
        slope = after[c] - before[c]
        flux = at[1] * at[c]
        slope = slope + (back(flux, 0) - ahead(flux, 0))
        flux = at[2] * at[c]
        slope = slope + (back(flux, 1) - ahead(flux, 1))
        result.append((at[c] - (0.5 * time_step) * slope) * here)
    return result


def laplace_of(at, before, after):
    beside = (before + after) + (back(at, 0) + ahead(at, 0))
    beside = beside + (back(at, 1) + ahead(at, 1))
    return at - beside * (1.0 / 6.0)


def pairs():
    return [(k // 2, (k + 1) // 2) for k in range(MOMENTS)]


def inner_lanes(flags, whole, powers, sums, edge, *work):
    row = rows((EY, NZ))
    in_y = jnp.where(row < NY, 1.0, jnp.where(row < NY + HALO, flags[3:4, :], flags[2:3, :]))
    below_x, above_x = in_y * flags[0:1, :], in_y * flags[1:2, :]

    def inside(x):
        return below_x if x < 0 else (above_x if x >= NX else in_y)

    def plane(x):
        return [whole[c, x % EX] for c in range(3)]

    def products(value):
        return [value[0] * value[c] for c in range(3)]

    lane = lanes((8, NZ))
    for c in range(3):
        for p in range(GROUPS):
            for t in range(3):
                part = slice(8 * t, 8 * t + 8)
                tile = jnp.zeros((8, NZ), jnp.float32)
                for g in range(GROUPS):
                    source = whole[c, GROUPS * g + p, part, :]
                    first = STEP * g + 4
                    tile = jnp.where((lane >= first) & (lane < first + 8), turned(source, first), tile)
                    first = STEP * g + 16
                    tile = jnp.where((lane >= first) & (lane < first + 8), turned(source, first - 120), tile)
                edge[c, p, part, :] = tile

    for x in range(-ITERS, NX + ITERS):
        new = section_of(plane(x), inside(x), products(plane(x - 1)), products(plane(x + 1)))
        for c in range(3):
            work[0][c, x % EX] = new[c]
            if 0 <= x < NX:
                powers[0, c, x] = new[c][:NY]
    for k in range(1, ITERS + 1):
        reach = ITERS - k
        for x in range(-reach, NX + reach):
            for c in range(3):
                source = work[k - 1]
                new = laplace_of(source[c, x % EX], source[c, (x - 1) % EX], source[c, (x + 1) % EX])
                if k < ITERS:
                    new = new * inside(x)
                    work[k][c, x % EX] = new
                if 0 <= x < NX:
                    powers[k, c, x] = new[:NY]
    valid = (lane >= HALO) & (lane < NZ - HALO)
    zero = jnp.zeros((8, NZ), jnp.float32)
    for c in range(3):
        total = [(zero, zero)] * MOMENTS
        for x in range(NX):
            for t in range(2):
                v = [powers[k, c, x, 8 * t : 8 * t + 8, :] for k in range(ITERS + 1)]
                total = [added(s, (v[a] * v[b], zero)) for s, (a, b) in zip(total, pairs())]
        for k in range(MOMENTS):
            for part in range(2):
                sums[c, k, part] = jnp.where(valid, total[k][part], 0.0)


def edge_lanes(flags, edge, low, high, sums, powers, moments, whole, *work):
    row = rows((EY, NZ))
    lane = lanes((EY, NZ))
    group, offset = lane // STEP, lane % STEP
    inside = jnp.where(row >= NY + HALO, flags[2:3, :], jnp.where(row >= NY, flags[3:4, :], 1.0))
    inside *= jnp.where(group == 3, flags[0:1, :], jnp.where(group == 2, flags[1:2, :], 1.0))
    inside *= jnp.where(offset < 4, flags[4:5, :], jnp.where(offset >= 24, flags[5:6, :], 1.0))
    for c in range(3):
        for p in range(GROUPS):
            value = jnp.where(offset < 4, turned(low[c], -4 * p), edge[c, p])
            whole[c, p] = jnp.where((offset >= 24) & (offset < 28), turned(high[c], 24 - 4 * p), value)

    def beyond(read, p):
        return turned(read(0), -STEP) if p == GROUPS - 1 else read(p + 1)

    def behind(read, p):
        return turned(read(GROUPS - 1), STEP) if p == 0 else read(p - 1)

    for p in range(GROUPS):
        at = [whole[c, p] for c in range(3)]
        before, after = (
            [side(lambda q, c=c: whole[0, q] * whole[c, q], p) for c in range(3)] for side in (behind, beyond)
        )
        new = section_of(at, inside, before, after)
        for c in range(3):
            work[0][c, p] = new[c]
            powers[0, c, p] = new[c][:NY]
    for k in range(1, ITERS + 1):
        for p in range(GROUPS):
            for c in range(3):
                read = functools.partial(lambda c, q: work[k - 1][c, q], c)
                new = laplace_of(read(p), behind(read, p), beyond(read, p))
                if k < ITERS:
                    new = new * inside
                    work[k][c, p] = new
                powers[k, c, p] = new[:NY]
    lane = lanes((8, NZ))
    group, offset = lane // STEP, lane % STEP
    valid = (group < 2) & (((offset >= 4) & (offset < 8)) | ((offset >= 20) & (offset < 24)))
    zero = jnp.zeros((8, NZ), jnp.float32)
    totals = []
    for k in range(MOMENTS):
        a, b = pairs()[k]
        for c in range(3):
            total = (sums[c, k, 0], sums[c, k, 1])
            for p in range(GROUPS):
                for t in range(2):
                    part = slice(8 * t, 8 * t + 8)
                    value = powers[a, c, p, part, :] * powers[b, c, p, part, :]
                    total = added(total, (jnp.where(valid, value, 0.0), zero))
            totals.append(total)
    moments[...] = jnp.broadcast_to(lane_totals(totals), moments.shape)


def weights_of(moments, scale):
    middle = moments[1][0] / moments[0][0]
    moments = list(moments)
    for r in range(1, MOMENTS):
        for k in range(MOMENTS - 1, r - 1, -1):
            total, rest = two_product(middle, moments[k - 1][0])
            rest = rest + middle * moments[k - 1][1]
            moments[k] = two_sum(*added(moments[k], (-total, -rest)))
    moments = [m[0] for m in moments]
    diagonal = 1.0 + scale * middle

    def inner(first, second):
        return sum(f * s * moments[i + j] for i, f in enumerate(first) for j, s in enumerate(second))

    def plus(first, factor, second):
        size = max(len(first), len(second))
        padded = [list(v) + [0.0] * (size - len(v)) for v in (first, second)]
        return [f + factor * s for f, s in zip(*padded)]

    def in_powers_of_l(weights):
        weights = list(weights)
        for r in range(len(weights) - 1):
            for k in range(len(weights) - 2, r - 1, -1):
                weights[k] = weights[k] - middle * weights[k + 1]
        return weights

    one = jnp.ones_like(scale)
    total, residual, direction = [], [one], [one]
    now = moments[0]
    for iteration in range(ITERS):
        image = plus([diagonal * d for d in direction], scale, [0.0] + direction)
        step = now / inner(direction, image)
        total = plus(total, step, direction)
        residual = plus(residual, -step, image)
        if iteration + 1 < ITERS:
            new = inner(residual, residual)
            direction = plus(residual, new / now, direction)
            now = new
    return in_powers_of_l(total), in_powers_of_l(residual)


def combine(parts, flags, powers, edges, total, rest):
    lane = lanes((8, NZ))
    high, low = folded(lambda first, size: parts[first : first + size, :], parts.shape[0])
    moments = [(turned(high, -3 * k), turned(low, -3 * k)) for k in range(MOMENTS)]

    def spread(value, c):
        return jnp.broadcast_to(jnp.sum(jnp.where(lane == c, value, 0.0), axis=1, keepdims=True), (8, NZ))

    for out, weights in zip((total, rest), weights_of(moments, jnp.broadcast_to(flags[6:7, :], (8, NZ)))):
        for c in range(3):
            factors = [spread(w, c) for w in weights]

            def mix(read):
                return sum(f * read(k) for k, f in enumerate(factors))

            for p in range(GROUPS):
                for t in range(2):
                    part = slice(8 * t, 8 * t + 8)
                    side = mix(lambda k: edges[k, c, p, part, :])
                    for g in range(2):
                        x = GROUPS * g + p
                        value = mix(lambda k: powers[k, c, x, part, :])
                        value = jnp.where(lane < HALO, turned(side, -(STEP * g + 4)), value)
                        value = jnp.where(lane >= NZ - HALO, turned(side, 104 - STEP * g), value)
                        out[c, x, part, :] = value


def kernel(body, outs, scratch=(), first=False, last=False):
    vmem = pl.BlockSpec(memory_space=pltpu.VMEM)
    shape = jax.ShapeDtypeStruct if last else pltpu.VMEM

    def call(*args):
        if not first:
            args = [pltpu.with_memory_space_constraint(a, pltpu.VMEM) for a in args]
        return pl.pallas_call(
            body,
            in_specs=[vmem] * len(args),
            out_specs=[vmem] * len(outs),
            out_shape=[shape(s, jnp.float32) for s in outs],
            scratch_shapes=[pltpu.VMEM(s, jnp.float32) for s in scratch],
            name=body.__name__,
        )(*args)

    return call


def exchanged(up, down, axis):
    size = lax.axis_size(axis)
    steps = [(i, i + 1) for i in range(size - 1)]
    return lax.ppermute(up, axis, steps), lax.ppermute(down, axis, [(b, a) for a, b in steps])


def swapped(first, second, axis):
    size = lax.axis_size(axis)

    def pairs_from(start):
        up = [(i, i + 1) for i in range(start, size - 1, 2)]
        return up + [(b, a) for a, b in up]

    return lax.ppermute(first, axis, pairs_from(1)), lax.ppermute(second, axis, pairs_from(0))


def gathered(row, axes):
    if row.shape[0] == 1:
        return lax.all_gather(row, axes, axis=0, tiled=True)
    return lax.all_to_all(row, axes, 0, 0, tiled=True)


def body(velocity, diffusion):
    ends = [f for a in (GX, GY, GZ) for f in (lax.axis_index(a) > 0, lax.axis_index(a) + 1 < lax.axis_size(a))]
    flags = jnp.broadcast_to(jnp.stack(ends).astype(jnp.float32)[:, None], (6, NZ))
    flags = jnp.concatenate([flags, jnp.broadcast_to(jnp.pad(6.0 * diffusion, (0, NZ - 3))[None], (2, NZ))])
    block, wide, tiles = (3, NX, NY, NZ), (3, EX, EY, NZ), (3, GROUPS, EY, NZ)
    own, up, down = kernel(pack_y, [block] + [(3, 4, 8, NZ)] * 2, first=True)(velocity)
    low, high = swapped(up, down, GY)
    up, down = kernel(pack_x, [(3, 11, 8, NZ)] * 2)(own, low, high)
    below, above = swapped(up, down, GX)
    whole, up, down = kernel(pack_z, [wide, (3, EY, NZ), (3, EY, NZ)])(own, low, high, below, above)
    low, high = exchanged(up, down, GZ)
    powers, sums, edge = kernel(
        inner_lanes, [(ITERS + 1,) + block, (3, MOMENTS, 2, 8, NZ), tiles], [wide] * ITERS
    )(flags, whole)
    planes = lax.axis_size(GX + GY)
    edges, row = kernel(
        edge_lanes, [(ITERS + 1, 3, GROUPS, NY, NZ), (planes, NZ)], [tiles] * (ITERS + 1)
    )(flags, edge, low, high, sums)
    (row,) = kernel(fold, [(1, NZ)])(gathered(row, GX + GY))
    return kernel(combine, [block] * 2, last=True)(gathered(row, GZ), flags, powers, edges)


def solution(mesh):
    finer = Mesh(
        mesh.devices.reshape(2, 2, 4, 4, mesh.shape["gz"]), ("gx_0", "gx_1", "gy_0", "gy_1", "gz")
    )
    return jax.shard_map(
        body,
        mesh=finer,
        in_specs=(P(None, GX, GY, "gz"), P()),
        out_specs=(P(None, GX, GY, "gz"), P(None, GX, GY, "gz")),
        check_vma=False,
    )
```

```python
import functools

import jax
import jax.numpy as jnp
from jax import lax
from jax.experimental import pallas as pl
from jax.experimental.pallas import tpu as pltpu
from jax.sharding import Mesh
from jax.sharding import PartitionSpec as P

ITERS = 3
GX = ("gx_0", "gx_1")
GY = ("gy_0", "gy_1")
GZ = ("gz",)
HALO = ITERS + 1

time_step = 0.25

NX, NY, NZ = 8, 16, 128
EX, EY = NX + 2 * HALO, NY + 2 * HALO
GROUPS = 4
STEP = NZ // GROUPS
MOMENTS = 2 * ITERS
Z_TILES = 5


def lanes(shape):
    return lax.broadcasted_iota(jnp.int32, shape, len(shape) - 1)


def rows(shape):
    return lax.broadcasted_iota(jnp.int32, shape, len(shape) - 2)


def back(value, axis):
    return pltpu.roll(value, value.shape[axis] - 1, axis)


def ahead(value, axis):
    return pltpu.roll(value, 1, axis)


def turned(value, shift):
    shift = shift % value.shape[-1]
    return pltpu.roll(value, shift, value.ndim - 1) if shift else value


def is_odd(axes):
    return lax.axis_index(axes) % 2 == 1


def pack_y(block, own, first, second):
    odd = is_odd(GY)
    sub = rows((8, NZ))
    own[...] = block[...]
    for c in range(3):
        for q in range(4):
            up = jnp.where(sub >= 4, block[c, q, 8:16, :], pltpu.roll(block[c, q + 4, 8:16, :], 4, 0))
            down = jnp.where(sub < 4, block[c, q, 0:8, :], pltpu.roll(block[c, q + 4, 0:8, :], 4, 0))
            first[c, q] = jnp.where(odd, up, down)
            second[c, q] = jnp.where(odd, down, up)


def beside_y(odd, first, second, c, x):
    low = jnp.where(odd, second[c, x % 4], first[c, x % 4])
    high = jnp.where(odd, first[c, x % 4], second[c, x % 4])
    sub = rows((8, NZ))
    if x < 4:
        return jnp.where(sub < 4, high, low)
    return pltpu.roll(jnp.where(sub < 4, low, high), 4, 0)


def pack_x(own, first_y, second_y, first, second):
    odd_y, odd = is_odd(GY), is_odd(GX)

    def put(c, n, up, down):
        first[c, n] = jnp.where(odd, up, down)
        second[c, n] = jnp.where(odd, down, up)

    for c in range(3):
        for n in range(HALO):
            for t in range(2):
                part = slice(8 * t, 8 * t + 8)
                put(c, 2 * n + t, own[c, NX - HALO + n, part, :], own[c, n, part, :])
        for n in range(HALO - 1):
            put(
                c,
                8 + n,
                beside_y(odd_y, first_y, second_y, c, NX - HALO + 1 + n),
                beside_y(odd_y, first_y, second_y, c, n),
            )


def pack_z(own, first_y, second_y, first_x, second_x, whole, first, second):
    odd_y, odd, odd_z = is_odd(GY), is_odd(GX), is_odd(GZ)
    lane = lanes((8, NZ))
    zero = jnp.zeros((8, NZ), jnp.float32)

    def tile_of(c, i, t):
        if i < NX:
            return own[c, i, 8 * t : 8 * t + 8, :] if t < 2 else beside_y(odd_y, first_y, second_y, c, i)
        n = i - NX
        if n < HALO:
            if t == 2 and n == HALO - 1:
                return zero
            k = 2 * n + t if t < 2 else 8 + n
            return jnp.where(odd, first_x[c, k], second_x[c, k])
        n -= HALO
        if t == 2 and n == 0:
            return zero
        k = 2 * n + t if t < 2 else 7 + n
        return jnp.where(odd, second_x[c, k], first_x[c, k])

    for k in range(Z_TILES):
        ups, downs = zero, zero
        for half in range(2):
            c, t = divmod(2 * k + half, 3)
            for i in range(EX if c < 3 else 0):
                tile = tile_of(c, i, t)
                whole[c, i, 8 * t : 8 * t + 8, :] = tile
                place = STEP * (i // 4) + 16 * half + 4 * (i % 4)
                here = (lane >= place) & (lane < place + 4)
                ups = jnp.where(here, turned(tile, place - (NZ - HALO)), ups)
                downs = jnp.where(here, turned(tile, place), downs)
        first[k] = jnp.where(odd_z, ups, downs)
        second[k] = jnp.where(odd_z, downs, ups)


def two_sum(a, b):
    total = a + b
    part = total - a
    return total, (a - (total - part)) + (b - part)


def split(a):
    large = a * 4097.0
    high = large - (large - a)
    return high, a - high


def two_product(a, b):
    total = a * b
    (ah, al), (bh, bl) = split(a), split(b)
    return total, ((ah * bh - total) + ah * bl + al * bh) + al * bl


def added(first, second):
    total, rest = two_sum(first[0], second[0])
    return total, (first[1] + second[1]) + rest


def rolled(value, shift, axis):
    return tuple(pltpu.roll(v, shift, axis) for v in value)


def chosen(where, first, second):
    return tuple(jnp.where(where, f, s) for f, s in zip(first, second))


def lane_totals(values):
    row, lane = rows((8, NZ)), lanes((8, NZ))
    reverse = (row % 2) * 4 + (row // 2 % 2) * 2 + row // 4
    zero = jnp.zeros((8, NZ), jnp.float32)
    found = zero
    for g in range(0, len(values), 8):
        group = values[g : g + 8]
        group = group + [(zero, zero)] * (8 - len(group))
        for half in (4, 2, 1):
            early = row % (2 * half) < half
            group = [
                added(
                    chosen(early, first, rolled(second, half, 0)),
                    chosen(early, rolled(first, 8 - half, 0), second),
                )
                for first, second in zip(group[::2], group[1::2])
            ]
        total = group[0]
        for half in (64, 32, 16, 8, 4, 2, 1):
            total = added(total, rolled(total, half, 1))
        total = two_sum(*total)
        found = jnp.where(lane == g + reverse, total[0], found)
        found = jnp.where(lane == 64 + g + reverse, total[1], found)
    return jnp.sum(found, axis=0, keepdims=True)


def folded(read, count):
    tiles = []
    for first in range(0, count, 8):
        size = min(8, count - first)
        tile = read(first, size)
        if size < 8:
            tile = jnp.concatenate([tile, jnp.zeros((8 - size, NZ), jnp.float32)], axis=0)
        tiles.append((tile, turned(tile, 64)))
    while len(tiles) > 1:
        tiles = [added(f, s) for f, s in zip(tiles[::2], tiles[1::2])] + tiles[len(tiles) // 2 * 2 :]
    total = tiles[0]
    for half in (4, 2, 1):
        total = added(total, rolled(total, half, 0))
    return two_sum(*total)


def fold(parts, out):
    high, rest = folded(lambda first, size: parts[first : first + size, :], parts.shape[0])
    row = jnp.where(lanes((8, NZ)) < 64, high, turned(rest, 64))[0:1]
    out[...] = jnp.broadcast_to(row, out.shape)


def section_of(at, here, before, after):
    result = []
    for c in range(3):
        slope = after[c] - before[c]
        flux = at[1] * at[c]
        slope = slope + (back(flux, 0) - ahead(flux, 0))
        flux = at[2] * at[c]
        slope = slope + (back(flux, 1) - ahead(flux, 1))
        result.append((at[c] - (0.5 * time_step) * slope) * here)
    return result


def laplace_of(at, before, after):
    beside = (before + after) + (back(at, 0) + ahead(at, 0))
    beside = beside + (back(at, 1) + ahead(at, 1))
    return at - beside * (1.0 / 6.0)


def pairs():
    return [(k // 2, (k + 1) // 2) for k in range(MOMENTS)]


def inner_lanes(flags, whole, powers, sums, edge, *work):
    row = rows((EY, NZ))
    in_y = jnp.where(row < NY, 1.0, jnp.where(row < NY + HALO, flags[3:4, :], flags[2:3, :]))
    below_x, above_x = in_y * flags[0:1, :], in_y * flags[1:2, :]

    def inside(x):
        return below_x if x < 0 else (above_x if x >= NX else in_y)

    def plane(x):
        return [whole[c, x % EX] for c in range(3)]

    def products(value):
        return [value[0] * value[c] for c in range(3)]

    lane = lanes((8, NZ))
    for c in range(3):
        for p in range(GROUPS):
            for t in range(3):
                part = slice(8 * t, 8 * t + 8)
                tile = jnp.zeros((8, NZ), jnp.float32)
                for g in range(GROUPS):
                    source = whole[c, GROUPS * g + p, part, :]
                    first = STEP * g + 4
                    tile = jnp.where((lane >= first) & (lane < first + 8), turned(source, first), tile)
                    first = STEP * g + 16
                    tile = jnp.where((lane >= first) & (lane < first + 8), turned(source, first - 120), tile)
                edge[c, p, part, :] = tile

    for x in range(-ITERS, NX + ITERS):
        new = section_of(plane(x), inside(x), products(plane(x - 1)), products(plane(x + 1)))
        for c in range(3):
            work[0][c, x % EX] = new[c]
            if 0 <= x < NX:
                powers[0, c, x] = new[c][:NY]
    for k in range(1, ITERS + 1):
        reach = ITERS - k
        for x in range(-reach, NX + reach):
            for c in range(3):
                source = work[k - 1]
                new = laplace_of(source[c, x % EX], source[c, (x - 1) % EX], source[c, (x + 1) % EX])
                if k < ITERS:
                    new = new * inside(x)
                    work[k][c, x % EX] = new
                if 0 <= x < NX:
                    powers[k, c, x] = new[:NY]
    valid = (lane >= HALO) & (lane < NZ - HALO)
    zero = jnp.zeros((8, NZ), jnp.float32)
    for c in range(3):
        total = [(zero, zero)] * MOMENTS
        for x in range(NX):
            for t in range(2):
                v = [powers[k, c, x, 8 * t : 8 * t + 8, :] for k in range(ITERS + 1)]
                total = [added(s, (v[a] * v[b], zero)) for s, (a, b) in zip(total, pairs())]
        for k in range(MOMENTS):
            for part in range(2):
                sums[c, k, part] = jnp.where(valid, total[k][part], 0.0)


def edge_lanes(flags, edge, first, second, sums, powers, moments, whole, *work):
    row = rows((EY, NZ))
    lane = lanes((EY, NZ))
    group, offset = lane // STEP, lane % STEP
    inside = jnp.where(row >= NY + HALO, flags[2:3, :], jnp.where(row >= NY, flags[3:4, :], 1.0))
    inside *= jnp.where(group == 3, flags[0:1, :], jnp.where(group == 2, flags[1:2, :], 1.0))
    inside *= jnp.where(offset < 4, flags[4:5, :], jnp.where(offset >= 24, flags[5:6, :], 1.0))
    odd = is_odd(GZ)
    lowest = lanes((8, NZ)) % STEP < 4
    highest = (lanes((8, NZ)) % STEP >= 24) & (lanes((8, NZ)) % STEP < 28)
    for k in range(Z_TILES):
        low = jnp.where(odd, second[k], first[k])
        high = jnp.where(odd, first[k], second[k])
        for half in range(2):
            c, t = divmod(2 * k + half, 3)
            part = slice(8 * t, 8 * t + 8)
            for p in range(GROUPS if c < 3 else 0):
                value = jnp.where(lowest, turned(low, -16 * half - 4 * p), edge[c, p, part, :])
                whole[c, p, part, :] = jnp.where(highest, turned(high, 24 - 16 * half - 4 * p), value)

    def beyond(read, p):
        return turned(read(0), -STEP) if p == GROUPS - 1 else read(p + 1)

    def behind(read, p):
        return turned(read(GROUPS - 1), STEP) if p == 0 else read(p - 1)

    for p in range(GROUPS):
        at = [whole[c, p] for c in range(3)]
        before, after = (
            [side(lambda q, c=c: whole[0, q] * whole[c, q], p) for c in range(3)] for side in (behind, beyond)
        )
        new = section_of(at, inside, before, after)
        for c in range(3):
            work[0][c, p] = new[c]
            powers[0, c, p] = new[c][:NY]
    for k in range(1, ITERS + 1):
        for p in range(GROUPS):
            for c in range(3):
                read = functools.partial(lambda c, q: work[k - 1][c, q], c)
                new = laplace_of(read(p), behind(read, p), beyond(read, p))
                if k < ITERS:
                    new = new * inside
                    work[k][c, p] = new
                powers[k, c, p] = new[:NY]
    lane = lanes((8, NZ))
    group, offset = lane // STEP, lane % STEP
    valid = (group < 2) & (((offset >= 4) & (offset < 8)) | ((offset >= 20) & (offset < 24)))
    zero = jnp.zeros((8, NZ), jnp.float32)
    totals = []
    for k in range(MOMENTS):
        a, b = pairs()[k]
        for c in range(3):
            total = (sums[c, k, 0], sums[c, k, 1])
            for p in range(GROUPS):
                for t in range(2):
                    part = slice(8 * t, 8 * t + 8)
                    value = powers[a, c, p, part, :] * powers[b, c, p, part, :]
                    total = added(total, (jnp.where(valid, value, 0.0), zero))
            totals.append(total)
    moments[...] = jnp.broadcast_to(lane_totals(totals), moments.shape)


def weights_of(moments, scale):
    middle = moments[1][0] / moments[0][0]
    moments = list(moments)
    for r in range(1, MOMENTS):
        for k in range(MOMENTS - 1, r - 1, -1):
            total, rest = two_product(middle, moments[k - 1][0])
            rest = rest + middle * moments[k - 1][1]
            moments[k] = two_sum(*added(moments[k], (-total, -rest)))
    moments = [m[0] for m in moments]
    diagonal = 1.0 + scale * middle

    def inner(first, second):
        return sum(f * s * moments[i + j] for i, f in enumerate(first) for j, s in enumerate(second))

    def plus(first, factor, second):
        size = max(len(first), len(second))
        padded = [list(v) + [0.0] * (size - len(v)) for v in (first, second)]
        return [f + factor * s for f, s in zip(*padded)]

    def in_powers_of_l(weights):
        weights = list(weights)
        for r in range(len(weights) - 1):
            for k in range(len(weights) - 2, r - 1, -1):
                weights[k] = weights[k] - middle * weights[k + 1]
        return weights

    one = jnp.ones_like(scale)
    total, residual, direction = [], [one], [one]
    now = moments[0]
    for iteration in range(ITERS):
        image = plus([diagonal * d for d in direction], scale, [0.0] + direction)
        step = now / inner(direction, image)
        total = plus(total, step, direction)
        residual = plus(residual, -step, image)
        if iteration + 1 < ITERS:
            new = inner(residual, residual)
            direction = plus(residual, new / now, direction)
            now = new
    return in_powers_of_l(total), in_powers_of_l(residual)


def combine(parts, flags, powers, edges, total, rest):
    lane = lanes((8, NZ))
    high, low = folded(lambda first, size: parts[first : first + size, :], parts.shape[0])
    moments = [(turned(high, -3 * k), turned(low, -3 * k)) for k in range(MOMENTS)]

    def spread(value, c):
        return jnp.broadcast_to(jnp.sum(jnp.where(lane == c, value, 0.0), axis=1, keepdims=True), (8, NZ))

    for out, weights in zip((total, rest), weights_of(moments, jnp.broadcast_to(flags[6:7, :], (8, NZ)))):
        for c in range(3):
            factors = [spread(w, c) for w in weights]

            def mix(read):
                return sum(f * read(k) for k, f in enumerate(factors))

            for p in range(GROUPS):
                for t in range(2):
                    part = slice(8 * t, 8 * t + 8)
                    side = mix(lambda k: edges[k, c, p, part, :])
                    for g in range(2):
                        x = GROUPS * g + p
                        value = mix(lambda k: powers[k, c, x, part, :])
                        value = jnp.where(lane < HALO, turned(side, -(STEP * g + 4)), value)
                        value = jnp.where(lane >= NZ - HALO, turned(side, 104 - STEP * g), value)
                        out[c, x, part, :] = value


def kernel(body, outs, scratch=(), first=False, last=False):
    vmem = pl.BlockSpec(memory_space=pltpu.VMEM)
    shape = jax.ShapeDtypeStruct if last else pltpu.VMEM

    def call(*args):
        if not first:
            args = [pltpu.with_memory_space_constraint(a, pltpu.VMEM) for a in args]
        return pl.pallas_call(
            body,
            in_specs=[vmem] * len(args),
            out_specs=[vmem] * len(outs),
            out_shape=[shape(s, jnp.float32) for s in outs],
            scratch_shapes=[pltpu.VMEM(s, jnp.float32) for s in scratch],
            name=body.__name__,
        )(*args)

    return call


def swapped(first, second, axis):
    size = lax.axis_size(axis)

    def pairs_from(start):
        up = [(i, i + 1) for i in range(start, size - 1, 2)]
        return up + [(b, a) for a, b in up]

    return lax.ppermute(first, axis, pairs_from(1)), lax.ppermute(second, axis, pairs_from(0))


def gathered(row, axes):
    return lax.all_to_all(row, axes, 0, 0, tiled=True)


def body(velocity, diffusion):
    ends = [f for a in (GX, GY, GZ) for f in (lax.axis_index(a) > 0, lax.axis_index(a) + 1 < lax.axis_size(a))]
    flags = jnp.broadcast_to(jnp.stack(ends).astype(jnp.float32)[:, None], (6, NZ))
    flags = jnp.concatenate([flags, jnp.broadcast_to(jnp.pad(6.0 * diffusion, (0, NZ - 3))[None], (2, NZ))])
    block, wide, tiles = (3, NX, NY, NZ), (3, EX, EY, NZ), (3, GROUPS, EY, NZ)
    own, first, second = kernel(pack_y, [block] + [(3, 4, 8, NZ)] * 2, first=True)(velocity)
    beside = swapped(first, second, GY)
    first, second = kernel(pack_x, [(3, 11, 8, NZ)] * 2)(own, *beside)
    beside += swapped(first, second, GX)
    whole, first, second = kernel(pack_z, [wide] + [(Z_TILES, 8, NZ)] * 2)(own, *beside)
    first, second = swapped(first, second, GZ)
    powers, sums, edge = kernel(
        inner_lanes, [(ITERS + 1,) + block, (3, MOMENTS, 2, 8, NZ), tiles], [wide] * ITERS
    )(flags, whole)
    planes, stack = lax.axis_size(GX + GY), lax.axis_size(GZ)
    edges, row = kernel(
        edge_lanes, [(ITERS + 1, 3, GROUPS, NY, NZ), (planes, NZ)], [tiles] * (ITERS + 1)
    )(flags, edge, first, second, sums)
    (row,) = kernel(fold, [(stack, NZ)])(gathered(row, GX + GY))
    return kernel(combine, [block] * 2, last=True)(gathered(row, GZ), flags, powers, edges)


def solution(mesh):
    finer = Mesh(
        mesh.devices.reshape(2, 2, 4, 4, mesh.shape["gz"]), ("gx_0", "gx_1", "gy_0", "gy_1", "gz")
    )
    return jax.shard_map(
        body,
        mesh=finer,
        in_specs=(P(None, GX, GY, "gz"), P()),
        out_specs=(P(None, GX, GY, "gz"), P(None, GX, GY, "gz")),
        check_vma=False,
    )
```

```python
import functools

import jax
import jax.numpy as jnp
from jax import lax
from jax.experimental import pallas as pl
from jax.experimental.pallas import tpu as pltpu
from jax.sharding import Mesh
from jax.sharding import PartitionSpec as P

ITERS = 3
GX = ("gx_0", "gx_1")
GY = ("gy_0", "gy_1")
GZ = ("gz",)
HALO = ITERS + 1

time_step = 0.25

NX, NY, NZ = 8, 16, 128
EX, EY = NX + 2 * HALO, NY + 2 * HALO
GROUPS = 4
STEP = NZ // GROUPS
MOMENTS = 2 * ITERS
Z_TILES = 5


def lanes(shape):
    return lax.broadcasted_iota(jnp.int32, shape, len(shape) - 1)


def rows(shape):
    return lax.broadcasted_iota(jnp.int32, shape, len(shape) - 2)


def back(value, axis):
    return pltpu.roll(value, value.shape[axis] - 1, axis)


def ahead(value, axis):
    return pltpu.roll(value, 1, axis)


def turned(value, shift):
    shift = shift % value.shape[-1]
    return pltpu.roll(value, shift, value.ndim - 1) if shift else value


def is_odd(axes):
    return lax.axis_index(axes) % 2 == 1


def pack_y(block, own, first, second, arrived):
    odd = is_odd(GY)
    sub = rows((8, NZ))
    copies = [pltpu.make_async_copy(block.at[c], own.at[c], arrived.at[c]) for c in range(3)]
    for copy in copies:
        copy.start()
    for c in range(3):
        copies[c].wait()
        for q in range(4):
            up = jnp.where(sub >= 4, own[c, q, 8:16, :], pltpu.roll(own[c, q + 4, 8:16, :], 4, 0))
            down = jnp.where(sub < 4, own[c, q, 0:8, :], pltpu.roll(own[c, q + 4, 0:8, :], 4, 0))
            first[c, q] = jnp.where(odd, up, down)
            second[c, q] = jnp.where(odd, down, up)


def beside_y(odd, first, second, c, x):
    low = jnp.where(odd, second[c, x % 4], first[c, x % 4])
    high = jnp.where(odd, first[c, x % 4], second[c, x % 4])
    sub = rows((8, NZ))
    if x < 4:
        return jnp.where(sub < 4, high, low)
    return pltpu.roll(jnp.where(sub < 4, low, high), 4, 0)


def pack_x(own, first_y, second_y, first, second):
    odd_y, odd = is_odd(GY), is_odd(GX)

    def put(c, n, up, down):
        first[c, n] = jnp.where(odd, up, down)
        second[c, n] = jnp.where(odd, down, up)

    for c in range(3):
        for n in range(HALO):
            for t in range(2):
                part = slice(8 * t, 8 * t + 8)
                put(c, 2 * n + t, own[c, NX - HALO + n, part, :], own[c, n, part, :])
        for n in range(HALO - 1):
            put(
                c,
                8 + n,
                beside_y(odd_y, first_y, second_y, c, NX - HALO + 1 + n),
                beside_y(odd_y, first_y, second_y, c, n),
            )


def pack_z(own, first_y, second_y, first_x, second_x, whole, first, second):
    odd_y, odd, odd_z = is_odd(GY), is_odd(GX), is_odd(GZ)
    lane = lanes((8, NZ))
    zero = jnp.zeros((8, NZ), jnp.float32)

    def tile_of(c, i, t):
        if i < NX:
            return own[c, i, 8 * t : 8 * t + 8, :] if t < 2 else beside_y(odd_y, first_y, second_y, c, i)
        n = i - NX
        if n < HALO:
            if t == 2 and n == HALO - 1:
                return zero
            k = 2 * n + t if t < 2 else 8 + n
            return jnp.where(odd, first_x[c, k], second_x[c, k])
        n -= HALO
        if t == 2 and n == 0:
            return zero
        k = 2 * n + t if t < 2 else 7 + n
        return jnp.where(odd, second_x[c, k], first_x[c, k])

    for k in range(Z_TILES):
        ups, downs = zero, zero
        for half in range(2):
            c, t = divmod(2 * k + half, 3)
            for i in range(EX if c < 3 else 0):
                tile = tile_of(c, i, t)
                whole[c, i, 8 * t : 8 * t + 8, :] = tile
                place = STEP * (i // 4) + 16 * half + 4 * (i % 4)
                here = (lane >= place) & (lane < place + 4)
                ups = jnp.where(here, turned(tile, place - (NZ - HALO)), ups)
                downs = jnp.where(here, turned(tile, place), downs)
        first[k] = jnp.where(odd_z, ups, downs)
        second[k] = jnp.where(odd_z, downs, ups)


def two_sum(a, b):
    total = a + b
    part = total - a
    return total, (a - (total - part)) + (b - part)


def split(a):
    large = a * 4097.0
    high = large - (large - a)
    return high, a - high


def two_product(a, b):
    total = a * b
    (ah, al), (bh, bl) = split(a), split(b)
    return total, ((ah * bh - total) + ah * bl + al * bh) + al * bl


def added(first, second):
    total, rest = two_sum(first[0], second[0])
    return total, (first[1] + second[1]) + rest


def rolled(value, shift, axis):
    return tuple(pltpu.roll(v, shift, axis) for v in value)


def chosen(where, first, second):
    return tuple(jnp.where(where, f, s) for f, s in zip(first, second))


def lane_totals(values):
    row, lane = rows((8, NZ)), lanes((8, NZ))
    reverse = (row % 2) * 4 + (row // 2 % 2) * 2 + row // 4
    zero = jnp.zeros((8, NZ), jnp.float32)
    found = zero
    for g in range(0, len(values), 8):
        group = values[g : g + 8]
        group = group + [(zero, zero)] * (8 - len(group))
        for half in (4, 2, 1):
            early = row % (2 * half) < half
            group = [
                added(
                    chosen(early, first, rolled(second, half, 0)),
                    chosen(early, rolled(first, 8 - half, 0), second),
                )
                for first, second in zip(group[::2], group[1::2])
            ]
        total = group[0]
        for half in (64, 32, 16, 8, 4, 2, 1):
            total = added(total, rolled(total, half, 1))
        total = two_sum(*total)
        found = jnp.where(lane == g + reverse, total[0], found)
        found = jnp.where(lane == 64 + g + reverse, total[1], found)
    return jnp.sum(found, axis=0, keepdims=True)


def folded(read, count):
    tiles = []
    for first in range(0, count, 8):
        size = min(8, count - first)
        tile = read(first, size)
        if size < 8:
            tile = jnp.concatenate([tile, jnp.zeros((8 - size, NZ), jnp.float32)], axis=0)
        tiles.append((tile, turned(tile, 64)))
    while len(tiles) > 1:
        tiles = [added(f, s) for f, s in zip(tiles[::2], tiles[1::2])] + tiles[len(tiles) // 2 * 2 :]
    total = tiles[0]
    for half in (4, 2, 1):
        total = added(total, rolled(total, half, 0))
    return two_sum(*total)


def fold(parts, out):
    high, rest = folded(lambda first, size: parts[first : first + size, :], parts.shape[0])
    row = jnp.where(lanes((8, NZ)) < 64, high, turned(rest, 64))[0:1]
    out[...] = jnp.broadcast_to(row, out.shape)


def section_of(at, here, before, after):
    result = []
    for c in range(3):
        slope = after[c] - before[c]
        flux = at[1] * at[c]
        slope = slope + (back(flux, 0) - ahead(flux, 0))
        flux = at[2] * at[c]
        slope = slope + (back(flux, 1) - ahead(flux, 1))
        result.append((at[c] - (0.5 * time_step) * slope) * here)
    return result


def laplace_of(at, before, after):
    beside = (before + after) + (back(at, 0) + ahead(at, 0))
    beside = beside + (back(at, 1) + ahead(at, 1))
    return at - beside * (1.0 / 6.0)


def pairs():
    return [(k // 2, (k + 1) // 2) for k in range(MOMENTS)]


def inner_lanes(flags, whole, powers, sums, edge, *work):
    row = rows((EY, NZ))
    in_y = jnp.where(row < NY, 1.0, jnp.where(row < NY + HALO, flags[3:4, :], flags[2:3, :]))
    below_x, above_x = in_y * flags[0:1, :], in_y * flags[1:2, :]

    def inside(x):
        return below_x if x < 0 else (above_x if x >= NX else in_y)

    def plane(x):
        return [whole[c, x % EX] for c in range(3)]

    def products(value):
        return [value[0] * value[c] for c in range(3)]

    lane = lanes((8, NZ))
    for c in range(3):
        for p in range(GROUPS):
            for t in range(3):
                part = slice(8 * t, 8 * t + 8)
                tile = jnp.zeros((8, NZ), jnp.float32)
                for g in range(GROUPS):
                    source = whole[c, GROUPS * g + p, part, :]
                    first = STEP * g + 4
                    tile = jnp.where((lane >= first) & (lane < first + 8), turned(source, first), tile)
                    first = STEP * g + 16
                    tile = jnp.where((lane >= first) & (lane < first + 8), turned(source, first - 120), tile)
                edge[c, p, part, :] = tile

    for x in range(-ITERS, NX + ITERS):
        new = section_of(plane(x), inside(x), products(plane(x - 1)), products(plane(x + 1)))
        for c in range(3):
            work[0][c, x % EX] = new[c]
            if 0 <= x < NX:
                powers[0, c, x] = new[c][:NY]
    for k in range(1, ITERS + 1):
        reach = ITERS - k
        for x in range(-reach, NX + reach):
            for c in range(3):
                source = work[k - 1]
                new = laplace_of(source[c, x % EX], source[c, (x - 1) % EX], source[c, (x + 1) % EX])
                if k < ITERS:
                    new = new * inside(x)
                    work[k][c, x % EX] = new
                if 0 <= x < NX:
                    powers[k, c, x] = new[:NY]
    valid = (lane >= HALO) & (lane < NZ - HALO)
    zero = jnp.zeros((8, NZ), jnp.float32)
    for c in range(3):
        total = [(zero, zero)] * MOMENTS
        for x in range(NX):
            for t in range(2):
                v = [powers[k, c, x, 8 * t : 8 * t + 8, :] for k in range(ITERS + 1)]
                total = [added(s, (v[a] * v[b], zero)) for s, (a, b) in zip(total, pairs())]
        for k in range(MOMENTS):
            for part in range(2):
                sums[c, k, part] = jnp.where(valid, total[k][part], 0.0)


def edge_lanes(flags, edge, first, second, sums, powers, moments, whole, *work):
    row = rows((EY, NZ))
    lane = lanes((EY, NZ))
    group, offset = lane // STEP, lane % STEP
    inside = jnp.where(row >= NY + HALO, flags[2:3, :], jnp.where(row >= NY, flags[3:4, :], 1.0))
    inside *= jnp.where(group == 3, flags[0:1, :], jnp.where(group == 2, flags[1:2, :], 1.0))
    inside *= jnp.where(offset < 4, flags[4:5, :], jnp.where(offset >= 24, flags[5:6, :], 1.0))
    odd = is_odd(GZ)
    lowest = lanes((8, NZ)) % STEP < 4
    highest = (lanes((8, NZ)) % STEP >= 24) & (lanes((8, NZ)) % STEP < 28)
    for k in range(Z_TILES):
        low = jnp.where(odd, second[k], first[k])
        high = jnp.where(odd, first[k], second[k])
        for half in range(2):
            c, t = divmod(2 * k + half, 3)
            part = slice(8 * t, 8 * t + 8)
            for p in range(GROUPS if c < 3 else 0):
                value = jnp.where(lowest, turned(low, -16 * half - 4 * p), edge[c, p, part, :])
                whole[c, p, part, :] = jnp.where(highest, turned(high, 24 - 16 * half - 4 * p), value)

    def beyond(read, p):
        return turned(read(0), -STEP) if p == GROUPS - 1 else read(p + 1)

    def behind(read, p):
        return turned(read(GROUPS - 1), STEP) if p == 0 else read(p - 1)

    for p in range(GROUPS):
        at = [whole[c, p] for c in range(3)]
        before, after = (
            [side(lambda q, c=c: whole[0, q] * whole[c, q], p) for c in range(3)] for side in (behind, beyond)
        )
        new = section_of(at, inside, before, after)
        for c in range(3):
            work[0][c, p] = new[c]
            powers[0, c, p] = new[c][:NY]
    for k in range(1, ITERS + 1):
        for p in range(GROUPS):
            for c in range(3):
                read = functools.partial(lambda c, q: work[k - 1][c, q], c)
                new = laplace_of(read(p), behind(read, p), beyond(read, p))
                if k < ITERS:
                    new = new * inside
                    work[k][c, p] = new
                powers[k, c, p] = new[:NY]
    lane = lanes((8, NZ))
    group, offset = lane // STEP, lane % STEP
    valid = (group < 2) & (((offset >= 4) & (offset < 8)) | ((offset >= 20) & (offset < 24)))
    zero = jnp.zeros((8, NZ), jnp.float32)
    totals = []
    for k in range(MOMENTS):
        a, b = pairs()[k]
        for c in range(3):
            total = (sums[c, k, 0], sums[c, k, 1])
            for p in range(GROUPS):
                for t in range(2):
                    part = slice(8 * t, 8 * t + 8)
                    value = powers[a, c, p, part, :] * powers[b, c, p, part, :]
                    total = added(total, (jnp.where(valid, value, 0.0), zero))
            totals.append(total)
    moments[...] = jnp.broadcast_to(lane_totals(totals), moments.shape)


def weights_of(moments, scale):
    middle = moments[1][0] / moments[0][0]
    moments = list(moments)
    for r in range(1, MOMENTS):
        for k in range(MOMENTS - 1, r - 1, -1):
            total, rest = two_product(middle, moments[k - 1][0])
            rest = rest + middle * moments[k - 1][1]
            moments[k] = two_sum(*added(moments[k], (-total, -rest)))
    moments = [m[0] for m in moments]
    diagonal = 1.0 + scale * middle

    def inner(first, second):
        return sum(f * s * moments[i + j] for i, f in enumerate(first) for j, s in enumerate(second))

    def plus(first, factor, second):
        size = max(len(first), len(second))
        padded = [list(v) + [0.0] * (size - len(v)) for v in (first, second)]
        return [f + factor * s for f, s in zip(*padded)]

    def in_powers_of_l(weights):
        weights = list(weights)
        for r in range(len(weights) - 1):
            for k in range(len(weights) - 2, r - 1, -1):
                weights[k] = weights[k] - middle * weights[k + 1]
        return weights

    one = jnp.ones_like(scale)
    total, residual, direction = [], [one], [one]
    now = moments[0]
    for iteration in range(ITERS):
        image = plus([diagonal * d for d in direction], scale, [0.0] + direction)
        step = now / inner(direction, image)
        total = plus(total, step, direction)
        residual = plus(residual, -step, image)
        if iteration + 1 < ITERS:
            new = inner(residual, residual)
            direction = plus(residual, new / now, direction)
            now = new
    return in_powers_of_l(total), in_powers_of_l(residual)


def combine(parts, flags, powers, edges, total, rest, total_here, rest_here, left):
    copies = []
    lane = lanes((8, NZ))
    high, low = folded(lambda first, size: parts[first : first + size, :], parts.shape[0])
    moments = [(turned(high, -3 * k), turned(low, -3 * k)) for k in range(MOMENTS)]

    def spread(value, c):
        return jnp.broadcast_to(jnp.sum(jnp.where(lane == c, value, 0.0), axis=1, keepdims=True), (8, NZ))

    for (target, out), weights in zip(((total, total_here), (rest, rest_here)), weights_of(moments, jnp.broadcast_to(flags[6:7, :], (8, NZ)))):
        for c in range(3):
            factors = [spread(w, c) for w in weights]

            def mix(read):
                return sum(f * read(k) for k, f in enumerate(factors))

            for p in range(GROUPS):
                for t in range(2):
                    part = slice(8 * t, 8 * t + 8)
                    side = mix(lambda k: edges[k, c, p, part, :])
                    for g in range(2):
                        x = GROUPS * g + p
                        value = mix(lambda k: powers[k, c, x, part, :])
                        value = jnp.where(lane < HALO, turned(side, -(STEP * g + 4)), value)
                        value = jnp.where(lane >= NZ - HALO, turned(side, 104 - STEP * g), value)
                        out[c, x, part, :] = value
            copies.append(pltpu.make_async_copy(out.at[c], target.at[c], left.at[len(copies)]))
            copies[-1].start()
    for copy in copies:
        copy.wait()


def kernel(body, outs, scratch=(), first=False, last=False):
    vmem, hbm = (pl.BlockSpec(memory_space=m) for m in (pltpu.VMEM, pl.ANY))
    shape = jax.ShapeDtypeStruct if last else pltpu.VMEM

    def call(*args):
        if not first:
            args = [pltpu.with_memory_space_constraint(a, pltpu.VMEM) for a in args]
        semaphores = [pltpu.SemaphoreType.DMA((2 * 3 if last else 3,))] if first or last else []
        return pl.pallas_call(
            body,
            in_specs=[hbm if first else vmem] * len(args),
            out_specs=[hbm if last else vmem] * len(outs),
            out_shape=[shape(s, jnp.float32) for s in outs],
            scratch_shapes=[pltpu.VMEM(s, jnp.float32) for s in scratch] + semaphores,
            name=body.__name__,
        )(*args)

    return call


def swapped(first, second, axis):
    size = lax.axis_size(axis)

    def pairs_from(start):
        up = [(i, i + 1) for i in range(start, size - 1, 2)]
        return up + [(b, a) for a, b in up]

    return lax.ppermute(first, axis, pairs_from(1)), lax.ppermute(second, axis, pairs_from(0))


def gathered(row, axes):
    return lax.all_to_all(row, axes, 0, 0, tiled=True)


def body(velocity, diffusion):
    ends = [f for a in (GX, GY, GZ) for f in (lax.axis_index(a) > 0, lax.axis_index(a) + 1 < lax.axis_size(a))]
    flags = jnp.broadcast_to(jnp.stack(ends).astype(jnp.float32)[:, None], (6, NZ))
    flags = jnp.concatenate([flags, jnp.broadcast_to(jnp.pad(6.0 * diffusion, (0, NZ - 3))[None], (2, NZ))])
    block, wide, tiles = (3, NX, NY, NZ), (3, EX, EY, NZ), (3, GROUPS, EY, NZ)
    own, first, second = kernel(pack_y, [block] + [(3, 4, 8, NZ)] * 2, first=True)(velocity)
    beside = swapped(first, second, GY)
    first, second = kernel(pack_x, [(3, 11, 8, NZ)] * 2)(own, *beside)
    beside += swapped(first, second, GX)
    whole, first, second = kernel(pack_z, [wide] + [(Z_TILES, 8, NZ)] * 2)(own, *beside)
    first, second = swapped(first, second, GZ)
    powers, sums, edge = kernel(
        inner_lanes, [(ITERS + 1,) + block, (3, MOMENTS, 2, 8, NZ), tiles], [wide] * ITERS
    )(flags, whole)
    near, far = GX[:1] + GY, GX[1:] + GZ
    planes, stack = lax.axis_size(near), lax.axis_size(far)
    edges, row = kernel(
        edge_lanes, [(ITERS + 1, 3, GROUPS, NY, NZ), (planes, NZ)], [tiles] * (ITERS + 1)
    )(flags, edge, first, second, sums)
    (row,) = kernel(fold, [(stack, NZ)])(gathered(row, near))
    return kernel(combine, [block] * 2, [block] * 2, last=True)(gathered(row, far), flags, powers, edges)


def solution(mesh):
    finer = Mesh(
        mesh.devices.reshape(2, 2, 4, 4, mesh.shape["gz"]), ("gx_0", "gx_1", "gy_0", "gy_1", "gz")
    )
    return jax.shard_map(
        body,
        mesh=finer,
        in_specs=(P(None, GX, GY, "gz"), P()),
        out_specs=(P(None, GX, GY, "gz"), P(None, GX, GY, "gz")),
        check_vma=False,
    )
```

```python
import functools

import jax
import jax.numpy as jnp
from jax import lax
from jax.experimental import pallas as pl
from jax.experimental.pallas import tpu as pltpu
from jax.sharding import Mesh
from jax.sharding import PartitionSpec as P

ITERS = 3
GX = ("gx_0", "gx_1")
GY = ("gy_0", "gy_1")
GZ = ("gz",)
HALO = ITERS + 1

time_step = 0.25

NX, NY, NZ = 8, 16, 128
EX, EY = NX + 2 * HALO, NY + 2 * HALO
GROUPS = 4
STEP = NZ // GROUPS
MOMENTS = 2 * ITERS
Z_TILES = 5


def lanes(shape):
    return lax.broadcasted_iota(jnp.int32, shape, len(shape) - 1)


def rows(shape):
    return lax.broadcasted_iota(jnp.int32, shape, len(shape) - 2)


def back(value, axis):
    return pltpu.roll(value, value.shape[axis] - 1, axis)


def ahead(value, axis):
    return pltpu.roll(value, 1, axis)


def turned(value, shift):
    shift = shift % value.shape[-1]
    return pltpu.roll(value, shift, value.ndim - 1) if shift else value


def is_odd(axes):
    return lax.axis_index(axes) % 2 == 1


def pack_y(block, own, first, second):
    odd = is_odd(GY)
    sub = rows((8, NZ))
    own[...] = block[...]
    for c in range(3):
        for q in range(4):
            up = jnp.where(sub >= 4, block[c, q, 8:16, :], pltpu.roll(block[c, q + 4, 8:16, :], 4, 0))
            down = jnp.where(sub < 4, block[c, q, 0:8, :], pltpu.roll(block[c, q + 4, 0:8, :], 4, 0))
            first[c, q] = jnp.where(odd, up, down)
            second[c, q] = jnp.where(odd, down, up)


def beside_y(odd, first, second, c, x):
    low = jnp.where(odd, second[c, x % 4], first[c, x % 4])
    high = jnp.where(odd, first[c, x % 4], second[c, x % 4])
    sub = rows((8, NZ))
    if x < 4:
        return jnp.where(sub < 4, high, low)
    return pltpu.roll(jnp.where(sub < 4, low, high), 4, 0)


def pack_x(own, first_y, second_y, first, second):
    odd_y, odd = is_odd(GY), is_odd(GX)

    def put(c, n, up, down):
        first[c, n] = jnp.where(odd, up, down)
        second[c, n] = jnp.where(odd, down, up)

    for c in range(3):
        for n in range(HALO):
            for t in range(2):
                part = slice(8 * t, 8 * t + 8)
                put(c, 2 * n + t, own[c, NX - HALO + n, part, :], own[c, n, part, :])
        for n in range(HALO - 1):
            put(
                c,
                8 + n,
                beside_y(odd_y, first_y, second_y, c, NX - HALO + 1 + n),
                beside_y(odd_y, first_y, second_y, c, n),
            )


def pack_z(own, first_y, second_y, first_x, second_x, whole, first, second):
    odd_y, odd, odd_z = is_odd(GY), is_odd(GX), is_odd(GZ)
    lane = lanes((8, NZ))
    zero = jnp.zeros((8, NZ), jnp.float32)

    def tile_of(c, i, t):
        if i < NX:
            return own[c, i, 8 * t : 8 * t + 8, :] if t < 2 else beside_y(odd_y, first_y, second_y, c, i)
        n = i - NX
        if n < HALO:
            if t == 2 and n == HALO - 1:
                return zero
            k = 2 * n + t if t < 2 else 8 + n
            return jnp.where(odd, first_x[c, k], second_x[c, k])
        n -= HALO
        if t == 2 and n == 0:
            return zero
        k = 2 * n + t if t < 2 else 7 + n
        return jnp.where(odd, second_x[c, k], first_x[c, k])

    def faces(c, t, i, count):
        if count == 1:
            tile = tile_of(c, i, t)
            whole[c, i, 8 * t : 8 * t + 8, :] = tile
            return turned(tile, 8 * i + HALO)
        count //= 2
        early, late = faces(c, t, i, count), faces(c, t, i + count, count)
        return jnp.where(lane // 8 // count % 2 == 1, late, early)

    both = [faces(c, t, 0, EX) for c in range(3) for t in range(3)] + [zero]
    for k in range(Z_TILES):
        early, late = both[2 * k : 2 * k + 2]
        if k == Z_TILES - 1:
            up, down = early, turned(early, -HALO)
        else:
            up = jnp.where(lane % 8 < HALO, early, turned(late, HALO))
            down = jnp.where(lane % 8 < HALO, turned(early, -HALO), late)
        first[k] = jnp.where(odd_z, up, down)
        second[k] = jnp.where(odd_z, down, up)


def two_sum(a, b):
    total = a + b
    part = total - a
    return total, (a - (total - part)) + (b - part)


def split(a):
    large = a * 4097.0
    high = large - (large - a)
    return high, a - high


def two_product(a, b):
    total = a * b
    (ah, al), (bh, bl) = split(a), split(b)
    return total, ((ah * bh - total) + ah * bl + al * bh) + al * bl


def added(first, second):
    total, rest = two_sum(first[0], second[0])
    return total, (first[1] + second[1]) + rest


def more(total, value):
    high, rest = two_sum(total[0], value)
    return high, total[1] + rest


def rolled(value, shift, axis):
    return tuple(pltpu.roll(v, shift, axis) for v in value)


def chosen(where, first, second):
    return tuple(jnp.where(where, f, s) for f, s in zip(first, second))


def lane_totals(values):
    row, lane = rows((8, NZ)), lanes((8, NZ))
    reverse = (row % 2) * 4 + (row // 2 % 2) * 2 + row // 4
    zero = jnp.zeros((8, NZ), jnp.float32)
    found = zero
    for g in range(0, len(values), 8):
        group = values[g : g + 8]
        group = group + [(zero, zero)] * (8 - len(group))
        for half in (4, 2, 1):
            early = row % (2 * half) < half
            group = [
                added(
                    chosen(early, first, rolled(second, half, 0)),
                    chosen(early, rolled(first, 8 - half, 0), second),
                )
                for first, second in zip(group[::2], group[1::2])
            ]
        total = group[0]
        for half in (64, 32, 16, 8, 4, 2, 1):
            total = added(total, rolled(total, half, 1))
        total = two_sum(*total)
        found = jnp.where(lane == g + reverse, total[0], found)
        found = jnp.where(lane == 64 + g + reverse, total[1], found)
    return jnp.sum(found, axis=0, keepdims=True)


def folded(read, count):
    tiles = []
    for first in range(0, count, 8):
        size = min(8, count - first)
        tile = read(first, size)
        if size < 8:
            tile = jnp.concatenate([tile, jnp.zeros((8 - size, NZ), jnp.float32)], axis=0)
        tiles.append((tile, turned(tile, 64)))
    while len(tiles) > 1:
        tiles = [added(f, s) for f, s in zip(tiles[::2], tiles[1::2])] + tiles[len(tiles) // 2 * 2 :]
    total = tiles[0]
    for half in (4, 2, 1):
        total = added(total, rolled(total, half, 0))
    return two_sum(*total)


def fold(parts, out):
    high, rest = folded(lambda first, size: parts[first : first + size, :], parts.shape[0])
    row = jnp.where(lanes((8, NZ)) < 64, high, turned(rest, 64))[0:1]
    out[...] = jnp.broadcast_to(row, out.shape)


def section_of(at, here, before, after):
    result = []
    for c in range(3):
        slope = after[c] - before[c]
        flux = at[1] * at[c]
        slope = slope + (back(flux, 0) - ahead(flux, 0))
        flux = at[2] * at[c]
        slope = slope + (back(flux, 1) - ahead(flux, 1))
        result.append((at[c] - (0.5 * time_step) * slope) * here)
    return result


def laplace_of(at, before, after):
    beside = (before + after) + (back(at, 0) + ahead(at, 0))
    beside = beside + (back(at, 1) + ahead(at, 1))
    return at - beside * (1.0 / 6.0)


def pairs():
    return [(k // 2, (k + 1) // 2) for k in range(MOMENTS)]


def inner_lanes(flags, whole, powers, sums, edge, *work):
    row = rows((EY, NZ))
    in_y = jnp.where(row < NY, 1.0, jnp.where(row < NY + HALO, flags[3:4, :], flags[2:3, :]))
    below_x, above_x = in_y * flags[0:1, :], in_y * flags[1:2, :]

    def inside(x):
        return below_x if x < 0 else (above_x if x >= NX else in_y)

    def plane(x):
        return [whole[c, x % EX] for c in range(3)]

    def products(value):
        return [value[0] * value[c] for c in range(3)]

    lane = lanes((8, NZ))
    for c in range(3):
        for p in range(GROUPS):
            for t in range(3):
                part = slice(8 * t, 8 * t + 8)
                tile = jnp.zeros((8, NZ), jnp.float32)
                for g in range(GROUPS):
                    source = whole[c, GROUPS * g + p, part, :]
                    first = STEP * g + 4
                    tile = jnp.where((lane >= first) & (lane < first + 8), turned(source, first), tile)
                    first = STEP * g + 16
                    tile = jnp.where((lane >= first) & (lane < first + 8), turned(source, first - 120), tile)
                edge[c, p, part, :] = tile

    for x in range(-ITERS, NX + ITERS):
        new = section_of(plane(x), inside(x), products(plane(x - 1)), products(plane(x + 1)))
        for c in range(3):
            work[0][c, x % EX] = new[c]
            if 0 <= x < NX:
                powers[0, c, x] = new[c][:NY]
    for k in range(1, ITERS + 1):
        reach = ITERS - k
        for x in range(-reach, NX + reach):
            for c in range(3):
                source = work[k - 1]
                new = laplace_of(source[c, x % EX], source[c, (x - 1) % EX], source[c, (x + 1) % EX])
                if k < ITERS:
                    new = new * inside(x)
                    work[k][c, x % EX] = new
                if 0 <= x < NX:
                    powers[k, c, x] = new[:NY]
    valid = (lane >= HALO) & (lane < NZ - HALO)
    zero = jnp.zeros((8, NZ), jnp.float32)
    for c in range(3):
        total = [(zero, zero)] * MOMENTS
        for x in range(NX):
            for t in range(2):
                v = [powers[k, c, x, 8 * t : 8 * t + 8, :] for k in range(ITERS + 1)]
                total = [more(s, v[a] * v[b]) for s, (a, b) in zip(total, pairs())]
        for k in range(MOMENTS):
            for part in range(2):
                sums[c, k, part] = jnp.where(valid, total[k][part], 0.0)


def edge_lanes(flags, edge, first, second, sums, powers, moments, whole, *work):
    row = rows((EY, NZ))
    lane = lanes((EY, NZ))
    group, offset = lane // STEP, lane % STEP
    inside = jnp.where(row >= NY + HALO, flags[2:3, :], jnp.where(row >= NY, flags[3:4, :], 1.0))
    inside *= jnp.where(group == 3, flags[0:1, :], jnp.where(group == 2, flags[1:2, :], 1.0))
    inside *= jnp.where(offset < 4, flags[4:5, :], jnp.where(offset >= 24, flags[5:6, :], 1.0))
    odd = is_odd(GZ)
    lowest = lanes((8, NZ)) % STEP < 4
    highest = (lanes((8, NZ)) % STEP >= 24) & (lanes((8, NZ)) % STEP < 28)
    for k in range(Z_TILES):
        low = jnp.where(odd, second[k], first[k])
        high = jnp.where(odd, first[k], second[k])
        for half in range(2):
            c, t = divmod(2 * k + half, 3)
            part = slice(8 * t, 8 * t + 8)
            for p in range(GROUPS if c < 3 else 0):
                value = jnp.where(lowest, turned(low, -4 * half - 8 * p), edge[c, p, part, :])
                whole[c, p, part, :] = jnp.where(highest, turned(high, 24 - 4 * half - 8 * p), value)

    def beyond(read, p):
        return turned(read(0), -STEP) if p == GROUPS - 1 else read(p + 1)

    def behind(read, p):
        return turned(read(GROUPS - 1), STEP) if p == 0 else read(p - 1)

    for p in range(GROUPS):
        at = [whole[c, p] for c in range(3)]
        before, after = (
            [side(lambda q, c=c: whole[0, q] * whole[c, q], p) for c in range(3)] for side in (behind, beyond)
        )
        new = section_of(at, inside, before, after)
        for c in range(3):
            work[0][c, p] = new[c]
            powers[0, c, p] = new[c][:NY]
    for k in range(1, ITERS + 1):
        for p in range(GROUPS):
            for c in range(3):
                read = functools.partial(lambda c, q: work[k - 1][c, q], c)
                new = laplace_of(read(p), behind(read, p), beyond(read, p))
                if k < ITERS:
                    new = new * inside
                    work[k][c, p] = new
                powers[k, c, p] = new[:NY]
    lane = lanes((8, NZ))
    group, offset = lane // STEP, lane % STEP
    valid = (group < 2) & (((offset >= 4) & (offset < 8)) | ((offset >= 20) & (offset < 24)))
    totals = []
    for k in range(MOMENTS):
        a, b = pairs()[k]
        for c in range(3):
            parts = [(p, slice(8 * t, 8 * t + 8)) for p in range(GROUPS) for t in range(2)]
            value = sum(powers[a, c, p, part, :] * powers[b, c, p, part, :] for p, part in parts)
            totals.append(more((sums[c, k, 0], sums[c, k, 1]), jnp.where(valid, value, 0.0)))
    moments[...] = jnp.broadcast_to(lane_totals(totals), moments.shape)


def weights_of(moments, scale):
    middle = moments[1][0] / moments[0][0]
    moments = list(moments)
    for r in range(1, MOMENTS):
        for k in range(MOMENTS - 1, r - 1, -1):
            total, rest = two_product(middle, moments[k - 1][0])
            rest = rest + middle * moments[k - 1][1]
            moments[k] = two_sum(*added(moments[k], (-total, -rest)))
    moments = [m[0] for m in moments]
    diagonal = 1.0 + scale * middle

    def inner(first, second):
        return sum(f * s * moments[i + j] for i, f in enumerate(first) for j, s in enumerate(second))

    def plus(first, factor, second):
        size = max(len(first), len(second))
        padded = [list(v) + [0.0] * (size - len(v)) for v in (first, second)]
        return [f + factor * s for f, s in zip(*padded)]

    def in_powers_of_l(weights):
        weights = list(weights)
        for r in range(len(weights) - 1):
            for k in range(len(weights) - 2, r - 1, -1):
                weights[k] = weights[k] - middle * weights[k + 1]
        return weights

    one = jnp.ones_like(scale)
    total, residual, direction = [], [one], [one]
    now = moments[0]
    for iteration in range(ITERS):
        image = plus([diagonal * d for d in direction], scale, [0.0] + direction)
        step = now / inner(direction, image)
        total = plus(total, step, direction)
        residual = plus(residual, -step, image)
        if iteration + 1 < ITERS:
            new = inner(residual, residual)
            direction = plus(residual, new / now, direction)
            now = new
    return in_powers_of_l(total), in_powers_of_l(residual)


def combine(parts, flags, powers, edges, total, rest):
    lane = lanes((8, NZ))
    high, low = folded(lambda first, size: parts[first : first + size, :], parts.shape[0])
    moments = [(turned(high, -3 * k), turned(low, -3 * k)) for k in range(MOMENTS)]

    def spread(value, c):
        return jnp.broadcast_to(jnp.sum(jnp.where(lane == c, value, 0.0), axis=1, keepdims=True), (8, NZ))

    for out, weights in zip((total, rest), weights_of(moments, jnp.broadcast_to(flags[6:7, :], (8, NZ)))):
        for c in range(3):
            factors = [spread(w, c) for w in weights]

            def mix(read):
                return sum(f * read(k) for k, f in enumerate(factors))

            for p in range(GROUPS):
                for t in range(2):
                    part = slice(8 * t, 8 * t + 8)
                    side = mix(lambda k: edges[k, c, p, part, :])
                    for g in range(2):
                        x = GROUPS * g + p
                        value = mix(lambda k: powers[k, c, x, part, :])
                        value = jnp.where(lane < HALO, turned(side, -(STEP * g + 4)), value)
                        value = jnp.where(lane >= NZ - HALO, turned(side, 104 - STEP * g), value)
                        out[c, x, part, :] = value


def kernel(body, outs, scratch=(), first=False, last=False):
    vmem = pl.BlockSpec(memory_space=pltpu.VMEM)
    shape = jax.ShapeDtypeStruct if last else pltpu.VMEM

    def call(*args):
        if not first:
            args = [pltpu.with_memory_space_constraint(a, pltpu.VMEM) for a in args]
        return pl.pallas_call(
            body,
            in_specs=[vmem] * len(args),
            out_specs=[vmem] * len(outs),
            out_shape=[shape(s, jnp.float32) for s in outs],
            scratch_shapes=[pltpu.VMEM(s, jnp.float32) for s in scratch],
            name=body.__name__,
        )(*args)

    return call


def swapped(first, second, axis):
    size = lax.axis_size(axis)

    def pairs_from(start):
        up = [(i, i + 1) for i in range(start, size - 1, 2)]
        return up + [(b, a) for a, b in up]

    return lax.ppermute(first, axis, pairs_from(1)), lax.ppermute(second, axis, pairs_from(0))


def gathered(row, axes):
    return lax.all_to_all(row, axes, 0, 0, tiled=True)


def body(velocity, diffusion):
    ends = [f for a in (GX, GY, GZ) for f in (lax.axis_index(a) > 0, lax.axis_index(a) + 1 < lax.axis_size(a))]
    flags = jnp.broadcast_to(jnp.stack(ends).astype(jnp.float32)[:, None], (6, NZ))
    flags = jnp.concatenate([flags, jnp.broadcast_to(jnp.pad(6.0 * diffusion, (0, NZ - 3))[None], (2, NZ))])
    block, wide, tiles = (3, NX, NY, NZ), (3, EX, EY, NZ), (3, GROUPS, EY, NZ)
    own, first, second = kernel(pack_y, [block] + [(3, 4, 8, NZ)] * 2, first=True)(velocity)
    beside = swapped(first, second, GY)
    first, second = kernel(pack_x, [(3, 11, 8, NZ)] * 2)(own, *beside)
    beside += swapped(first, second, GX)
    whole, first, second = kernel(pack_z, [wide] + [(Z_TILES, 8, NZ)] * 2)(own, *beside)
    first, second = swapped(first, second, GZ)
    powers, sums, edge = kernel(
        inner_lanes, [(ITERS + 1,) + block, (3, MOMENTS, 2, 8, NZ), tiles], [wide] * ITERS
    )(flags, whole)
    planes, stack = lax.axis_size(GX + GY), lax.axis_size(GZ)
    edges, row = kernel(
        edge_lanes, [(ITERS + 1, 3, GROUPS, NY, NZ), (planes, NZ)], [tiles] * (ITERS + 1)
    )(flags, edge, first, second, sums)
    (row,) = kernel(fold, [(stack, NZ)])(gathered(row, GX + GY))
    return kernel(combine, [block] * 2, last=True)(gathered(row, GZ), flags, powers, edges)


def solution(mesh):
    finer = Mesh(
        mesh.devices.reshape(2, 2, 4, 4, mesh.shape["gz"]), ("gx_0", "gx_1", "gy_0", "gy_1", "gz")
    )
    return jax.shard_map(
        body,
        mesh=finer,
        in_specs=(P(None, GX, GY, "gz"), P()),
        out_specs=(P(None, GX, GY, "gz"), P(None, GX, GY, "gz")),
        check_vma=False,
    )
```

```python
import functools

import jax
import jax.numpy as jnp
from jax import lax
from jax.experimental import pallas as pl
from jax.experimental.pallas import tpu as pltpu
from jax.sharding import Mesh
from jax.sharding import PartitionSpec as P

ITERS = 3
GX = ("gx_0", "gx_1")
GY = ("gy_0", "gy_1")
GZ = ("gz",)
HALO = ITERS + 1

time_step = 0.25

NX, NY, NZ = 8, 16, 128
EX, EY = NX + 2 * HALO, NY + 2 * HALO
GROUPS = 4
STEP = NZ // GROUPS
MOMENTS = 2 * ITERS
Z_TILES = 5


def lanes(shape):
    return lax.broadcasted_iota(jnp.int32, shape, len(shape) - 1)


def rows(shape):
    return lax.broadcasted_iota(jnp.int32, shape, len(shape) - 2)


def back(value, axis):
    return pltpu.roll(value, value.shape[axis] - 1, axis)


def ahead(value, axis):
    return pltpu.roll(value, 1, axis)


def turned(value, shift):
    shift = shift % value.shape[-1]
    return pltpu.roll(value, shift, value.ndim - 1) if shift else value


def is_odd(axes):
    return lax.axis_index(axes) % 2 == 1


def pack_y(block, own, first, second):
    odd = is_odd(GY)
    sub = rows((8, NZ))
    own[...] = block[...]
    for c in range(3):
        for q in range(4):
            up = jnp.where(sub >= 4, block[c, q, 8:16, :], pltpu.roll(block[c, q + 4, 8:16, :], 4, 0))
            down = jnp.where(sub < 4, block[c, q, 0:8, :], pltpu.roll(block[c, q + 4, 0:8, :], 4, 0))
            first[c, q] = jnp.where(odd, up, down)
            second[c, q] = jnp.where(odd, down, up)


def beside_y(odd, first, second, c, x):
    low = jnp.where(odd, second[c, x % 4], first[c, x % 4])
    high = jnp.where(odd, first[c, x % 4], second[c, x % 4])
    sub = rows((8, NZ))
    if x < 4:
        return jnp.where(sub < 4, high, low)
    return pltpu.roll(jnp.where(sub < 4, low, high), 4, 0)


def pack_x(own, first_y, second_y, first, second):
    odd_y, odd = is_odd(GY), is_odd(GX)

    def put(c, n, up, down):
        first[c, n] = jnp.where(odd, up, down)
        second[c, n] = jnp.where(odd, down, up)

    for c in range(3):
        for n in range(HALO):
            for t in range(2):
                part = slice(8 * t, 8 * t + 8)
                put(c, 2 * n + t, own[c, NX - HALO + n, part, :], own[c, n, part, :])
        for n in range(HALO - 1):
            put(
                c,
                8 + n,
                beside_y(odd_y, first_y, second_y, c, NX - HALO + 1 + n),
                beside_y(odd_y, first_y, second_y, c, n),
            )


def pack_z(own, first_y, second_y, first_x, second_x, whole, first, second):
    odd_y, odd, odd_z = is_odd(GY), is_odd(GX), is_odd(GZ)
    lane = lanes((8, NZ))
    zero = jnp.zeros((8, NZ), jnp.float32)

    def tile_of(c, i, t):
        if i < NX:
            return own[c, i, 8 * t : 8 * t + 8, :] if t < 2 else beside_y(odd_y, first_y, second_y, c, i)
        n = i - NX
        if n < HALO:
            if t == 2 and n == HALO - 1:
                return zero
            k = 2 * n + t if t < 2 else 8 + n
            return jnp.where(odd, first_x[c, k], second_x[c, k])
        n -= HALO
        if t == 2 and n == 0:
            return zero
        k = 2 * n + t if t < 2 else 7 + n
        return jnp.where(odd, second_x[c, k], first_x[c, k])

    def faces(c, t, i, count):
        if count == 1:
            tile = tile_of(c, i, t)
            whole[c, i, 8 * t : 8 * t + 8, :] = tile
            return turned(tile, 8 * i + HALO)
        count //= 2
        early, late = faces(c, t, i, count), faces(c, t, i + count, count)
        return jnp.where(lane // 8 // count % 2 == 1, late, early)

    both = [faces(c, t, 0, EX) for c in range(3) for t in range(3)] + [zero]
    for k in range(Z_TILES):
        early, late = both[2 * k : 2 * k + 2]
        if k == Z_TILES - 1:
            up, down = early, turned(early, -HALO)
        else:
            up = jnp.where(lane % 8 < HALO, early, turned(late, HALO))
            down = jnp.where(lane % 8 < HALO, turned(early, -HALO), late)
        first[k] = jnp.where(odd_z, up, down)
        second[k] = jnp.where(odd_z, down, up)


def two_sum(a, b):
    total = a + b
    part = total - a
    return total, (a - (total - part)) + (b - part)


def split(a):
    large = a * 4097.0
    high = large - (large - a)
    return high, a - high


def two_product(a, b):
    total = a * b
    (ah, al), (bh, bl) = split(a), split(b)
    return total, ((ah * bh - total) + ah * bl + al * bh) + al * bl


def added(first, second):
    total, rest = two_sum(first[0], second[0])
    return total, (first[1] + second[1]) + rest


def more(total, value):
    high, rest = two_sum(total[0], value)
    return high, total[1] + rest


def rolled(value, shift, axis):
    return tuple(pltpu.roll(v, shift, axis) for v in value)


def chosen(where, first, second):
    return tuple(jnp.where(where, f, s) for f, s in zip(first, second))


def lane_totals(values):
    row, lane = rows((8, NZ)), lanes((8, NZ))
    reverse = (row % 2) * 4 + (row // 2 % 2) * 2 + row // 4
    zero = jnp.zeros((8, NZ), jnp.float32)
    found = zero
    for g in range(0, len(values), 8):
        group = values[g : g + 8]
        group = group + [(zero, zero)] * (8 - len(group))
        for half in (4, 2, 1):
            early = row % (2 * half) < half
            group = [
                added(
                    chosen(early, first, rolled(second, half, 0)),
                    chosen(early, rolled(first, 8 - half, 0), second),
                )
                for first, second in zip(group[::2], group[1::2])
            ]
        total = group[0]
        for half in (64, 32, 16, 8, 4, 2, 1):
            total = added(total, rolled(total, half, 1))
        total = two_sum(*total)
        found = jnp.where(lane == g + reverse, total[0], found)
        found = jnp.where(lane == 64 + g + reverse, total[1], found)
    return jnp.sum(found, axis=0, keepdims=True)


def folded(read, count):
    tiles = []
    for first in range(0, count, 8):
        size = min(8, count - first)
        tile = read(first, size)
        if size < 8:
            tile = jnp.concatenate([tile, jnp.zeros((8 - size, NZ), jnp.float32)], axis=0)
        tiles.append((tile, turned(tile, 64)))
    while len(tiles) > 1:
        tiles = [added(f, s) for f, s in zip(tiles[::2], tiles[1::2])] + tiles[len(tiles) // 2 * 2 :]
    total = tiles[0]
    for half in (4, 2, 1):
        total = added(total, rolled(total, half, 0))
    return two_sum(*total)


def fold(parts, out):
    high, rest = folded(lambda first, size: parts[first : first + size, :], parts.shape[0])
    row = jnp.where(lanes((8, NZ)) < 64, high, turned(rest, 64))[0:1]
    out[...] = jnp.broadcast_to(row, out.shape)


def section_of(at, here, before, after):
    result = []
    for c in range(3):
        slope = after[c] - before[c]
        flux = at[1] * at[c]
        slope = slope + (back(flux, 0) - ahead(flux, 0))
        flux = at[2] * at[c]
        slope = slope + (back(flux, 1) - ahead(flux, 1))
        result.append((at[c] - (0.5 * time_step) * slope) * here)
    return result


def laplace_of(at, before, after):
    beside = (before + after) + (back(at, 0) + ahead(at, 0))
    beside = beside + (back(at, 1) + ahead(at, 1))
    return at - beside * (1.0 / 6.0)


def pairs():
    return [(k // 2, (k + 1) // 2) for k in range(MOMENTS)]


def inner_lanes(flags, whole, powers, sums, edge, *work):
    row = rows((EY, NZ))
    in_y = jnp.where(row < NY, 1.0, jnp.where(row < NY + HALO, flags[3:4, :], flags[2:3, :]))
    below_x, above_x = in_y * flags[0:1, :], in_y * flags[1:2, :]

    def inside(x):
        return below_x if x < 0 else (above_x if x >= NX else in_y)

    def plane(x):
        return [whole[c, x % EX] for c in range(3)]

    def products(value):
        return [value[0] * value[c] for c in range(3)]

    lane = lanes((8, NZ))
    for c in range(3):
        for p in range(GROUPS):
            for t in range(3):
                part = slice(8 * t, 8 * t + 8)
                tile = jnp.zeros((8, NZ), jnp.float32)
                for g in range(GROUPS):
                    source = whole[c, GROUPS * g + p, part, :]
                    first = STEP * g + 4
                    tile = jnp.where((lane >= first) & (lane < first + 8), turned(source, first), tile)
                    first = STEP * g + 16
                    tile = jnp.where((lane >= first) & (lane < first + 8), turned(source, first - 120), tile)
                edge[c, p, part, :] = tile

    for x in range(-ITERS, NX + ITERS):
        new = section_of(plane(x), inside(x), products(plane(x - 1)), products(plane(x + 1)))
        for c in range(3):
            work[0][c, x % EX] = new[c]
            if 0 <= x < NX:
                powers[0, c, x] = new[c][:NY]
    for k in range(1, ITERS + 1):
        reach = ITERS - k
        for x in range(-reach, NX + reach):
            for c in range(3):
                source = work[k - 1]
                new = laplace_of(source[c, x % EX], source[c, (x - 1) % EX], source[c, (x + 1) % EX])
                if k < ITERS:
                    new = new * inside(x)
                    work[k][c, x % EX] = new
                if 0 <= x < NX:
                    powers[k, c, x] = new[:NY]
    valid = (lane >= HALO) & (lane < NZ - HALO)
    zero = jnp.zeros((8, NZ), jnp.float32)
    for c in range(3):
        total = [(zero, zero)] * MOMENTS
        for x in range(NX):
            for t in range(2):
                v = [powers[k, c, x, 8 * t : 8 * t + 8, :] for k in range(ITERS + 1)]
                total = [more(s, v[a] * v[b]) for s, (a, b) in zip(total, pairs())]
        for k in range(MOMENTS):
            for part in range(2):
                sums[c, k, part] = jnp.where(valid, total[k][part], 0.0)


def edge_lanes(flags, edge, first, second, sums, powers, moments, whole, *work):
    row = rows((EY, NZ))
    lane = lanes((EY, NZ))
    group, offset = lane // STEP, lane % STEP
    inside = jnp.where(row >= NY + HALO, flags[2:3, :], jnp.where(row >= NY, flags[3:4, :], 1.0))
    inside *= jnp.where(group == 3, flags[0:1, :], jnp.where(group == 2, flags[1:2, :], 1.0))
    inside *= jnp.where(offset < 4, flags[4:5, :], jnp.where(offset >= 24, flags[5:6, :], 1.0))
    odd = is_odd(GZ)
    lowest = lanes((8, NZ)) % STEP < 4
    highest = (lanes((8, NZ)) % STEP >= 24) & (lanes((8, NZ)) % STEP < 28)
    for k in range(Z_TILES):
        low = jnp.where(odd, second[k], first[k])
        high = jnp.where(odd, first[k], second[k])
        for half in range(2):
            c, t = divmod(2 * k + half, 3)
            part = slice(8 * t, 8 * t + 8)
            for p in range(GROUPS if c < 3 else 0):
                value = jnp.where(lowest, turned(low, -4 * half - 8 * p), edge[c, p, part, :])
                whole[c, p, part, :] = jnp.where(highest, turned(high, 24 - 4 * half - 8 * p), value)

    def beyond(read, p):
        return turned(read(0), -STEP) if p == GROUPS - 1 else read(p + 1)

    def behind(read, p):
        return turned(read(GROUPS - 1), STEP) if p == 0 else read(p - 1)

    for p in range(GROUPS):
        at = [whole[c, p] for c in range(3)]
        before, after = (
            [side(lambda q, c=c: whole[0, q] * whole[c, q], p) for c in range(3)] for side in (behind, beyond)
        )
        new = section_of(at, inside, before, after)
        for c in range(3):
            work[0][c, p] = new[c]
            powers[0, c, p] = new[c][:NY]
    for k in range(1, ITERS + 1):
        for p in range(GROUPS):
            for c in range(3):
                read = functools.partial(lambda c, q: work[k - 1][c, q], c)
                new = laplace_of(read(p), behind(read, p), beyond(read, p))
                if k < ITERS:
                    new = new * inside
                    work[k][c, p] = new
                powers[k, c, p] = new[:NY]
    lane = lanes((8, NZ))
    group, offset = lane // STEP, lane % STEP
    valid = (group < 2) & (((offset >= 4) & (offset < 8)) | ((offset >= 20) & (offset < 24)))
    totals = []
    for k in range(MOMENTS):
        a, b = pairs()[k]
        for c in range(3):
            parts = [(p, slice(8 * t, 8 * t + 8)) for p in range(GROUPS) for t in range(2)]
            value = sum(powers[a, c, p, part, :] * powers[b, c, p, part, :] for p, part in parts)
            totals.append(more((sums[c, k, 0], sums[c, k, 1]), jnp.where(valid, value, 0.0)))
    moments[...] = jnp.broadcast_to(lane_totals(totals), moments.shape)


def weights_of(moments, scale):
    middle = moments[1][0] / moments[0][0]
    moments = list(moments)
    for r in range(1, MOMENTS):
        for k in range(MOMENTS - 1, r - 1, -1):
            total, rest = two_product(middle, moments[k - 1][0])
            rest = rest + middle * moments[k - 1][1]
            moments[k] = two_sum(*added(moments[k], (-total, -rest)))
    moments = [m[0] for m in moments]
    diagonal = 1.0 + scale * middle

    def inner(first, second):
        return sum(f * s * moments[i + j] for i, f in enumerate(first) for j, s in enumerate(second))

    def plus(first, factor, second):
        size = max(len(first), len(second))
        padded = [list(v) + [0.0] * (size - len(v)) for v in (first, second)]
        return [f + factor * s for f, s in zip(*padded)]

    def in_powers_of_l(weights):
        weights = list(weights)
        for r in range(len(weights) - 1):
            for k in range(len(weights) - 2, r - 1, -1):
                weights[k] = weights[k] - middle * weights[k + 1]
        return weights

    one = jnp.ones_like(scale)
    total, residual, direction = [], [one], [one]
    now = moments[0]
    for iteration in range(ITERS):
        image = plus([diagonal * d for d in direction], scale, [0.0] + direction)
        step = now / inner(direction, image)
        total = plus(total, step, direction)
        residual = plus(residual, -step, image)
        if iteration + 1 < ITERS:
            new = inner(residual, residual)
            direction = plus(residual, new / now, direction)
            now = new
    return in_powers_of_l(total), in_powers_of_l(residual)


def combine(parts, flags, powers, edges, total, rest):
    lane = lanes((8, NZ))
    high, low = folded(lambda first, size: parts[first : first + size, :], parts.shape[0])
    moments = [(turned(high, -3 * k), turned(low, -3 * k)) for k in range(MOMENTS)]

    def spread(value, c):
        return jnp.broadcast_to(jnp.sum(jnp.where(lane == c, value, 0.0), axis=1, keepdims=True), (8, NZ))

    for out, weights in zip((total, rest), weights_of(moments, jnp.broadcast_to(flags[6:7, :], (8, NZ)))):
        for c in range(3):
            factors = [spread(w, c) for w in weights]

            def mix(read):
                return sum(f * read(k) for k, f in enumerate(factors))

            for p in range(GROUPS):
                for t in range(2):
                    part = slice(8 * t, 8 * t + 8)
                    side = mix(lambda k: edges[k, c, p, part, :])
                    for g in range(2):
                        x = GROUPS * g + p
                        value = mix(lambda k: powers[k, c, x, part, :])
                        value = jnp.where(lane < HALO, turned(side, -(STEP * g + 4)), value)
                        value = jnp.where(lane >= NZ - HALO, turned(side, 104 - STEP * g), value)
                        out[c, x, part, :] = value


def kernel(body, outs, scratch=(), first=False, last=False):
    vmem = pl.BlockSpec(memory_space=pltpu.VMEM)
    shape = jax.ShapeDtypeStruct if last else pltpu.VMEM

    def call(*args):
        if not first:
            args = [pltpu.with_memory_space_constraint(a, pltpu.VMEM) for a in args]
        return pl.pallas_call(
            body,
            in_specs=[vmem] * len(args),
            out_specs=[vmem] * len(outs),
            out_shape=[shape(s, jnp.float32) for s in outs],
            scratch_shapes=[pltpu.VMEM(s, jnp.float32) for s in scratch],
            name=body.__name__,
        )(*args)

    return call


def swapped(first, second, axis):
    size = lax.axis_size(axis)

    def pairs_from(start):
        up = [(i, i + 1) for i in range(start, size - 1, 2)]
        return up + [(b, a) for a, b in up]

    return lax.ppermute(first, axis, pairs_from(1)), lax.ppermute(second, axis, pairs_from(0))


def gathered(row, axes):
    return lax.all_to_all(row, axes, 0, 0, tiled=True)


def body(velocity, diffusion):
    ends = [f for a in (GX, GY, GZ) for f in (lax.axis_index(a) > 0, lax.axis_index(a) + 1 < lax.axis_size(a))]
    flags = jnp.broadcast_to(jnp.stack(ends).astype(jnp.float32)[:, None], (6, NZ))
    flags = jnp.concatenate([flags, jnp.broadcast_to(jnp.pad(6.0 * diffusion, (0, NZ - 3))[None], (2, NZ))])
    block, wide, tiles = (3, NX, NY, NZ), (3, EX, EY, NZ), (3, GROUPS, EY, NZ)
    own, first, second = kernel(pack_y, [block] + [(3, 4, 8, NZ)] * 2, first=True)(velocity)
    beside = swapped(first, second, GY)
    first, second = kernel(pack_x, [(3, 11, 8, NZ)] * 2)(own, *beside)
    beside += swapped(first, second, GX)
    whole, first, second = kernel(pack_z, [wide] + [(Z_TILES, 8, NZ)] * 2)(own, *beside)
    first, second = swapped(first, second, GZ)
    powers, sums, edge = kernel(
        inner_lanes, [(ITERS + 1,) + block, (3, MOMENTS, 2, 8, NZ), tiles], [wide] * ITERS
    )(flags, whole)
    planes, stack = lax.axis_size(GX + GY), lax.axis_size(GZ)
    edges, row = kernel(
        edge_lanes, [(ITERS + 1, 3, GROUPS, NY, NZ), (planes, NZ)], [tiles] * (ITERS + 1)
    )(flags, edge, first, second, sums)
    (row,) = kernel(fold, [(stack, NZ)])(gathered(row, GY + GX))
    return kernel(combine, [block] * 2, last=True)(gathered(row, GZ), flags, powers, edges)


def solution(mesh):
    finer = Mesh(
        mesh.devices.reshape(2, 2, 4, 4, mesh.shape["gz"]), ("gx_0", "gx_1", "gy_0", "gy_1", "gz")
    )
    return jax.shard_map(
        body,
        mesh=finer,
        in_specs=(P(None, GX, GY, "gz"), P()),
        out_specs=(P(None, GX, GY, "gz"), P(None, GX, GY, "gz")),
        check_vma=False,
    )
```

```python
import functools

import jax
import jax.numpy as jnp
from jax import lax
from jax.experimental import pallas as pl
from jax.experimental.pallas import tpu as pltpu
from jax.sharding import Mesh
from jax.sharding import PartitionSpec as P

ITERS = 3
GX = ("gx_0", "gx_1")
GY = ("gy_0", "gy_1")
GZ = ("gz",)
HALO = ITERS + 1

time_step = 0.25

NX, NY, NZ = 8, 16, 128
EX, EY = NX + 2 * HALO, NY + 2 * HALO
GROUPS = 4
STEP = NZ // GROUPS
MOMENTS = 2 * ITERS
Z_TILES = 5


def lanes(shape):
    return lax.broadcasted_iota(jnp.int32, shape, len(shape) - 1)


def rows(shape):
    return lax.broadcasted_iota(jnp.int32, shape, len(shape) - 2)


def back(value, axis):
    return pltpu.roll(value, value.shape[axis] - 1, axis)


def ahead(value, axis):
    return pltpu.roll(value, 1, axis)


def turned(value, shift):
    shift = shift % value.shape[-1]
    return pltpu.roll(value, shift, value.ndim - 1) if shift else value


def is_odd(axes):
    return lax.axis_index(axes) % 2 == 1


def pack_y(block, own, first, second):
    odd = is_odd(GY)
    sub = rows((8, NZ))
    own[...] = block[...]
    for c in range(3):
        for q in range(4):
            up = jnp.where(sub >= 4, block[c, q, 8:16, :], pltpu.roll(block[c, q + 4, 8:16, :], 4, 0))
            down = jnp.where(sub < 4, block[c, q, 0:8, :], pltpu.roll(block[c, q + 4, 0:8, :], 4, 0))
            first[c, q] = jnp.where(odd, up, down)
            second[c, q] = jnp.where(odd, down, up)


def beside_y(odd, first, second, c, x):
    low = jnp.where(odd, second[c, x % 4], first[c, x % 4])
    high = jnp.where(odd, first[c, x % 4], second[c, x % 4])
    sub = rows((8, NZ))
    if x < 4:
        return jnp.where(sub < 4, high, low)
    return pltpu.roll(jnp.where(sub < 4, low, high), 4, 0)


def pack_x(own, first_y, second_y, first, second):
    odd_y, odd = is_odd(GY), is_odd(GX)

    def put(c, n, up, down):
        first[c, n] = jnp.where(odd, up, down)
        second[c, n] = jnp.where(odd, down, up)

    for c in range(3):
        for n in range(HALO):
            for t in range(2):
                part = slice(8 * t, 8 * t + 8)
                put(c, 2 * n + t, own[c, NX - HALO + n, part, :], own[c, n, part, :])
        for n in range(HALO - 1):
            put(
                c,
                8 + n,
                beside_y(odd_y, first_y, second_y, c, NX - HALO + 1 + n),
                beside_y(odd_y, first_y, second_y, c, n),
            )


def pack_z(own, first_y, second_y, first_x, second_x, whole, first, second):
    odd_y, odd, even_z = is_odd(GY), is_odd(GX), ~is_odd(GZ)
    lane = lanes((8, NZ))
    zero = jnp.zeros((8, NZ), jnp.float32)

    def tile_of(c, i, t):
        if i < NX:
            return own[c, i, 8 * t : 8 * t + 8, :] if t < 2 else beside_y(odd_y, first_y, second_y, c, i)
        n = i - NX
        if n < HALO:
            if t == 2 and n == HALO - 1:
                return zero
            k = 2 * n + t if t < 2 else 8 + n
            return jnp.where(odd, first_x[c, k], second_x[c, k])
        n -= HALO
        if t == 2 and n == 0:
            return zero
        k = 2 * n + t if t < 2 else 7 + n
        return jnp.where(odd, second_x[c, k], first_x[c, k])

    def faces(c, t, i, count):
        if count == 1:
            tile = tile_of(c, i, t)
            whole[c, i, 8 * t : 8 * t + 8, :] = tile
            return turned(tile, 8 * i + HALO)
        count //= 2
        early, late = faces(c, t, i, count), faces(c, t, i + count, count)
        return jnp.where(lane // 8 // count % 2 == 1, late, early)

    both = [faces(c, t, 0, EX) for c in range(3) for t in range(3)] + [zero]
    for k in range(Z_TILES):
        early, late = both[2 * k : 2 * k + 2]
        if k == Z_TILES - 1:
            up, down = early, turned(early, -HALO)
        else:
            up = jnp.where(lane % 8 < HALO, early, turned(late, HALO))
            down = jnp.where(lane % 8 < HALO, turned(early, -HALO), late)
        first[k] = jnp.where(even_z, up, down)
        second[k] = jnp.where(even_z, down, up)


def two_sum(a, b):
    total = a + b
    part = total - a
    return total, (a - (total - part)) + (b - part)


def split(a):
    large = a * 4097.0
    high = large - (large - a)
    return high, a - high


def two_product(a, b):
    total = a * b
    (ah, al), (bh, bl) = split(a), split(b)
    return total, ((ah * bh - total) + ah * bl + al * bh) + al * bl


def added(first, second):
    total, rest = two_sum(first[0], second[0])
    return total, (first[1] + second[1]) + rest


def more(total, value):
    high, rest = two_sum(total[0], value)
    return high, total[1] + rest


def rolled(value, shift, axis):
    return tuple(pltpu.roll(v, shift, axis) for v in value)


def chosen(where, first, second):
    return tuple(jnp.where(where, f, s) for f, s in zip(first, second))


def lane_totals(values):
    row, lane = rows((8, NZ)), lanes((8, NZ))
    reverse = (row % 2) * 4 + (row // 2 % 2) * 2 + row // 4
    zero = jnp.zeros((8, NZ), jnp.float32)
    found = zero
    for g in range(0, len(values), 8):
        group = values[g : g + 8]
        group = group + [(zero, zero)] * (8 - len(group))
        for half in (4, 2, 1):
            early = row % (2 * half) < half
            group = [
                added(
                    chosen(early, first, rolled(second, half, 0)),
                    chosen(early, rolled(first, 8 - half, 0), second),
                )
                for first, second in zip(group[::2], group[1::2])
            ]
        total = group[0]
        for half in (64, 32, 16, 8, 4, 2, 1):
            total = added(total, rolled(total, half, 1))
        total = two_sum(*total)
        found = jnp.where(lane == g + reverse, total[0], found)
        found = jnp.where(lane == 64 + g + reverse, total[1], found)
    return jnp.sum(found, axis=0, keepdims=True)


def folded(read, count):
    tiles = []
    for first in range(0, count, 8):
        size = min(8, count - first)
        tile = read(first, size)
        if size < 8:
            tile = jnp.concatenate([tile, jnp.zeros((8 - size, NZ), jnp.float32)], axis=0)
        tiles.append((tile, turned(tile, 64)))
    while len(tiles) > 1:
        tiles = [added(f, s) for f, s in zip(tiles[::2], tiles[1::2])] + tiles[len(tiles) // 2 * 2 :]
    total = tiles[0]
    for half in (4, 2, 1):
        total = added(total, rolled(total, half, 0))
    return two_sum(*total)


def fold(parts, out):
    high, rest = folded(lambda first, size: parts[first : first + size, :], parts.shape[0])
    row = jnp.where(lanes((8, NZ)) < 64, high, turned(rest, 64))[0:1]
    out[...] = jnp.broadcast_to(row, out.shape)


def section_of(at, here, before, after):
    result = []
    for c in range(3):
        slope = after[c] - before[c]
        flux = at[1] * at[c]
        slope = slope + (back(flux, 0) - ahead(flux, 0))
        flux = at[2] * at[c]
        slope = slope + (back(flux, 1) - ahead(flux, 1))
        result.append((at[c] - (0.5 * time_step) * slope) * here)
    return result


def laplace_of(at, before, after):
    beside = (before + after) + (back(at, 0) + ahead(at, 0))
    beside = beside + (back(at, 1) + ahead(at, 1))
    return at - beside * (1.0 / 6.0)


def pairs():
    return [(k // 2, (k + 1) // 2) for k in range(MOMENTS)]


def inner_lanes(flags, whole, powers, sums, edge, *work):
    row = rows((EY, NZ))
    in_y = jnp.where(row < NY, 1.0, jnp.where(row < NY + HALO, flags[3:4, :], flags[2:3, :]))
    below_x, above_x = in_y * flags[0:1, :], in_y * flags[1:2, :]

    def inside(x):
        return below_x if x < 0 else (above_x if x >= NX else in_y)

    def plane(x):
        return [whole[c, x % EX] for c in range(3)]

    def products(value):
        return [value[0] * value[c] for c in range(3)]

    lane = lanes((8, NZ))
    for c in range(3):
        for p in range(GROUPS):
            for t in range(3):
                part = slice(8 * t, 8 * t + 8)
                tile = jnp.zeros((8, NZ), jnp.float32)
                for g in range(GROUPS):
                    source = whole[c, GROUPS * g + p, part, :]
                    first = STEP * g + 4
                    tile = jnp.where((lane >= first) & (lane < first + 8), turned(source, first), tile)
                    first = STEP * g + 16
                    tile = jnp.where((lane >= first) & (lane < first + 8), turned(source, first - 120), tile)
                edge[c, p, part, :] = tile

    for x in range(-ITERS, NX + ITERS):
        new = section_of(plane(x), inside(x), products(plane(x - 1)), products(plane(x + 1)))
        for c in range(3):
            work[0][c, x % EX] = new[c]
            if 0 <= x < NX:
                powers[0, c, x] = new[c][:NY]
    for k in range(1, ITERS + 1):
        reach = ITERS - k
        for x in range(-reach, NX + reach):
            for c in range(3):
                source = work[k - 1]
                new = laplace_of(source[c, x % EX], source[c, (x - 1) % EX], source[c, (x + 1) % EX])
                if k < ITERS:
                    new = new * inside(x)
                    work[k][c, x % EX] = new
                if 0 <= x < NX:
                    powers[k, c, x] = new[:NY]
    valid = (lane >= HALO) & (lane < NZ - HALO)
    zero = jnp.zeros((8, NZ), jnp.float32)
    for c in range(3):
        total = [(zero, zero)] * MOMENTS
        for x in range(NX):
            for t in range(2):
                v = [powers[k, c, x, 8 * t : 8 * t + 8, :] for k in range(ITERS + 1)]
                total = [more(s, v[a] * v[b]) for s, (a, b) in zip(total, pairs())]
        for k in range(MOMENTS):
            for part in range(2):
                sums[c, k, part] = jnp.where(valid, total[k][part], 0.0)


def edge_lanes(flags, edge, first, second, sums, powers, moments, whole, *work):
    row = rows((EY, NZ))
    lane = lanes((EY, NZ))
    group, offset = lane // STEP, lane % STEP
    inside = jnp.where(row >= NY + HALO, flags[2:3, :], jnp.where(row >= NY, flags[3:4, :], 1.0))
    inside *= jnp.where(group == 3, flags[0:1, :], jnp.where(group == 2, flags[1:2, :], 1.0))
    inside *= jnp.where(offset < 4, flags[4:5, :], jnp.where(offset >= 24, flags[5:6, :], 1.0))
    even = ~is_odd(GZ)
    lowest = lanes((8, NZ)) % STEP < 4
    highest = (lanes((8, NZ)) % STEP >= 24) & (lanes((8, NZ)) % STEP < 28)
    for k in range(Z_TILES):
        low = jnp.where(even, second[k], first[k])
        high = jnp.where(even, first[k], second[k])
        for half in range(2):
            c, t = divmod(2 * k + half, 3)
            part = slice(8 * t, 8 * t + 8)
            for p in range(GROUPS if c < 3 else 0):
                value = jnp.where(lowest, turned(low, -4 * half - 8 * p), edge[c, p, part, :])
                whole[c, p, part, :] = jnp.where(highest, turned(high, 24 - 4 * half - 8 * p), value)

    def beyond(read, p):
        return turned(read(0), -STEP) if p == GROUPS - 1 else read(p + 1)

    def behind(read, p):
        return turned(read(GROUPS - 1), STEP) if p == 0 else read(p - 1)

    for p in range(GROUPS):
        at = [whole[c, p] for c in range(3)]
        before, after = (
            [side(lambda q, c=c: whole[0, q] * whole[c, q], p) for c in range(3)] for side in (behind, beyond)
        )
        new = section_of(at, inside, before, after)
        for c in range(3):
            work[0][c, p] = new[c]
            powers[0, c, p] = new[c][:NY]
    for k in range(1, ITERS + 1):
        for p in range(GROUPS):
            for c in range(3):
                read = functools.partial(lambda c, q: work[k - 1][c, q], c)
                new = laplace_of(read(p), behind(read, p), beyond(read, p))
                if k < ITERS:
                    new = new * inside
                    work[k][c, p] = new
                powers[k, c, p] = new[:NY]
    lane = lanes((8, NZ))
    group, offset = lane // STEP, lane % STEP
    valid = (group < 2) & (((offset >= 4) & (offset < 8)) | ((offset >= 20) & (offset < 24)))
    totals = []
    for k in range(MOMENTS):
        a, b = pairs()[k]
        for c in range(3):
            parts = [(p, slice(8 * t, 8 * t + 8)) for p in range(GROUPS) for t in range(2)]
            value = sum(powers[a, c, p, part, :] * powers[b, c, p, part, :] for p, part in parts)
            totals.append(more((sums[c, k, 0], sums[c, k, 1]), jnp.where(valid, value, 0.0)))
    moments[...] = jnp.broadcast_to(lane_totals(totals), moments.shape)


def weights_of(moments, scale):
    middle = moments[1][0] / moments[0][0]
    moments = list(moments)
    for r in range(1, MOMENTS):
        for k in range(MOMENTS - 1, r - 1, -1):
            total, rest = two_product(middle, moments[k - 1][0])
            rest = rest + middle * moments[k - 1][1]
            moments[k] = two_sum(*added(moments[k], (-total, -rest)))
    moments = [m[0] for m in moments]
    diagonal = 1.0 + scale * middle

    def inner(first, second):
        return sum(f * s * moments[i + j] for i, f in enumerate(first) for j, s in enumerate(second))

    def plus(first, factor, second):
        size = max(len(first), len(second))
        padded = [list(v) + [0.0] * (size - len(v)) for v in (first, second)]
        return [f + factor * s for f, s in zip(*padded)]

    def in_powers_of_l(weights):
        weights = list(weights)
        for r in range(len(weights) - 1):
            for k in range(len(weights) - 2, r - 1, -1):
                weights[k] = weights[k] - middle * weights[k + 1]
        return weights

    one = jnp.ones_like(scale)
    total, residual, direction = [], [one], [one]
    now = moments[0]
    for iteration in range(ITERS):
        image = plus([diagonal * d for d in direction], scale, [0.0] + direction)
        step = now / inner(direction, image)
        total = plus(total, step, direction)
        residual = plus(residual, -step, image)
        if iteration + 1 < ITERS:
            new = inner(residual, residual)
            direction = plus(residual, new / now, direction)
            now = new
    return in_powers_of_l(total), in_powers_of_l(residual)


def combine(parts, flags, powers, edges, total, rest):
    lane = lanes((8, NZ))
    high, low = folded(lambda first, size: parts[first : first + size, :], parts.shape[0])
    moments = [(turned(high, -3 * k), turned(low, -3 * k)) for k in range(MOMENTS)]

    def spread(value, c):
        return jnp.broadcast_to(jnp.sum(jnp.where(lane == c, value, 0.0), axis=1, keepdims=True), (8, NZ))

    for out, weights in zip((total, rest), weights_of(moments, jnp.broadcast_to(flags[6:7, :], (8, NZ)))):
        for c in range(3):
            factors = [spread(w, c) for w in weights]

            def mix(read):
                return sum(f * read(k) for k, f in enumerate(factors))

            for p in range(GROUPS):
                for t in range(2):
                    part = slice(8 * t, 8 * t + 8)
                    side = mix(lambda k: edges[k, c, p, part, :])
                    for g in range(2):
                        x = GROUPS * g + p
                        value = mix(lambda k: powers[k, c, x, part, :])
                        value = jnp.where(lane < HALO, turned(side, -(STEP * g + 4)), value)
                        value = jnp.where(lane >= NZ - HALO, turned(side, 104 - STEP * g), value)
                        out[c, x, part, :] = value


def kernel(body, outs, scratch=(), first=False, last=False):
    vmem = pl.BlockSpec(memory_space=pltpu.VMEM)
    shape = jax.ShapeDtypeStruct if last else pltpu.VMEM

    def call(*args):
        if not first:
            args = [pltpu.with_memory_space_constraint(a, pltpu.VMEM) for a in args]
        return pl.pallas_call(
            body,
            in_specs=[vmem] * len(args),
            out_specs=[vmem] * len(outs),
            out_shape=[shape(s, jnp.float32) for s in outs],
            scratch_shapes=[pltpu.VMEM(s, jnp.float32) for s in scratch],
            name=body.__name__,
        )(*args)

    return call


def swapped(first, second, axis, start=1):
    size = lax.axis_size(axis)

    def pairs_from(start):
        up = [(i, i + 1) for i in range(start, size - 1, 2)]
        return up + [(b, a) for a, b in up]

    return lax.ppermute(first, axis, pairs_from(start)), lax.ppermute(second, axis, pairs_from(1 - start))


def gathered(row, axes):
    return lax.all_to_all(row, axes, 0, 0, tiled=True)


def body(velocity, diffusion):
    ends = [f for a in (GX, GY, GZ) for f in (lax.axis_index(a) > 0, lax.axis_index(a) + 1 < lax.axis_size(a))]
    flags = jnp.broadcast_to(jnp.stack(ends).astype(jnp.float32)[:, None], (6, NZ))
    flags = jnp.concatenate([flags, jnp.broadcast_to(jnp.pad(6.0 * diffusion, (0, NZ - 3))[None], (2, NZ))])
    block, wide, tiles = (3, NX, NY, NZ), (3, EX, EY, NZ), (3, GROUPS, EY, NZ)
    own, first, second = kernel(pack_y, [block] + [(3, 4, 8, NZ)] * 2, first=True)(velocity)
    beside = swapped(first, second, GY)
    first, second = kernel(pack_x, [(3, 11, 8, NZ)] * 2)(own, *beside)
    beside += swapped(first, second, GX)
    whole, first, second = kernel(pack_z, [wide] + [(Z_TILES, 8, NZ)] * 2)(own, *beside)
    first, second = swapped(first, second, GZ, start=0)
    powers, sums, edge = kernel(
        inner_lanes, [(ITERS + 1,) + block, (3, MOMENTS, 2, 8, NZ), tiles], [wide] * ITERS
    )(flags, whole)
    planes, stack = lax.axis_size(GX + GY), lax.axis_size(GZ)
    edges, row = kernel(
        edge_lanes, [(ITERS + 1, 3, GROUPS, NY, NZ), (planes, NZ)], [tiles] * (ITERS + 1)
    )(flags, edge, first, second, sums)
    (row,) = kernel(fold, [(stack, NZ)])(gathered(row, GX + GY))
    return kernel(combine, [block] * 2, last=True)(gathered(row, GZ), flags, powers, edges)


def solution(mesh):
    finer = Mesh(
        mesh.devices.reshape(2, 2, 4, 4, mesh.shape["gz"]), ("gx_0", "gx_1", "gy_0", "gy_1", "gz")
    )
    return jax.shard_map(
        body,
        mesh=finer,
        in_specs=(P(None, GX, GY, "gz"), P()),
        out_specs=(P(None, GX, GY, "gz"), P(None, GX, GY, "gz")),
        check_vma=False,
    )
```

```python
import functools

import jax
import jax.numpy as jnp
from jax import lax
from jax.experimental import pallas as pl
from jax.experimental.pallas import tpu as pltpu
from jax.sharding import Mesh
from jax.sharding import PartitionSpec as P

ITERS = 3
GX = ("gx_0", "gx_1")
GY = ("gy_0", "gy_1")
GZ = ("gz",)
HALO = ITERS + 1

time_step = 0.25

NX, NY, NZ = 8, 16, 128
EX, EY = NX + 2 * HALO, NY + 2 * HALO
GROUPS = 4
STEP = NZ // GROUPS
MOMENTS = 2 * ITERS
Z_TILES = 5


def lanes(shape):
    return lax.broadcasted_iota(jnp.int32, shape, len(shape) - 1)


def rows(shape):
    return lax.broadcasted_iota(jnp.int32, shape, len(shape) - 2)


def back(value, axis):
    return pltpu.roll(value, value.shape[axis] - 1, axis)


def ahead(value, axis):
    return pltpu.roll(value, 1, axis)


def turned(value, shift):
    shift = shift % value.shape[-1]
    return pltpu.roll(value, shift, value.ndim - 1) if shift else value


def is_odd(axes):
    return lax.axis_index(axes) % 2 == 1


def pack_y(block, own, first, second):
    even = ~is_odd(GY)
    sub = rows((8, NZ))
    own[...] = block[...]
    for c in range(3):
        for q in range(4):
            up = jnp.where(sub >= 4, block[c, q, 8:16, :], pltpu.roll(block[c, q + 4, 8:16, :], 4, 0))
            down = jnp.where(sub < 4, block[c, q, 0:8, :], pltpu.roll(block[c, q + 4, 0:8, :], 4, 0))
            first[c, q] = jnp.where(even, up, down)
            second[c, q] = jnp.where(even, down, up)


def beside_y(even, first, second, c, x):
    low = jnp.where(even, second[c, x % 4], first[c, x % 4])
    high = jnp.where(even, first[c, x % 4], second[c, x % 4])
    sub = rows((8, NZ))
    if x < 4:
        return jnp.where(sub < 4, high, low)
    return pltpu.roll(jnp.where(sub < 4, low, high), 4, 0)


def pack_x(own, first_y, second_y, first, second):
    even_y, odd = ~is_odd(GY), is_odd(GX)

    def put(c, n, up, down):
        first[c, n] = jnp.where(odd, up, down)
        second[c, n] = jnp.where(odd, down, up)

    for c in range(3):
        for n in range(HALO):
            for t in range(2):
                part = slice(8 * t, 8 * t + 8)
                put(c, 2 * n + t, own[c, NX - HALO + n, part, :], own[c, n, part, :])
        for n in range(HALO - 1):
            put(
                c,
                8 + n,
                beside_y(even_y, first_y, second_y, c, NX - HALO + 1 + n),
                beside_y(even_y, first_y, second_y, c, n),
            )


def pack_z(own, first_y, second_y, first_x, second_x, whole, first, second):
    even_y, odd, even_z = ~is_odd(GY), is_odd(GX), ~is_odd(GZ)
    lane = lanes((8, NZ))
    zero = jnp.zeros((8, NZ), jnp.float32)

    def tile_of(c, i, t):
        if i < NX:
            return own[c, i, 8 * t : 8 * t + 8, :] if t < 2 else beside_y(even_y, first_y, second_y, c, i)
        n = i - NX
        if n < HALO:
            if t == 2 and n == HALO - 1:
                return zero
            k = 2 * n + t if t < 2 else 8 + n
            return jnp.where(odd, first_x[c, k], second_x[c, k])
        n -= HALO
        if t == 2 and n == 0:
            return zero
        k = 2 * n + t if t < 2 else 7 + n
        return jnp.where(odd, second_x[c, k], first_x[c, k])

    def faces(c, t, i, count):
        if count == 1:
            tile = tile_of(c, i, t)
            whole[c, i, 8 * t : 8 * t + 8, :] = tile
            return turned(tile, 8 * i + HALO)
        count //= 2
        early, late = faces(c, t, i, count), faces(c, t, i + count, count)
        return jnp.where(lane // 8 // count % 2 == 1, late, early)

    both = [faces(c, t, 0, EX) for c in range(3) for t in range(3)] + [zero]
    for k in range(Z_TILES):
        early, late = both[2 * k : 2 * k + 2]
        if k == Z_TILES - 1:
            up, down = early, turned(early, -HALO)
        else:
            up = jnp.where(lane % 8 < HALO, early, turned(late, HALO))
            down = jnp.where(lane % 8 < HALO, turned(early, -HALO), late)
        first[k] = jnp.where(even_z, up, down)
        second[k] = jnp.where(even_z, down, up)


def two_sum(a, b):
    total = a + b
    part = total - a
    return total, (a - (total - part)) + (b - part)


def split(a):
    large = a * 4097.0
    high = large - (large - a)
    return high, a - high


def two_product(a, b):
    total = a * b
    (ah, al), (bh, bl) = split(a), split(b)
    return total, ((ah * bh - total) + ah * bl + al * bh) + al * bl


def added(first, second):
    total, rest = two_sum(first[0], second[0])
    return total, (first[1] + second[1]) + rest


def more(total, value):
    high, rest = two_sum(total[0], value)
    return high, total[1] + rest


def rolled(value, shift, axis):
    return tuple(pltpu.roll(v, shift, axis) for v in value)


def chosen(where, first, second):
    return tuple(jnp.where(where, f, s) for f, s in zip(first, second))


def lane_totals(values):
    row, lane = rows((8, NZ)), lanes((8, NZ))
    reverse = (row % 2) * 4 + (row // 2 % 2) * 2 + row // 4
    zero = jnp.zeros((8, NZ), jnp.float32)
    found = zero
    for g in range(0, len(values), 8):
        group = values[g : g + 8]
        group = group + [(zero, zero)] * (8 - len(group))
        for half in (4, 2, 1):
            early = row % (2 * half) < half
            group = [
                added(
                    chosen(early, first, rolled(second, half, 0)),
                    chosen(early, rolled(first, 8 - half, 0), second),
                )
                for first, second in zip(group[::2], group[1::2])
            ]
        total = group[0]
        for half in (64, 32, 16, 8, 4, 2, 1):
            total = added(total, rolled(total, half, 1))
        total = two_sum(*total)
        found = jnp.where(lane == g + reverse, total[0], found)
        found = jnp.where(lane == 64 + g + reverse, total[1], found)
    return jnp.sum(found, axis=0, keepdims=True)


def folded(read, count):
    tiles = []
    for first in range(0, count, 8):
        size = min(8, count - first)
        tile = read(first, size)
        if size < 8:
            tile = jnp.concatenate([tile, jnp.zeros((8 - size, NZ), jnp.float32)], axis=0)
        tiles.append((tile, turned(tile, 64)))
    while len(tiles) > 1:
        tiles = [added(f, s) for f, s in zip(tiles[::2], tiles[1::2])] + tiles[len(tiles) // 2 * 2 :]
    total = tiles[0]
    for half in (4, 2, 1):
        total = added(total, rolled(total, half, 0))
    return two_sum(*total)


def fold(parts, out):
    high, rest = folded(lambda first, size: parts[first : first + size, :], parts.shape[0])
    row = jnp.where(lanes((8, NZ)) < 64, high, turned(rest, 64))[0:1]
    out[...] = jnp.broadcast_to(row, out.shape)


def section_of(at, here, before, after):
    result = []
    for c in range(3):
        slope = after[c] - before[c]
        flux = at[1] * at[c]
        slope = slope + (back(flux, 0) - ahead(flux, 0))
        flux = at[2] * at[c]
        slope = slope + (back(flux, 1) - ahead(flux, 1))
        result.append((at[c] - (0.5 * time_step) * slope) * here)
    return result


def laplace_of(at, before, after):
    beside = (before + after) + (back(at, 0) + ahead(at, 0))
    beside = beside + (back(at, 1) + ahead(at, 1))
    return at - beside * (1.0 / 6.0)


def pairs():
    return [(k // 2, (k + 1) // 2) for k in range(MOMENTS)]


def inner_lanes(flags, whole, powers, sums, edge, *work):
    row = rows((EY, NZ))
    in_y = jnp.where(row < NY, 1.0, jnp.where(row < NY + HALO, flags[3:4, :], flags[2:3, :]))
    below_x, above_x = in_y * flags[0:1, :], in_y * flags[1:2, :]

    def inside(x):
        return below_x if x < 0 else (above_x if x >= NX else in_y)

    def plane(x):
        return [whole[c, x % EX] for c in range(3)]

    def products(value):
        return [value[0] * value[c] for c in range(3)]

    lane = lanes((8, NZ))
    for c in range(3):
        for p in range(GROUPS):
            for t in range(3):
                part = slice(8 * t, 8 * t + 8)
                tile = jnp.zeros((8, NZ), jnp.float32)
                for g in range(GROUPS):
                    source = whole[c, GROUPS * g + p, part, :]
                    first = STEP * g + 4
                    tile = jnp.where((lane >= first) & (lane < first + 8), turned(source, first), tile)
                    first = STEP * g + 16
                    tile = jnp.where((lane >= first) & (lane < first + 8), turned(source, first - 120), tile)
                edge[c, p, part, :] = tile

    for x in range(-ITERS, NX + ITERS):
        new = section_of(plane(x), inside(x), products(plane(x - 1)), products(plane(x + 1)))
        for c in range(3):
            work[0][c, x % EX] = new[c]
            if 0 <= x < NX:
                powers[0, c, x] = new[c][:NY]
    for k in range(1, ITERS + 1):
        reach = ITERS - k
        for x in range(-reach, NX + reach):
            for c in range(3):
                source = work[k - 1]
                new = laplace_of(source[c, x % EX], source[c, (x - 1) % EX], source[c, (x + 1) % EX])
                if k < ITERS:
                    new = new * inside(x)
                    work[k][c, x % EX] = new
                if 0 <= x < NX:
                    powers[k, c, x] = new[:NY]
    valid = (lane >= HALO) & (lane < NZ - HALO)
    zero = jnp.zeros((8, NZ), jnp.float32)
    for c in range(3):
        total = [(zero, zero)] * MOMENTS
        for x in range(NX):
            for t in range(2):
                v = [powers[k, c, x, 8 * t : 8 * t + 8, :] for k in range(ITERS + 1)]
                total = [more(s, v[a] * v[b]) for s, (a, b) in zip(total, pairs())]
        for k in range(MOMENTS):
            for part in range(2):
                sums[c, k, part] = jnp.where(valid, total[k][part], 0.0)


def edge_lanes(flags, edge, first, second, sums, powers, moments, whole, *work):
    row = rows((EY, NZ))
    lane = lanes((EY, NZ))
    group, offset = lane // STEP, lane % STEP
    inside = jnp.where(row >= NY + HALO, flags[2:3, :], jnp.where(row >= NY, flags[3:4, :], 1.0))
    inside *= jnp.where(group == 3, flags[0:1, :], jnp.where(group == 2, flags[1:2, :], 1.0))
    inside *= jnp.where(offset < 4, flags[4:5, :], jnp.where(offset >= 24, flags[5:6, :], 1.0))
    even = ~is_odd(GZ)
    lowest = lanes((8, NZ)) % STEP < 4
    highest = (lanes((8, NZ)) % STEP >= 24) & (lanes((8, NZ)) % STEP < 28)
    for k in range(Z_TILES):
        low = jnp.where(even, second[k], first[k])
        high = jnp.where(even, first[k], second[k])
        for half in range(2):
            c, t = divmod(2 * k + half, 3)
            part = slice(8 * t, 8 * t + 8)
            for p in range(GROUPS if c < 3 else 0):
                value = jnp.where(lowest, turned(low, -4 * half - 8 * p), edge[c, p, part, :])
                whole[c, p, part, :] = jnp.where(highest, turned(high, 24 - 4 * half - 8 * p), value)

    def beyond(read, p):
        return turned(read(0), -STEP) if p == GROUPS - 1 else read(p + 1)

    def behind(read, p):
        return turned(read(GROUPS - 1), STEP) if p == 0 else read(p - 1)

    for p in range(GROUPS):
        at = [whole[c, p] for c in range(3)]
        before, after = (
            [side(lambda q, c=c: whole[0, q] * whole[c, q], p) for c in range(3)] for side in (behind, beyond)
        )
        new = section_of(at, inside, before, after)
        for c in range(3):
            work[0][c, p] = new[c]
            powers[0, c, p] = new[c][:NY]
    for k in range(1, ITERS + 1):
        for p in range(GROUPS):
            for c in range(3):
                read = functools.partial(lambda c, q: work[k - 1][c, q], c)
                new = laplace_of(read(p), behind(read, p), beyond(read, p))
                if k < ITERS:
                    new = new * inside
                    work[k][c, p] = new
                powers[k, c, p] = new[:NY]
    lane = lanes((8, NZ))
    group, offset = lane // STEP, lane % STEP
    valid = (group < 2) & (((offset >= 4) & (offset < 8)) | ((offset >= 20) & (offset < 24)))
    totals = []
    for k in range(MOMENTS):
        a, b = pairs()[k]
        for c in range(3):
            parts = [(p, slice(8 * t, 8 * t + 8)) for p in range(GROUPS) for t in range(2)]
            value = sum(powers[a, c, p, part, :] * powers[b, c, p, part, :] for p, part in parts)
            totals.append(more((sums[c, k, 0], sums[c, k, 1]), jnp.where(valid, value, 0.0)))
    moments[...] = jnp.broadcast_to(lane_totals(totals), moments.shape)


def weights_of(moments, scale):
    middle = moments[1][0] / moments[0][0]
    moments = list(moments)
    for r in range(1, MOMENTS):
        for k in range(MOMENTS - 1, r - 1, -1):
            total, rest = two_product(middle, moments[k - 1][0])
            rest = rest + middle * moments[k - 1][1]
            moments[k] = two_sum(*added(moments[k], (-total, -rest)))
    moments = [m[0] for m in moments]
    diagonal = 1.0 + scale * middle

    def inner(first, second):
        return sum(f * s * moments[i + j] for i, f in enumerate(first) for j, s in enumerate(second))

    def plus(first, factor, second):
        size = max(len(first), len(second))
        padded = [list(v) + [0.0] * (size - len(v)) for v in (first, second)]
        return [f + factor * s for f, s in zip(*padded)]

    def in_powers_of_l(weights):
        weights = list(weights)
        for r in range(len(weights) - 1):
            for k in range(len(weights) - 2, r - 1, -1):
                weights[k] = weights[k] - middle * weights[k + 1]
        return weights

    one = jnp.ones_like(scale)
    total, residual, direction = [], [one], [one]
    now = moments[0]
    for iteration in range(ITERS):
        image = plus([diagonal * d for d in direction], scale, [0.0] + direction)
        step = now / inner(direction, image)
        total = plus(total, step, direction)
        residual = plus(residual, -step, image)
        if iteration + 1 < ITERS:
            new = inner(residual, residual)
            direction = plus(residual, new / now, direction)
            now = new
    return in_powers_of_l(total), in_powers_of_l(residual)


def combine(parts, flags, powers, edges, total, rest):
    lane = lanes((8, NZ))
    high, low = folded(lambda first, size: parts[first : first + size, :], parts.shape[0])
    moments = [(turned(high, -3 * k), turned(low, -3 * k)) for k in range(MOMENTS)]

    def spread(value, c):
        return jnp.broadcast_to(jnp.sum(jnp.where(lane == c, value, 0.0), axis=1, keepdims=True), (8, NZ))

    for out, weights in zip((total, rest), weights_of(moments, jnp.broadcast_to(flags[6:7, :], (8, NZ)))):
        for c in range(3):
            factors = [spread(w, c) for w in weights]

            def mix(read):
                return sum(f * read(k) for k, f in enumerate(factors))

            for p in range(GROUPS):
                for t in range(2):
                    part = slice(8 * t, 8 * t + 8)
                    side = mix(lambda k: edges[k, c, p, part, :])
                    for g in range(2):
                        x = GROUPS * g + p
                        value = mix(lambda k: powers[k, c, x, part, :])
                        value = jnp.where(lane < HALO, turned(side, -(STEP * g + 4)), value)
                        value = jnp.where(lane >= NZ - HALO, turned(side, 104 - STEP * g), value)
                        out[c, x, part, :] = value


def kernel(body, outs, scratch=(), first=False, last=False):
    vmem = pl.BlockSpec(memory_space=pltpu.VMEM)
    shape = jax.ShapeDtypeStruct if last else pltpu.VMEM

    def call(*args):
        if not first:
            args = [pltpu.with_memory_space_constraint(a, pltpu.VMEM) for a in args]
        return pl.pallas_call(
            body,
            in_specs=[vmem] * len(args),
            out_specs=[vmem] * len(outs),
            out_shape=[shape(s, jnp.float32) for s in outs],
            scratch_shapes=[pltpu.VMEM(s, jnp.float32) for s in scratch],
            name=body.__name__,
        )(*args)

    return call


def swapped(first, second, axis, start=1):
    size = lax.axis_size(axis)

    def pairs_from(start):
        up = [(i, i + 1) for i in range(start, size - 1, 2)]
        return up + [(b, a) for a, b in up]

    return lax.ppermute(first, axis, pairs_from(start)), lax.ppermute(second, axis, pairs_from(1 - start))


def gathered(row, axes):
    return lax.all_to_all(row, axes, 0, 0, tiled=True)


def body(velocity, diffusion):
    ends = [f for a in (GX, GY, GZ) for f in (lax.axis_index(a) > 0, lax.axis_index(a) + 1 < lax.axis_size(a))]
    flags = jnp.broadcast_to(jnp.stack(ends).astype(jnp.float32)[:, None], (6, NZ))
    flags = jnp.concatenate([flags, jnp.broadcast_to(jnp.pad(6.0 * diffusion, (0, NZ - 3))[None], (2, NZ))])
    block, wide, tiles = (3, NX, NY, NZ), (3, EX, EY, NZ), (3, GROUPS, EY, NZ)
    own, first, second = kernel(pack_y, [block] + [(3, 4, 8, NZ)] * 2, first=True)(velocity)
    beside = swapped(first, second, GY, start=0)
    first, second = kernel(pack_x, [(3, 11, 8, NZ)] * 2)(own, *beside)
    beside += swapped(first, second, GX)
    whole, first, second = kernel(pack_z, [wide] + [(Z_TILES, 8, NZ)] * 2)(own, *beside)
    first, second = swapped(first, second, GZ, start=0)
    powers, sums, edge = kernel(
        inner_lanes, [(ITERS + 1,) + block, (3, MOMENTS, 2, 8, NZ), tiles], [wide] * ITERS
    )(flags, whole)
    planes, stack = lax.axis_size(GX + GY), lax.axis_size(GZ)
    edges, row = kernel(
        edge_lanes, [(ITERS + 1, 3, GROUPS, NY, NZ), (planes, NZ)], [tiles] * (ITERS + 1)
    )(flags, edge, first, second, sums)
    (row,) = kernel(fold, [(stack, NZ)])(gathered(row, GX + GY))
    return kernel(combine, [block] * 2, last=True)(gathered(row, GZ), flags, powers, edges)


def solution(mesh):
    finer = Mesh(
        mesh.devices.reshape(2, 2, 4, 4, mesh.shape["gz"]), ("gx_0", "gx_1", "gy_0", "gy_1", "gz")
    )
    return jax.shard_map(
        body,
        mesh=finer,
        in_specs=(P(None, GX, GY, "gz"), P()),
        out_specs=(P(None, GX, GY, "gz"), P(None, GX, GY, "gz")),
        check_vma=False,
    )
```
